8 devices in a mesh: stage: 2 (over z, y), data: 4 (over x, core).
Axes of the slice: x: 2, y: 2, z: 1, core: 2. Of those that a mesh axis runs over, the one named last changes fastest.
Arguments:
- grad_attn: float32 [8, 4, 448, 448], P(('stage', 'data')), parts along dimension 0
- grad_shared_in: float32 [8, 2, 448, 2560], P(('stage', 'data')), parts along dimension 0
- grad_shared_out: float32 [8, 1, 2560, 448], P(('stage', 'data')), parts along dimension 0
- grad_expert_in: float32 [8, 32, 448, 320], P(('stage', 'data')), parts along dimension 0
- grad_expert_out: float32 [8, 16, 320, 448], P(('stage', 'data')), parts along dimension 0
- mom_attn: float32 [8, 448, 448], P('stage', 'data'), parts along dimension 0
- mom_shared_in: float32 [4, 448, 2560], P('stage', 'data'), parts along dimension 0
- mom_shared_out: float32 [2, 2560, 448], P('stage', 'data'), parts along dimension 0
- mom_expert_in: float32 [64, 448, 320], P('stage', 'data'), parts along dimension 0
- mom_expert_out: float32 [32, 320, 448], P('stage', 'data'), parts along dimension 0
- master_attn: float32 [8, 448, 448], P('stage', 'data'), parts along dimension 0
- master_shared_in: float32 [4, 448, 2560], P('stage', 'data'), parts along dimension 0
- master_shared_out: float32 [2, 2560, 448], P('stage', 'data'), parts along dimension 0
- master_expert_in: float32 [64, 448, 320], P('stage', 'data'), parts along dimension 0
- master_expert_out: float32 [32, 320, 448], P('stage', 'data'), parts along dimension 0
Outputs:
- output 1: float32 [8, 448, 448], P('stage', 'data'), parts along dimension 0
- output 2: float32 [4, 448, 2560], P('stage', 'data'), parts along dimension 0
- output 3: float32 [2, 2560, 448], P('stage', 'data'), parts along dimension 0
- output 4: float32 [64, 448, 320], P('stage', 'data'), parts along dimension 0
- output 5: float32 [32, 320, 448], P('stage', 'data'), parts along dimension 0
- output 6: float32 [8, 448, 448], P('stage', 'data'), parts along dimension 0
- output 7: float32 [4, 448, 2560], P('stage', 'data'), parts along dimension 0
- output 8: float32 [2, 2560, 448], P('stage', 'data'), parts along dimension 0
- output 9: float32 [64, 448, 320], P('stage', 'data'), parts along dimension 0
- output 10: float32 [32, 320, 448], P('stage', 'data'), parts along dimension 0
- output 11: bfloat16 [8, 448, 448], P('stage'), parts along dimension 0
- output 12: bfloat16 [4, 448, 2560], P('stage'), parts along dimension 0
- output 13: bfloat16 [2, 2560, 448], P('stage'), parts along dimension 0
- output 14: bfloat16 [64, 448, 320], P('stage'), parts along dimension 0
- output 15: bfloat16 [32, 320, 448], P('stage'), parts along dimension 0
There are 2 independent parts. The reference program is written for one: setup_inputs(seed, part) draws one part's arguments, and reference() takes and returns one part's arrays. A program takes and returns all parts, laid end to end along the dimension named above; each array names one.
All inputs are finite; a program needn't handle non-finite values.
Results may differ from the reference program's by a relative error of at most 0.00507594.
Values are sent between devices in bfloat16 or wider.
A program may use at most 1 GiB of HBM per device.

```python
import math
import jax
import jax.numpy as jnp
from jax import lax

DATA_DEVICES = 4
DIM_MODEL = 448
DIM_EXPERT = 320
DIM_SHARED = 2560
NUM_EXPERTS = 16
NS_STEPS = 5

MOMENTUM = 0.95
LEARN_RATE = 0.2
WEIGHT_DECAY = 0.25
NORM_EPS = 1e-7
COEF_A = 3.4445
COEF_B = -4.7750
COEF_C = 2.0315
KIND_NAMES = ("attn", "shared_in", "shared_out", "expert_in", "expert_out")


def kind_shapes():
    return (
        (4, DIM_MODEL, DIM_MODEL),
        (2, DIM_MODEL, DIM_SHARED),
        (1, DIM_SHARED, DIM_MODEL),
        (2 * NUM_EXPERTS, DIM_MODEL, DIM_EXPERT),
        (NUM_EXPERTS, DIM_EXPERT, DIM_MODEL),
    )


def setup_inputs(seed: int = 0, part: int = 0) -> dict:
    base_key = jax.random.fold_in(jax.random.key(seed), part)
    mom_scale = DATA_DEVICES ** -0.5
    grads = {}
    moms = {}
    masters = {}
    for kind_index, (kind_name, mat_shape) in enumerate(zip(KIND_NAMES, kind_shapes())):
        grad_key, mom_key, master_key = jax.random.split(jax.random.fold_in(base_key, kind_index), 3)
        grads["grad_" + kind_name] = jax.random.normal(grad_key, (DATA_DEVICES,) + mat_shape, jnp.float32)
        moms["mom_" + kind_name] = mom_scale * jax.random.normal(mom_key, mat_shape, jnp.float32)
        masters["master_" + kind_name] = 0.5 * jax.random.normal(master_key, mat_shape, jnp.float32)
    result = {}
    result.update(grads)
    result.update(moms)
    result.update(masters)
    return result


def orthogonalize(matrix):
    is_tall = matrix.shape[0] > matrix.shape[1]
    frob_norm = jnp.sqrt(jnp.sum(matrix * matrix))
    iterate = (matrix / (frob_norm + NORM_EPS)).astype(jnp.bfloat16)
    if is_tall:
        iterate = iterate.T
    for iteration in range(NS_STEPS):
        gram_mat = jnp.dot(iterate, iterate.T, preferred_element_type=jnp.float32).astype(jnp.bfloat16)
        square = jnp.dot(gram_mat, gram_mat, preferred_element_type=jnp.float32)
        poly_mat = (COEF_B * gram_mat.astype(jnp.float32) + COEF_C * square).astype(jnp.bfloat16)
        update = jnp.dot(poly_mat, iterate, preferred_element_type=jnp.float32)
        iterate = (COEF_A * iterate.astype(jnp.float32) + update).astype(jnp.bfloat16)
    if is_tall:
        iterate = iterate.T
    return iterate


def kind_step(grad_stack, old_mom, master):
    num_rows = old_mom.shape[1]
    num_cols = old_mom.shape[2]
    grad_mean = jnp.sum(grad_stack, axis=0) / DATA_DEVICES
    new_mom = MOMENTUM * old_mom + grad_mean
    ortho_mat = lax.map(orthogonalize, new_mom)
    step_scale = 0.2 * math.sqrt(max(num_rows, num_cols))
    new_master = master - LEARN_RATE * (step_scale * ortho_mat.astype(jnp.float32) + WEIGHT_DECAY * master)
    return new_mom, new_master, new_master.astype(jnp.bfloat16)


def reference(grad_attn, grad_shared_in, grad_shared_out, grad_expert_in, grad_expert_out,
              mom_attn, mom_shared_in, mom_shared_out, mom_expert_in, mom_expert_out,
              master_attn, master_shared_in, master_shared_out, master_expert_in, master_expert_out):
    grad_list = (grad_attn, grad_shared_in, grad_shared_out, grad_expert_in, grad_expert_out)
    mom_list = (mom_attn, mom_shared_in, mom_shared_out, mom_expert_in, mom_expert_out)
    master_list = (master_attn, master_shared_in, master_shared_out, master_expert_in, master_expert_out)
    results = [kind_step(grad_list[kind_index], mom_list[kind_index], master_list[kind_index]) for kind_index in range(5)]
    return (results[0][0], results[1][0], results[2][0], results[3][0], results[4][0],
            results[0][1], results[1][1], results[2][1], results[3][1], results[4][1],
            results[0][2], results[1][2], results[2][2], results[3][2], results[4][2])
```

```python
import functools
import math
import jax
import jax.numpy as jnp
from jax import lax
from jax.experimental import pallas as pl
from jax.experimental.pallas import tpu as pltpu
from jax.sharding import PartitionSpec as P

NS_STEPS = 5
MOMENTUM = 0.95
LEARN_RATE = 0.2
WEIGHT_DECAY = 0.25
NORM_EPS = 1e-7
COEF_A = 3.4445
COEF_B = -4.7750
COEF_C = 2.0315
F32 = jnp.float32
BF16 = jnp.bfloat16

UNIT_MATS = (2, 2, 1, 4, 4)
ORDER = (3, 2, 1, 0, 4)
LAGS = (0, 2, 3, 4, 5, 6, 7)


class Kind:
    def __init__(self, index, count, rows, cols):
        self.index = index
        self.count, self.rows, self.cols = count, rows, cols
        self.quarter = rows // 4
        self.unit = UNIT_MATS[index]
        self.units = count // self.unit
        self.split = self.unit % 2 == 0
        self.half = self.unit // 2 if self.split else self.unit
        self.single = self.units == 1
        self.tall = rows > cols
        self.scale = 0.2 * math.sqrt(max(rows, cols))
        if index == 1:
            self.chunks = [(0, 1, 0, self.quarter), (1, 1, 0, self.quarter)]
        elif index == 2:
            step = self.quarter // 2
            self.chunks = [(0, 1, 0, step), (0, 1, step, step)]
        else:
            self.chunks = [(0, self.unit, 0, self.quarter)]

    def scratch(self):
        unit, quarter, cols = self.unit, self.quarter, self.cols
        _, cmats, _, crows = self.chunks[0]
        chunk = pltpu.VMEM((cmats, crows, cols), F32)
        shapes = dict(
            gf=chunk, df=chunk, gn=chunk, dn=chunk, xl=chunk,
            mo=pltpu.VMEM((1 if self.single else 2, unit, quarter, cols), F32),
            sb=pltpu.VMEM((1 if self.single else 2, unit, quarter, cols), F32),
            xs=pltpu.VMEM((1 if self.single else 2, unit, quarter, cols), BF16),
            pb=pltpu.VMEM((unit, quarter, cols), BF16),
            xg=pltpu.VMEM((self.units, self.half, self.rows, cols), BF16),
            nr=pltpu.VMEM((self.units, 4, 8, 128), F32),
            d2d_s=pltpu.SemaphoreType.DMA((self.units, 2)),
            d2d_r=pltpu.SemaphoreType.DMA((self.units, 2)),
            rs_s=pltpu.SemaphoreType.DMA((self.units,)),
            rs_r=pltpu.SemaphoreType.DMA((self.units,)),
            nm_s=pltpu.SemaphoreType.DMA((self.units, 3)),
            nm_r=pltpu.SemaphoreType.DMA((self.units, 3)),
            x_s=pltpu.SemaphoreType.DMA((self.units, 3)),
            x_r=pltpu.SemaphoreType.DMA((self.units, 3)),
            p_s=pltpu.SemaphoreType.DMA((self.units, 3)),
            p_r=pltpu.SemaphoreType.DMA((self.units, 3)),
            loc=pltpu.SemaphoreType.DMA((10,)),
        )
        if not self.single:
            shapes["w"] = pltpu.VMEM((unit, quarter, cols), F32)
        if self.split:
            shapes["orow"] = pltpu.VMEM((self.units, self.half, quarter, cols), BF16)
            shapes["o_s"] = pltpu.SemaphoreType.DMA((self.units,))
            shapes["o_r"] = pltpu.SemaphoreType.DMA((self.units,))
        return shapes


def dot(left, right, dims):
    return lax.dot_general(left, right, (dims, ((), ())), preferred_element_type=F32)


def newton_schulz(kind, xg, u, gram_acc):
    rows, cols = kind.rows, kind.cols

    def poly(gram_mat):
        square = dot(gram_mat, gram_mat, ((1,), (0,)))
        return (COEF_B * gram_mat.astype(F32) + COEF_C * square).astype(BF16)

    if kind.index == 2:
        block = 512

        def iteration(_, carry):
            gram_acc[...] = jnp.zeros_like(gram_acc)

            def add(b, c):
                part = xg[u, 0, pl.ds(pl.multiple_of(b * block, block), block), :]
                gram_acc[...] += dot(part, part, ((0,), (0,)))
                return c

            lax.fori_loop(0, rows // block, add, 0)
            poly_mat = poly(gram_acc[...].astype(BF16))

            def apply(b, c):
                cut = pl.ds(pl.multiple_of(b * block, block), block)
                part = xg[u, 0, cut, :]
                update = dot(part, poly_mat, ((1,), (1,)))
                xg[u, 0, cut, :] = (COEF_A * part.astype(F32) + update).astype(BF16)
                return c

            lax.fori_loop(0, rows // block, apply, 0)
            return carry
    elif kind.index == 1:
        block = 512

        def iteration(_, carry):
            gram_acc[...] = jnp.zeros_like(gram_acc)

            def add(b, c):
                part = xg[u, 0, :, pl.ds(pl.multiple_of(b * block, block), block)]
                gram_acc[...] += dot(part, part, ((1,), (1,)))
                return c

            lax.fori_loop(0, cols // block, add, 0)
            poly_mat = poly(gram_acc[...].astype(BF16))

            def apply(b, c):
                cut = pl.ds(pl.multiple_of(b * block, block), block)
                part = xg[u, 0, :, cut]
                update = dot(poly_mat, part, ((1,), (0,)))
                xg[u, 0, :, cut] = (COEF_A * part.astype(F32) + update).astype(BF16)
                return c

            lax.fori_loop(0, cols // block, apply, 0)
            return carry
    else:

        def iteration(_, carry):
            for j in range(kind.half):
                mat = xg[u, j]
                if kind.tall:
                    gram_mat = dot(mat, mat, ((0,), (0,))).astype(BF16)
                    update = dot(mat, poly(gram_mat), ((1,), (1,)))
                else:
                    gram_mat = dot(mat, mat, ((1,), (1,))).astype(BF16)
                    update = dot(poly(gram_mat), mat, ((1,), (0,)))
                xg[u, j] = (COEF_A * mat.astype(F32) + update).astype(BF16)
            return carry

    lax.fori_loop(0, NS_STEPS, iteration, 0)


def kernel(kinds, names, *refs):
    num = len(kinds)
    grads, moms, masters = refs[:num], refs[num:2 * num], refs[2 * num:3 * num]
    outs = refs[3 * num:8 * num]
    new_moms, new_masters, params, lands, far_lands = [outs[i * num:(i + 1) * num] for i in range(5)]
    rest = list(refs[8 * num:])
    bufs = []
    for k in range(num):
        bufs.append({name: rest.pop(0) for name in names[k]})
    gram_acc = rest.pop(0)

    me = lax.axis_index("data")
    chip, core = me // 2, me % 2
    far, other = 1 - chip, 1 - core
    partner, far_same, far_other = 2 * chip + other, 2 * far + core, 2 * far + other

    def to(device):
        return dict(device_id={"data": device}, device_id_type=pl.DeviceIdType.MESH)

    def remote(src, dst, send, recv, device):
        return pltpu.make_async_remote_copy(src_ref=src, dst_ref=dst, send_sem=send, recv_sem=recv, **to(device))

    def local(src, dst, sem):
        return pltpu.make_async_copy(src, dst, sem)

    barrier = pltpu.get_barrier_semaphore()
    for device in (partner, far_same, far_other):
        pl.semaphore_signal(barrier, inc=1, **to(device))
    pl.semaphore_wait(barrier, 3)

    def rows_of(kind, device, offset=0, size=None):
        size = kind.quarter if size is None else size
        return pl.ds(pl.multiple_of(device * kind.quarter + offset, 16), size)

    class Stage:
        def __init__(self, kind):
            self.kind = kind
            self.b = bufs[kind.index]
            self.grad, self.mom, self.master = grads[kind.index], moms[kind.index], masters[kind.index]
            self.new_mom, self.new_master, self.param = new_moms[kind.index], new_masters[kind.index], params[kind.index]
            self.land, self.far_land = lands[kind.index], far_lands[kind.index]

        def mats(self, u, offset=0, size=None):
            kind = self.kind
            return pl.ds(u * kind.unit + offset, kind.unit if size is None else size)

        def slot(self, u):
            return 0 if self.kind.single else u % 2

        def exchange(self, u):
            kind, b = self.kind, self.b
            mats = self.mats(u)
            return [
                remote(self.grad.at[0, mats, rows_of(kind, quarter), :], self.land.at[mats, i],
                       b["d2d_s"].at[u, i], b["d2d_r"].at[u, i], partner)
                for i, quarter in enumerate((far_other, partner))
            ]

        def load_pair(self, u, chunk, which):
            kind, b = self.kind, self.b
            mat, nmat, row, nrow = chunk
            mats = self.mats(u, mat, nmat)
            quarter, g, d, i = (far_same, "gf", "df", 0) if which == 0 else (me, "gn", "dn", 1)
            return [
                local(self.grad.at[0, mats, rows_of(kind, quarter, row, nrow), :], b[g], b["loc"].at[2 * i]),
                local(self.land.at[mats, i, pl.ds(row, nrow), :], b[d], b["loc"].at[2 * i + 1]),
            ]

        def load_mom(self, u):
            return local(self.mom.at[self.mats(u)], self.b["mo"].at[self.slot(u)], self.b["loc"].at[4])

        def weight(self):
            return self.b["sb"].at[0] if self.kind.single else self.b["w"]

        def load_weight(self, u):
            return local(self.master.at[self.mats(u)], self.weight(), self.b["loc"].at[5])

        def partial_send(self, u):
            b = self.b
            return remote(b["sb"].at[self.slot(u)], self.far_land.at[self.mats(u)], b["rs_s"].at[u], b["rs_r"].at[u], far_same)

        def first_loads(self, u):
            for i, copy in enumerate(self.exchange(u)):
                copy.wait()
            for copy in self.load_pair(u, self.kind.chunks[0], 0):
                copy.start()

        def partial(self, u):
            kind, b = self.kind, self.b
            for index, chunk in enumerate(kind.chunks):
                mat, nmat, row, nrow = chunk
                copies = self.load_pair(u, chunk, 0)
                if index:
                    for copy in copies:
                        copy.start()
                for copy in copies:
                    copy.wait()
                b["sb"][self.slot(u), mat:mat + nmat, row:row + nrow, :] = b["gf"][...] + b["df"][...]

        def partial_start(self, u):
            self.partial_send(u).start()

        def second_loads(self, u):
            for copy in self.load_pair(u, self.kind.chunks[0], 1):
                copy.start()
            self.load_mom(u).start()

        def norm_sends(self, u):
            b = self.b
            return [
                remote(b["nr"].at[u, me], b["nr"].at[u, me], b["nm_s"].at[u, i], b["nm_r"].at[u, i], device)
                for i, device in enumerate((partner, far_same, far_other))
            ]

        def mom_out(self, u):
            return local(self.b["mo"].at[self.slot(u)], self.new_mom.at[self.mats(u)], self.b["loc"].at[7])

        def momentum(self, u):
            kind, b = self.kind, self.b
            slot = self.slot(u)
            self.partial_send(u).wait()
            self.load_mom(u).wait()
            sums = [None] * kind.unit
            for index, chunk in enumerate(kind.chunks):
                mat, nmat, row, nrow = chunk
                far_copy = local(self.far_land.at[self.mats(u, mat, nmat), pl.ds(row, nrow), :], b["xl"], b["loc"].at[6])
                far_copy.start()
                copies = self.load_pair(u, chunk, 1)
                if index:
                    for copy in copies:
                        copy.start()
                for copy in copies:
                    copy.wait()
                far_copy.wait()
                for i in range(nmat):
                    total = (b["gn"][i] + b["dn"][i]) + b["xl"][i]
                    value = MOMENTUM * b["mo"][slot, mat + i, row:row + nrow, :] + total * 0.25
                    b["mo"][slot, mat + i, row:row + nrow, :] = value
                    sq_sum = jnp.sum(jnp.sum(value * value, axis=0, keepdims=True), axis=1, keepdims=True)
                    sums[mat + i] = sq_sum if sums[mat + i] is None else sums[mat + i] + sq_sum
            for i in range(kind.unit):
                b["nr"][u, me, i:i + 1, :] = jnp.broadcast_to(sums[i], (1, 128))
            self.mom_out(u).start()

        def norm_start(self, u):
            for copy in self.norm_sends(u):
                copy.start()

        def start_sends(self, u):
            kind, b = self.kind, self.b
            slot = self.slot(u)
            place = b["xg"].at[u, :, rows_of(kind, me), :]
            if kind.split:
                mine = b["xs"].at[slot, pl.ds(core * kind.half, kind.half)]
                theirs = b["xs"].at[slot, pl.ds(other * kind.half, kind.half)]
                routes = ((theirs, partner), (mine, far_same), (theirs, far_other))
            else:
                routes = ((b["xs"].at[slot], partner), (b["xs"].at[slot], far_same))
            return [remote(src, place, b["x_s"].at[u, i], b["x_r"].at[u, i], device) for i, (src, device) in enumerate(routes)]

        def start_forward(self, u):
            kind, b = self.kind, self.b
            place = b["xg"].at[u, :, rows_of(kind, far_same), :]
            return remote(place, place, b["x_s"].at[u, 2], b["x_r"].at[u, 2], partner)

        def start_matrix(self, u):
            kind, b = self.kind, self.b
            slot = self.slot(u)
            for copy in self.norm_sends(u):
                copy.wait()
            total = ((b["nr"][u, 0] + b["nr"][u, 1]) + b["nr"][u, 2]) + b["nr"][u, 3]
            norm = jnp.sqrt(total) + NORM_EPS
            for i in range(kind.unit):
                b["xs"][slot, i] = (b["mo"][slot, i] / norm[i:i + 1, 0:1]).astype(BF16)
            if kind.split:
                b["xg"][u, :, rows_of(kind, me), :] = b["xs"][slot, pl.ds(core * kind.half, kind.half)]
            else:
                b["xg"][u, :, rows_of(kind, me), :] = b["xs"][slot]
            self.mom_out(u).wait()
            for copy in self.start_sends(u):
                copy.start()

        def ortho_send(self, u):
            kind, b = self.kind, self.b
            return remote(b["xg"].at[u, :, rows_of(kind, partner), :], b["orow"].at[u], b["o_s"].at[u], b["o_r"].at[u], partner)

        def iterate(self, u):
            for copy in self.start_sends(u):
                copy.wait()
            if not self.kind.split:
                forward = self.start_forward(u)
                forward.start()
                forward.wait()
            newton_schulz(self.kind, self.b["xg"], u, gram_acc)

        def iterate_start(self, u):
            if self.kind.split:
                self.ortho_send(u).start()

        def weight_out(self, u):
            return local(self.weight(), self.new_master.at[self.mats(u)], self.b["loc"].at[8])

        def param_out(self, u):
            return local(self.b["pb"], self.param.at[self.mats(u), rows_of(self.kind, me), :], self.b["loc"].at[9])

        def param_sends(self, u):
            kind, b = self.kind, self.b
            place = self.param.at[self.mats(u), rows_of(kind, me), :]
            return [
                remote(b["pb"], place, b["p_s"].at[u, i], b["p_r"].at[u, i], device)
                for i, device in enumerate((partner, far_same))
            ]

        def param_forward(self, u):
            kind, b = self.kind, self.b
            place = self.param.at[self.mats(u), rows_of(kind, far_same), :]
            return remote(place, place, b["p_s"].at[u, 2], b["p_r"].at[u, 2], partner)

        def update(self, u):
            kind, b = self.kind, self.b
            self.load_weight(u).wait()
            weight = self.weight()
            if kind.split:
                self.ortho_send(u).wait()
                parts = ((core * kind.half, lambda j: b["xg"][u, j, rows_of(kind, me), :]),
                         (other * kind.half, lambda j: b["orow"][u, j]))
            else:
                parts = ((0, lambda j: b["xg"][u, j, rows_of(kind, me), :]),)
            for base, ortho in parts:
                for j in range(kind.half):
                    old = weight[base + j]
                    new = old - LEARN_RATE * (kind.scale * ortho(j).astype(F32) + WEIGHT_DECAY * old)
                    weight[base + j] = new
                    b["pb"][base + j] = new.astype(BF16)

        def update_start(self, u):
            self.weight_out(u).start()
            self.param_out(u).start()
            for copy in self.param_sends(u):
                copy.start()

        def forward(self, u):
            self.weight_out(u).wait()
            self.param_out(u).wait()
            for copy in self.param_sends(u):
                copy.wait()
            self.param_forward(u).start()

        def finish(self, u):
            self.param_forward(u).wait()

    stages = [Stage(kind) for kind in kinds]
    bases = {}
    total_units = 0
    for k in ORDER:
        bases[k] = total_units
        total_units += kinds[k].units

    for k in ORDER:
        stage = stages[k]

        def send_all(u, carry, stage=stage):
            for copy in stage.exchange(u):
                copy.start()
            return carry

        lax.fori_loop(0, kinds[k].units, send_all, 0)

    def step(t, carry):
        def run(name, lag):
            for k in ORDER:
                u = t - lag - bases[k]

                @pl.when((u >= 0) & (u < kinds[k].units))
                def _(k=k, u=u):
                    getattr(stages[k], name)(u)

        run("finish", LAGS[6])
        run("forward", LAGS[5])
        run("start_matrix", LAGS[2])
        run("load_weight_start", LAGS[4])
        run("first_loads", LAGS[0])
        run("second_loads", LAGS[1])
        run("iterate", LAGS[3])
        run("update", LAGS[4])
        run("iterate_start", LAGS[3])
        run("update_start", LAGS[4])
        run("momentum", LAGS[1])
        run("partial", LAGS[0])
        run("norm_start", LAGS[1])
        run("partial_start", LAGS[0])
        return carry

    Stage.load_weight_start = lambda self, u: self.load_weight(u).start()
    lax.fori_loop(0, total_units + LAGS[-1], step, 0)


def solution(mesh):
    def local_step(*arrays):
        num = len(arrays) // 3
        kinds = [Kind(k, *arrays[k].shape[1:]) for k in range(num)]
        scratch = [kind.scratch() for kind in kinds]
        names = [tuple(shapes) for shapes in scratch]
        flat = [shape for shapes in scratch for shape in shapes.values()]
        flat.append(pltpu.VMEM((kinds[1].rows, kinds[1].rows), F32))
        row_shapes = [jax.ShapeDtypeStruct((kind.count, kind.quarter, kind.cols), F32) for kind in kinds]
        full_shapes = [jax.ShapeDtypeStruct((kind.count, kind.rows, kind.cols), BF16) for kind in kinds]
        land_shapes = [jax.ShapeDtypeStruct((kind.count, 2, kind.quarter, kind.cols), F32) for kind in kinds]
        outs = pl.pallas_call(
            functools.partial(kernel, kinds, names),
            out_shape=row_shapes + row_shapes + full_shapes + land_shapes + row_shapes,
            in_specs=[pl.BlockSpec(memory_space=pl.ANY)] * (3 * num),
            out_specs=[pl.BlockSpec(memory_space=pl.ANY)] * (5 * num),
            scratch_shapes=flat,
            compiler_params=pltpu.CompilerParams(
                collective_id=0, has_side_effects=True, vmem_limit_bytes=67043328
            ),
        )(*arrays)
        return tuple(outs[:3 * num])

    grad_spec = P(("stage", "data"), None, None, None)
    row_spec = P("stage", "data", None)
    full_spec = P("stage", None, None)
    in_specs = (grad_spec,) * 5 + (row_spec,) * 10
    out_specs = (row_spec,) * 10 + (full_spec,) * 5
    return jax.shard_map(local_step, mesh=mesh, in_specs=in_specs, out_specs=out_specs, check_vma=False)
```

```python
import functools
import math
import jax
import jax.numpy as jnp
from jax import lax
from jax.experimental import pallas as pl
from jax.experimental.pallas import tpu as pltpu
from jax.sharding import PartitionSpec as P

NS_STEPS = 5
MOMENTUM = 0.95
LEARN_RATE = 0.2
WEIGHT_DECAY = 0.25
NORM_EPS = 1e-7
COEF_A = 3.4445
COEF_B = -4.7750
COEF_C = 2.0315
F32 = jnp.float32
BF16 = jnp.bfloat16

UNIT_MATS = (2, 2, 1, 4, 4)
ORDER = (3, 2, 1, 0, 4)
LAGS = (0, 2, 3, 4, 5, 6, 7, 8)
SCHEDULE = (
    ("close", 7), ("finish", 6), ("forward", 5), ("combine", 1), ("start_matrix", 2),
    ("load_weight_start", 4), ("first_loads", 0), ("second_loads", 1),
    ("start_start", 2), ("combine_start", 1),
    ("iterate", 3), ("update", 4), ("iterate_start", 3), ("update_start", 4),
    ("momentum", 1), ("partial", 0), ("norm_start", 1), ("partial_start", 0),
)


class Kind:
    def __init__(self, index, count, rows, cols):
        self.index = index
        self.scale = 0.2 * math.sqrt(max(rows, cols))
        self.flip = index in (2, 3)
        if self.flip:
            rows, cols = cols, rows
        self.lanes = index == 3
        self.count, self.rows, self.cols = count, rows, cols
        self.q_rows, self.q_cols = (rows, cols // 4) if self.flip else (rows // 4, cols)
        self.unit = UNIT_MATS[index]
        self.units = count // self.unit
        self.split = self.unit % 2 == 0
        self.half = self.unit // 2 if self.split else self.unit
        self.single = self.units == 1
        if index == 1:
            self.chunks = [(0, 1, 0, self.q_rows), (1, 1, 0, self.q_rows)]
        elif index == 2:
            step = self.q_rows // 2
            self.chunks = [(0, 1, 0, step), (0, 1, step, step)]
        else:
            self.chunks = [(0, self.unit, 0, self.q_rows)]

    def sems(self):
        shapes = {name: pltpu.SemaphoreType.DMA((self.units, 3)) for name in (
            "d2d_s", "d2d_r", "rs_s", "rs_r", "nm_s", "nm_r", "x_s", "x_r", "o_s", "o_r", "p_s", "p_r", "t_s", "t_r")}
        shapes["loc"] = pltpu.SemaphoreType.DMA((10,))
        return shapes

    def scratch(self):
        if self.lanes:
            return self.lane_scratch()
        unit, q_rows, q_cols = self.unit, self.q_rows, self.q_cols
        slots = 1 if self.single else 2
        _, cmats, _, crows = self.chunks[0]
        chunk = pltpu.VMEM((cmats, crows, q_cols), F32)
        shapes = dict(
            gf=chunk, df=chunk, xl=chunk,
            mo=pltpu.VMEM((slots, unit, q_rows, q_cols), F32),
            sb=pltpu.VMEM((slots, unit, q_rows, q_cols), F32),
            xs=pltpu.VMEM((slots, unit, q_rows, q_cols), BF16),
            xg=pltpu.VMEM((self.units, self.half, self.rows, self.cols), BF16),
            nr=pltpu.VMEM((self.units, 4, 8, 128), F32),
        )
        if not self.single:
            shapes["gn"] = chunk
            shapes["dn"] = chunk
            shapes["w"] = pltpu.VMEM((unit, q_rows, q_cols), F32)
            shapes["pb"] = pltpu.VMEM((unit, q_rows, q_cols), BF16)
        if self.split:
            shapes["orow"] = pltpu.VMEM((self.units, self.half, q_rows, q_cols), BF16)
        shapes.update(self.sems())
        return shapes

    def lane_scratch(self):
        unit, half, rows, cols, lanes, units = self.unit, self.half, self.rows, self.cols, self.q_cols, self.units
        shapes = dict(
            gf=pltpu.VMEM((half, rows, cols), F32),
            df=pltpu.VMEM((half, rows, cols), F32),
            sb=pltpu.VMEM((2, 7, rows // 2, 128), F32),
            nb=pltpu.VMEM((2, 2, half, rows, lanes), F32),
            xl=pltpu.VMEM((7, rows // 2, 128), F32),
            tq=pltpu.VMEM((half, rows, lanes), F32),
            tr=pltpu.VMEM((units, half, rows, lanes), F32),
            mo=pltpu.VMEM((2, unit, rows, lanes), F32),
            w=pltpu.VMEM((unit, rows, lanes), F32),
            xs=pltpu.VMEM((2, unit, rows, 128), BF16),
            xp=pltpu.VMEM((2, 2, 7, rows // 4, 128), BF16),
            xq=pltpu.VMEM((units, 2, 7, rows // 4, 128), BF16),
            xg=pltpu.VMEM((units, half, rows, 512), BF16),
            orow=pltpu.VMEM((units, half, rows, 128), BF16),
            pb=pltpu.VMEM((unit, rows, lanes), BF16),
            pk=pltpu.VMEM((7, rows // 2, 128), BF16),
            pv=pltpu.VMEM((4, 7, rows // 2, 128), BF16),
            pa=pltpu.VMEM((unit, rows, cols), BF16),
            nr=pltpu.VMEM((units, 4, 8, 128), F32),
        )
        shapes.update(self.sems())
        return shapes


def pack(pieces):
    last = pieces[7]
    return [jnp.concatenate([pieces[g], last[:, 16 * g:16 * g + 16]], axis=1) for g in range(7)]


def unpack(blocks):
    return [block[:, :112] for block in blocks] + [jnp.concatenate([block[:, 112:128] for block in blocks], axis=1)]


def dot(left, right, dims):
    return lax.dot_general(left, right, (dims, ((), ())), preferred_element_type=F32)


def newton_schulz(kind, xg, u, gram_acc):
    cols = kind.cols

    def poly(gram_mat):
        square = dot(gram_mat, gram_mat, ((1,), (0,)))
        return (COEF_B * gram_mat.astype(F32) + COEF_C * square).astype(BF16)

    if kind.single:
        block = 512

        def iteration(_, carry):
            gram_acc[...] = jnp.zeros_like(gram_acc)

            def add(b, c):
                part = xg[u, 0, :, pl.ds(pl.multiple_of(b * block, block), block)]
                gram_acc[...] += dot(part, part, ((1,), (1,)))
                return c

            lax.fori_loop(0, cols // block, add, 0)
            poly_mat = poly(gram_acc[...].astype(BF16))

            def apply(b, c):
                cut = pl.ds(pl.multiple_of(b * block, block), block)
                part = xg[u, 0, :, cut]
                update = dot(poly_mat, part, ((1,), (0,)))
                xg[u, 0, :, cut] = (COEF_A * part.astype(F32) + update).astype(BF16)
                return c

            lax.fori_loop(0, cols // block, apply, 0)
            return carry
    else:

        def iteration(_, carry):
            for j in range(kind.half):
                mat = xg[u, j]
                gram_mat = dot(mat, mat, ((1,), (1,))).astype(BF16)
                update = dot(poly(gram_mat), mat, ((1,), (0,)))
                xg[u, j] = (COEF_A * mat.astype(F32) + update).astype(BF16)
            return carry

    lax.fori_loop(0, NS_STEPS, iteration, 0)


def kernel(kinds, names, *refs):
    num = len(kinds)
    grads, moms, masters = refs[:num], refs[num:2 * num], refs[2 * num:3 * num]
    outs = refs[3 * num:8 * num]
    new_moms, new_masters, params, lands, far_lands = [outs[i * num:(i + 1) * num] for i in range(5)]
    param_land = refs[8 * num]
    rest = list(refs[8 * num + 1:])
    bufs = []
    for k in range(num):
        bufs.append({name: rest.pop(0) for name in names[k]})
    gram_acc = rest.pop(0)

    me = lax.axis_index("data")
    chip, core = me // 2, me % 2
    far, other = 1 - chip, 1 - core
    partner, far_same, far_other = 2 * chip + other, 2 * far + core, 2 * far + other

    def to(device):
        return dict(device_id={"data": device}, device_id_type=pl.DeviceIdType.MESH)

    def remote(src, dst, send, recv, device):
        return pltpu.make_async_remote_copy(src_ref=src, dst_ref=dst, send_sem=send, recv_sem=recv, **to(device))

    def local(src, dst, sem):
        return pltpu.make_async_copy(src, dst, sem)

    barrier = pltpu.get_barrier_semaphore()
    for device in (partner, far_same, far_other):
        pl.semaphore_signal(barrier, inc=1, **to(device))
    pl.semaphore_wait(barrier, 3)

    def block_of(kind, device, row=0, nrow=None):
        nrow = kind.q_rows if nrow is None else nrow
        if kind.flip:
            return pl.ds(row, nrow), pl.ds(pl.multiple_of(device * kind.q_cols, 128), kind.q_cols)
        return pl.ds(pl.multiple_of(device * kind.q_rows + row, 16), nrow), slice(None)

    class Stage:
        def __init__(self, kind):
            self.kind = kind
            self.b = bufs[kind.index]
            self.grad, self.mom, self.master = grads[kind.index], moms[kind.index], masters[kind.index]
            self.new_mom, self.new_master, self.param = new_moms[kind.index], new_masters[kind.index], params[kind.index]
            self.land, self.far_land = lands[kind.index], far_lands[kind.index]
            self.param_land = param_land

        def mats(self, u, offset=0, size=None):
            kind = self.kind
            return pl.ds(u * kind.unit + offset, kind.unit if size is None else size)

        def slot(self, u):
            return 0 if self.kind.single else u % 2

        def exchange(self, u):
            kind, b = self.kind, self.b
            mats = self.mats(u)
            return [
                remote(self.grad.at[(0, mats) + block_of(kind, quarter)], self.land.at[mats, i],
                       b["d2d_s"].at[u, i], b["d2d_r"].at[u, i], partner)
                for i, quarter in enumerate((far_other, partner))
            ]

        def load_pair(self, u, chunk, which):
            kind, b = self.kind, self.b
            mat, nmat, row, nrow = chunk
            mats = self.mats(u, mat, nmat)
            quarter, g, d, i = (far_same, "gf", "df", 0) if which == 0 else (me,) + (("gf", "df") if kind.single else ("gn", "dn")) + (1,)
            return [
                local(self.grad.at[(0, mats) + block_of(kind, quarter, row, nrow)], b[g], b["loc"].at[2 * i]),
                local(self.land.at[mats, i, pl.ds(row, nrow), :], b[d], b["loc"].at[2 * i + 1]),
            ]

        def load_mom(self, u):
            return local(self.mom.at[self.mats(u)], self.b["mo"].at[self.slot(u)], self.b["loc"].at[4])

        def weight(self):
            return self.b["sb"].at[0] if self.kind.single else self.b["w"]

        def rounded(self):
            return self.b["xs"].at[0] if self.kind.single else self.b["pb"]

        def load_weight(self, u):
            return local(self.master.at[self.mats(u)], self.weight(), self.b["loc"].at[5])

        def partial_send(self, u):
            b = self.b
            return remote(b["sb"].at[self.slot(u)], self.far_land.at[self.mats(u)], b["rs_s"].at[u, 0], b["rs_r"].at[u, 0], far_same)

        def first_loads(self, u):
            for i, copy in enumerate(self.exchange(u)):
                copy.wait()
            for copy in self.load_pair(u, self.kind.chunks[0], 0):
                copy.start()

        def partial(self, u):
            kind, b = self.kind, self.b
            for index, chunk in enumerate(kind.chunks):
                mat, nmat, row, nrow = chunk
                copies = self.load_pair(u, chunk, 0)
                if index:
                    for copy in copies:
                        copy.start()
                for copy in copies:
                    copy.wait()
                b["sb"][self.slot(u), mat:mat + nmat, row:row + nrow, :] = b["gf"][...] + b["df"][...]

        def partial_start(self, u):
            self.partial_send(u).start()

        def second_loads(self, u):
            for copy in self.load_pair(u, self.kind.chunks[0], 1):
                copy.start()
            self.load_mom(u).start()

        def norm_sends(self, u):
            b = self.b
            return [
                remote(b["nr"].at[u, me], b["nr"].at[u, me], b["nm_s"].at[u, i], b["nm_r"].at[u, i], device)
                for i, device in enumerate((partner, far_same, far_other))
            ]

        def mom_out(self, u):
            return local(self.b["mo"].at[self.slot(u)], self.new_mom.at[self.mats(u)], self.b["loc"].at[7])

        def momentum(self, u):
            kind, b = self.kind, self.b
            slot = self.slot(u)
            self.partial_send(u).wait()
            self.load_mom(u).wait()
            near_g, near_d = ("gf", "df") if kind.single else ("gn", "dn")
            sums = [None] * kind.unit
            for index, chunk in enumerate(kind.chunks):
                mat, nmat, row, nrow = chunk
                far_copy = local(self.far_land.at[self.mats(u, mat, nmat), pl.ds(row, nrow), :], b["xl"], b["loc"].at[6])
                far_copy.start()
                copies = self.load_pair(u, chunk, 1)
                if index:
                    for copy in copies:
                        copy.start()
                for copy in copies:
                    copy.wait()
                far_copy.wait()
                for i in range(nmat):
                    total = (b[near_g][i] + b[near_d][i]) + b["xl"][i]
                    value = MOMENTUM * b["mo"][slot, mat + i, row:row + nrow, :] + total * 0.25
                    b["mo"][slot, mat + i, row:row + nrow, :] = value
                    sq_sum = jnp.sum(jnp.sum(value * value, axis=0, keepdims=True), axis=1, keepdims=True)
                    sums[mat + i] = sq_sum if sums[mat + i] is None else sums[mat + i] + sq_sum
            for i in range(kind.unit):
                b["nr"][u, me, i:i + 1, :] = jnp.broadcast_to(sums[i], (1, 128))
            self.mom_out(u).start()

        def norm_start(self, u):
            for copy in self.norm_sends(u):
                copy.start()

        def start_sends(self, u):
            kind, b = self.kind, self.b
            slot = self.slot(u)
            place = b["xg"].at[(u, slice(None)) + block_of(kind, me)]
            if kind.split:
                mine = b["xs"].at[slot, pl.ds(core * kind.half, kind.half)]
                theirs = b["xs"].at[slot, pl.ds(other * kind.half, kind.half)]
                routes = ((theirs, partner), (mine, far_same), (theirs, far_other))
            else:
                routes = ((b["xs"].at[slot], partner), (b["xs"].at[slot], far_same))
            return [remote(src, place, b["x_s"].at[u, i], b["x_r"].at[u, i], device) for i, (src, device) in enumerate(routes)]

        def start_forward(self, u):
            kind, b = self.kind, self.b
            place = b["xg"].at[(u, slice(None)) + block_of(kind, far_same)]
            return remote(place, place, b["x_s"].at[u, 2], b["x_r"].at[u, 2], partner)

        def start_matrix(self, u):
            kind, b = self.kind, self.b
            slot = self.slot(u)
            for copy in self.norm_sends(u):
                copy.wait()
            total = ((b["nr"][u, 0] + b["nr"][u, 1]) + b["nr"][u, 2]) + b["nr"][u, 3]
            norm = jnp.sqrt(total) + NORM_EPS
            for i in range(kind.unit):
                b["xs"][slot, i] = (b["mo"][slot, i] / norm[i:i + 1, 0:1]).astype(BF16)
            if kind.split:
                b["xg"][(u, slice(None)) + block_of(kind, me)] = b["xs"][slot, pl.ds(core * kind.half, kind.half)]
            else:
                b["xg"][(u, slice(None)) + block_of(kind, me)] = b["xs"][slot]
            self.mom_out(u).wait()

        def start_start(self, u):
            for copy in self.start_sends(u):
                copy.start()

        def ortho_send(self, u):
            kind, b = self.kind, self.b
            return remote(b["xg"].at[(u, slice(None)) + block_of(kind, partner)], b["orow"].at[u], b["o_s"].at[u, 0], b["o_r"].at[u, 0], partner)

        def iterate(self, u):
            for copy in self.start_sends(u):
                copy.wait()
            if not self.kind.split:
                forward = self.start_forward(u)
                forward.start()
                forward.wait()
            newton_schulz(self.kind, self.b["xg"], u, gram_acc)

        def iterate_start(self, u):
            if self.kind.split:
                self.ortho_send(u).start()

        def weight_out(self, u):
            return local(self.weight(), self.new_master.at[self.mats(u)], self.b["loc"].at[8])

        def param_out(self, u):
            return local(self.rounded(), self.param.at[(self.mats(u),) + block_of(self.kind, me)], self.b["loc"].at[9])

        def param_sends(self, u):
            kind, b = self.kind, self.b
            place = self.param.at[(self.mats(u),) + block_of(kind, me)]
            return [
                remote(self.rounded(), place, b["p_s"].at[u, i], b["p_r"].at[u, i], device)
                for i, device in enumerate((partner, far_same))
            ]

        def param_forward(self, u):
            kind, b = self.kind, self.b
            place = self.param.at[(self.mats(u),) + block_of(kind, far_same)]
            return remote(place, place, b["p_s"].at[u, 2], b["p_r"].at[u, 2], partner)

        def update(self, u):
            kind, b = self.kind, self.b
            self.load_weight(u).wait()
            weight = self.weight()
            if kind.split:
                self.ortho_send(u).wait()
                parts = ((core * kind.half, lambda j: b["xg"][(u, j) + block_of(kind, me)]),
                         (other * kind.half, lambda j: b["orow"][u, j]))
            else:
                parts = ((0, lambda j: b["xg"][(u, j) + block_of(kind, me)]),)
            for base, ortho in parts:
                for j in range(kind.half):
                    old = weight[base + j]
                    new = old - LEARN_RATE * (kind.scale * ortho(j).astype(F32) + WEIGHT_DECAY * old)
                    weight[base + j] = new
                    self.rounded()[base + j] = new.astype(BF16)

        def update_start(self, u):
            self.weight_out(u).start()
            self.param_out(u).start()
            for copy in self.param_sends(u):
                copy.start()

        def forward(self, u):
            self.weight_out(u).wait()
            self.param_out(u).wait()
            for copy in self.param_sends(u):
                copy.wait()
            self.param_forward(u).start()

        def finish(self, u):
            self.param_forward(u).wait()

        def load_weight_start(self, u):
            self.load_weight(u).start()

    class LaneStage(Stage):
        def exchange(self, u):
            b = self.b
            half = self.kind.half
            src = self.grad.at[0, pl.ds(u * self.kind.unit + other * half, half)]
            return [remote(src, self.land.at[pl.ds(u * half, half)], b["d2d_s"].at[u, 0], b["d2d_r"].at[u, 0], partner)]

        def own_loads(self, u):
            b = self.b
            half = self.kind.half
            return [local(self.grad.at[0, pl.ds(u * self.kind.unit + core * half, half)], b["gf"], b["loc"].at[0]),
                    local(self.land.at[pl.ds(u * half, half)], b["df"], b["loc"].at[1])]

        def first_loads(self, u):
            for copy in self.exchange(u):
                copy.wait()
            for copy in self.own_loads(u):
                copy.start()

        def partial(self, u):
            kind, b = self.kind, self.b
            slot = self.slot(u)
            for copy in self.own_loads(u):
                copy.wait()
            cut = kind.rows // 2

            def far_piece(i, j, r):
                both = b["gf"][i, r * cut:(r + 1) * cut, :] + b["df"][i, r * cut:(r + 1) * cut, :]
                quarters = [both[:, 112 * d:112 * (d + 1)] for d in range(4)]
                if j == 0:
                    near = [jnp.where(chip == 0, quarters[d], quarters[2 + d]) for d in range(2)]
                    b["nb"][slot, 0, i, r * cut:(r + 1) * cut, :] = jnp.where(core == 0, near[0], near[1])
                    b["nb"][slot, 1, i, r * cut:(r + 1) * cut, :] = jnp.where(core == 0, near[1], near[0])
                return jnp.where(chip == 0, quarters[2 + j], quarters[j])

            last = far_piece(1, 1, 1)
            for g in range(7):
                piece = far_piece(g // 4, g // 2 % 2, g % 2)
                b["sb"][slot, g] = jnp.concatenate([piece, last[:, 16 * g:16 * g + 16]], axis=1)

        def partial_send(self, u):
            b = self.b
            return remote(b["sb"].at[self.slot(u)], self.far_land.at[u], b["rs_s"].at[u, 0], b["rs_r"].at[u, 0], far_same)

        def second_loads(self, u):
            self.load_mom(u).start()

        def combine(self, u):
            kind, b = self.kind, self.b
            slot = self.slot(u)
            self.partial_send(u).wait()
            copy = local(self.far_land.at[u], b["xl"], b["loc"].at[6])
            copy.start()
            copy.wait()
            cut = kind.rows // 2
            for i in range(kind.half):
                for r in range(2):
                    rows = slice(r * cut, (r + 1) * cut)
                    first = b["xl"][i * 4 + r][:, :112]
                    if i * 4 + 2 + r < 7:
                        second = b["xl"][i * 4 + 2 + r][:, :112]
                    else:
                        second = jnp.concatenate([b["xl"][g][:, 112:128] for g in range(7)], axis=1)
                    b["nb"][slot, 0, i, rows, :] = b["nb"][slot, 0, i, rows, :] + jnp.where(core == 0, first, second)
                    b["tq"][i, rows, :] = b["nb"][slot, 1, i, rows, :] + jnp.where(core == 0, second, first)

        def total_send(self, u):
            b = self.b
            return remote(b["tq"], b["tr"].at[u], b["t_s"].at[u, 0], b["t_r"].at[u, 0], partner)

        def combine_start(self, u):
            self.total_send(u).start()

        def momentum(self, u):
            kind, b = self.kind, self.b
            slot = self.slot(u)
            self.load_mom(u).wait()
            self.total_send(u).wait()
            for base, total in ((core * kind.half, lambda i: b["nb"][slot, 0, i]), (other * kind.half, lambda i: b["tr"][u, i])):
                for i in range(kind.half):
                    value = MOMENTUM * b["mo"][slot, base + i] + total(i) * 0.25
                    b["mo"][slot, base + i] = value
                    sq_sum = jnp.sum(jnp.sum(value * value, axis=0, keepdims=True), axis=1, keepdims=True)
                    b["nr"][u, me, pl.ds(base + i, 1), :] = jnp.broadcast_to(sq_sum, (1, 128))
            self.mom_out(u).start()

        def lane_block(self, device):
            return pl.ds(pl.multiple_of(device * 128, 128), 128)

        def start_sends(self, u):
            kind, b = self.kind, self.b
            slot = self.slot(u)
            routes = (
                (b["xs"].at[slot, pl.ds(other * kind.half, kind.half)], b["xg"].at[u, :, :, self.lane_block(me)], partner),
                (b["xp"].at[slot, 0], b["xq"].at[u, 0], far_same),
                (b["xp"].at[slot, 1], b["xq"].at[u, 1], far_other),
            )
            return [remote(src, dst, b["x_s"].at[u, i], b["x_r"].at[u, i], device) for i, (src, dst, device) in enumerate(routes)]

        def start_matrix(self, u):
            kind, b = self.kind, self.b
            slot = self.slot(u)
            for copy in self.norm_sends(u):
                copy.wait()
            total = ((b["nr"][u, 0] + b["nr"][u, 1]) + b["nr"][u, 2]) + b["nr"][u, 3]
            norm = jnp.sqrt(total) + NORM_EPS
            pad = jnp.zeros((kind.rows, 16), F32)
            for i in range(kind.unit):
                start = b["mo"][slot, i] / norm[i:i + 1, 0:1]
                b["xs"][slot, i] = jnp.concatenate([start, pad], axis=1).astype(BF16)
            b["xg"][u, :, :, self.lane_block(me)] = b["xs"][slot, pl.ds(core * kind.half, kind.half)]
            cut = kind.rows // 4
            for h, base in enumerate((core * kind.half, other * kind.half)):
                pieces = [b["xs"][slot, base + g // 4, g % 4 * cut:(g % 4 + 1) * cut, :].astype(F32)[:, :112] for g in range(8)]
                for g, block in enumerate(pack(pieces)):
                    b["xp"][slot, h, g] = block.astype(BF16)
            self.mom_out(u).wait()

        def iterate(self, u):
            kind, b = self.kind, self.b
            for copy in self.start_sends(u):
                copy.wait()
            cut = kind.rows // 4
            pad = jnp.zeros((cut, 16), F32)
            for h, device in enumerate((far_same, far_other)):
                pieces = unpack([b["xq"][u, h, g].astype(F32) for g in range(7)])
                for g, piece in enumerate(pieces):
                    block = jnp.concatenate([piece, pad], axis=1).astype(BF16)
                    b["xg"][u, g // 4, g % 4 * cut:(g % 4 + 1) * cut, self.lane_block(device)] = block
            newton_schulz(kind, b["xg"], u, gram_acc)

        def ortho_send(self, u):
            b = self.b
            return remote(b["xg"].at[u, :, :, self.lane_block(partner)], b["orow"].at[u], b["o_s"].at[u, 0], b["o_r"].at[u, 0], partner)

        def param_out(self, u):
            return local(self.b["pk"], self.param_land.at[u, me], self.b["loc"].at[9])

        def param_sends(self, u):
            b = self.b
            place = self.param_land.at[u, me]
            return [
                remote(b["pk"], place, b["p_s"].at[u, i], b["p_r"].at[u, i], device)
                for i, device in enumerate((partner, far_same))
            ]

        def param_forward(self, u):
            b = self.b
            place = self.param_land.at[u, far_same]
            return remote(place, place, b["p_s"].at[u, 2], b["p_r"].at[u, 2], partner)

        def update(self, u):
            kind, b = self.kind, self.b
            self.load_weight(u).wait()
            self.ortho_send(u).wait()
            weight = b["w"]
            parts = ((core * kind.half, lambda j: b["xg"][u, j, :, self.lane_block(me)]),
                     (other * kind.half, lambda j: b["orow"][u, j]))
            for base, ortho in parts:
                for j in range(kind.half):
                    old = weight[base + j]
                    new = old - LEARN_RATE * (kind.scale * ortho(j).astype(F32)[:, :112] + WEIGHT_DECAY * old)
                    weight[base + j] = new
                    b["pb"][base + j] = new.astype(BF16)
            cut = kind.rows // 2
            pieces = [b["pb"][g // 2, g % 2 * cut:(g % 2 + 1) * cut, :].astype(F32) for g in range(8)]
            for g, block in enumerate(pack(pieces)):
                b["pk"][g] = block.astype(BF16)

        def matrix_out(self, u):
            return local(self.b["pa"], self.param.at[self.mats(u)], self.b["loc"].at[2])

        def finish(self, u):
            kind, b = self.kind, self.b
            self.param_forward(u).wait()
            copy = local(self.param_land.at[u], b["pv"], b["loc"].at[3])
            copy.start()
            copy.wait()
            cut = kind.rows // 2
            for g in range(8):
                if g < 7:
                    quarters = [b["pv"][d, g].astype(F32)[:, :112] for d in range(4)]
                else:
                    quarters = [unpack([b["pv"][d, k].astype(F32) for k in range(7)])[7] for d in range(4)]
                b["pa"][g // 2, g % 2 * cut:(g % 2 + 1) * cut, :] = jnp.concatenate(quarters, axis=1).astype(BF16)
            self.matrix_out(u).start()

        def close(self, u):
            self.matrix_out(u).wait()

    stages = [LaneStage(kind) if kind.lanes else Stage(kind) for kind in kinds]
    bases = {}
    total_units = 0
    for k in ORDER:
        bases[k] = total_units
        total_units += kinds[k].units

    for k in ORDER:
        stage = stages[k]

        def send_all(u, carry, stage=stage):
            for copy in stage.exchange(u):
                copy.start()
            return carry

        lax.fori_loop(0, kinds[k].units, send_all, 0)

    def step(t, carry):
        def run(name, lag):
            for k in ORDER:
                method = getattr(stages[k], name, None)
                if method is None:
                    continue
                u = t - lag - bases[k]

                @pl.when((u >= 0) & (u < kinds[k].units))
                def _(method=method, u=u):
                    method(u)

        for name, lag in SCHEDULE:
            run(name, LAGS[lag])
        return carry

    lax.fori_loop(0, total_units + LAGS[-1], step, 0)


def solution(mesh):
    def local_step(*arrays):
        num = len(arrays) // 3
        kinds = [Kind(k, *arrays[k].shape[1:]) for k in range(num)]
        scratch = [kind.scratch() for kind in kinds]
        names = [tuple(shapes) for shapes in scratch]
        flat = [shape for shapes in scratch for shape in shapes.values()]
        flat.append(pltpu.VMEM((kinds[1].rows, kinds[1].rows), F32))
        row_shapes = [jax.ShapeDtypeStruct((kind.count, kind.q_rows, kind.q_cols), F32) for kind in kinds]
        full_shapes = [jax.ShapeDtypeStruct((kind.count, kind.rows, kind.cols), BF16) for kind in kinds]
        land_shapes = [jax.ShapeDtypeStruct((kind.count, 2, kind.q_rows, kind.q_cols), F32) for kind in kinds]
        far_shapes = list(row_shapes)
        lane = kinds[3]
        land_shapes[3] = jax.ShapeDtypeStruct((lane.count // 2, lane.rows, lane.cols), F32)
        far_shapes[3] = jax.ShapeDtypeStruct((lane.units, 7, lane.rows // 2, 128), F32)
        param_shape = jax.ShapeDtypeStruct((lane.units, 4, 7, lane.rows // 2, 128), BF16)
        flipped = [jnp.swapaxes(array, -1, -2) if kinds[i % num].flip else array for i, array in enumerate(arrays)]
        outs = pl.pallas_call(
            functools.partial(kernel, kinds, names),
            out_shape=row_shapes + row_shapes + full_shapes + land_shapes + far_shapes + [param_shape],
            in_specs=[pl.BlockSpec(memory_space=pl.ANY)] * (3 * num),
            out_specs=[pl.BlockSpec(memory_space=pl.ANY)] * (5 * num + 1),
            scratch_shapes=flat,
            compiler_params=pltpu.CompilerParams(
                collective_id=0, has_side_effects=True, vmem_limit_bytes=67043328
            ),
        )(*flipped)
        return tuple(jnp.swapaxes(array, -1, -2) if kinds[i % num].flip else array for i, array in enumerate(outs[:3 * num]))

    grad_spec = P(("stage", "data"), None, None, None)
    row_spec = P("stage", "data", None)
    full_spec = P("stage", None, None)
    in_specs = (grad_spec,) * 5 + (row_spec,) * 10
    out_specs = (row_spec,) * 10 + (full_spec,) * 5
    return jax.shard_map(local_step, mesh=mesh, in_specs=in_specs, out_specs=out_specs, check_vma=False)
```

```python
import functools
import math
import jax
import jax.numpy as jnp
from jax import lax
from jax.experimental import pallas as pl
from jax.experimental.pallas import tpu as pltpu
from jax.sharding import PartitionSpec as P

NS_STEPS = 5
MOMENTUM = 0.95
LEARN_RATE = 0.2
WEIGHT_DECAY = 0.25
NORM_EPS = 1e-7
COEF_A = 3.4445
COEF_B = -4.7750
COEF_C = 2.0315
F32 = jnp.float32
BF16 = jnp.bfloat16

UNIT_MATS = (2, 2, 1, 4, 4)
ORDER = (4, 2, 1, 3, 0)
LAGS = (0, 2, 4, 5, 6, 7, 8, 9)
SCHEDULE = (
    ("combine", 1), ("start_matrix", 2), ("close", 7), ("drain", 5),
    ("load_weight_start", 4), ("first_loads", 0), ("second_loads", 1),
    ("start_start", 2), ("combine_start", 1),
    ("iterate", 3), ("finish", 6), ("forward", 5), ("update", 4), ("iterate_start", 3), ("update_start", 4),
    ("momentum", 1), ("partial", 0), ("norm_start", 1), ("partial_start", 0),
)


class Kind:
    def __init__(self, index, count, rows, cols):
        self.index = index
        self.scale = 0.2 * math.sqrt(max(rows, cols))
        self.flip = index in (2, 3)
        if self.flip:
            rows, cols = cols, rows
        self.lanes = index == 3
        self.tail = index in (0, 4)
        self.count, self.rows, self.cols = count, rows, cols
        self.q_rows, self.q_cols = (rows, cols // 4) if self.flip else (rows // 4, cols)
        self.unit = UNIT_MATS[index]
        self.units = count // self.unit
        self.split = self.unit % 2 == 0
        self.half = self.unit // 2 if self.split else self.unit
        self.single = self.units == 1
        self.pair = self.unit // 2
        self.half_pair = self.half // 2 if self.tail else 0
        if index == 1:
            self.chunks = [(0, 1, 0, self.q_rows), (1, 1, 0, self.q_rows)]
        elif index == 2:
            step = self.q_rows // 2
            self.chunks = [(0, 1, 0, step), (0, 1, step, step)]
        else:
            self.chunks = [(0, self.unit, 0, self.q_rows)]

    def sems(self):
        shapes = {name: pltpu.SemaphoreType.DMA((self.units, 5)) for name in (
            "d2d_s", "d2d_r", "rs_s", "rs_r", "nm_s", "nm_r", "x_s", "x_r", "o_s", "o_r", "p_s", "p_r", "t_s", "t_r")}
        shapes["loc"] = pltpu.SemaphoreType.DMA((14,))
        return shapes

    def scratch(self):
        if self.lanes:
            return self.lane_scratch()
        unit, q_rows, q_cols = self.unit, self.q_rows, self.q_cols
        slots = 1 if self.single else 2
        _, cmats, _, crows = self.chunks[0]
        chunk = pltpu.VMEM((cmats, crows, q_cols), F32)
        shapes = dict(
            gf=chunk, df=chunk, xl=chunk,
            mo=pltpu.VMEM((slots, unit, q_rows, q_cols), F32),
            sb=pltpu.VMEM((slots, unit, q_rows, q_cols), F32),
            xs=pltpu.VMEM((slots, unit, q_rows, q_cols), BF16),
            xg=pltpu.VMEM((self.units, self.half, self.rows, self.cols), BF16),
            nr=pltpu.VMEM((self.units, 4, 8, 128), F32),
        )
        if not self.single:
            shapes["gn"] = chunk
            shapes["dn"] = chunk
            shapes["w"] = pltpu.VMEM((unit, q_rows, q_cols), F32)
            shapes["pb"] = pltpu.VMEM((unit, q_rows, q_cols), BF16)
        if self.tail:
            shapes["st"] = pltpu.VMEM((slots, self.pair, q_rows, 128), F32)
            shapes["xt"] = pltpu.VMEM((self.pair, q_rows, 128), F32)
            shapes["pst"] = pltpu.VMEM((self.pair, q_rows, 128), BF16)
            shapes["ptq"] = pltpu.VMEM((self.units, self.pair, q_rows, 128), BF16)
            shapes["ptu"] = pltpu.VMEM((unit, q_rows, 64), BF16)
        if self.half_pair:
            shapes["xts"] = pltpu.VMEM((slots, 2, self.half_pair, q_rows, 128), BF16)
            shapes["xtq"] = pltpu.VMEM((self.units, 2, self.half_pair, q_rows, 128), BF16)
        if self.split:
            shapes["orow"] = pltpu.VMEM((self.units, self.half, q_rows, q_cols), BF16)
        shapes.update(self.sems())
        return shapes

    def lane_scratch(self):
        unit, half, rows, cols, lanes, units = self.unit, self.half, self.rows, self.cols, self.q_cols, self.units
        shapes = dict(
            gf=pltpu.VMEM((half, rows, cols), F32),
            df=pltpu.VMEM((half, rows, cols), F32),
            sb=pltpu.VMEM((2, 7, rows // 2, 128), F32),
            nb=pltpu.VMEM((2, 2, half, rows, lanes), F32),
            xl=pltpu.VMEM((7, rows // 2, 128), F32),
            tq=pltpu.VMEM((half, rows, lanes), F32),
            tr=pltpu.VMEM((units, half, rows, lanes), F32),
            mo=pltpu.VMEM((2, unit, rows, lanes), F32),
            w=pltpu.VMEM((unit, rows, lanes), F32),
            xs=pltpu.VMEM((2, unit, rows, 128), BF16),
            xp=pltpu.VMEM((2, 2, 7, rows // 4, 128), BF16),
            xq=pltpu.VMEM((units, 2, 7, rows // 4, 128), BF16),
            xg=pltpu.VMEM((units, half, rows, 512), BF16),
            orow=pltpu.VMEM((units, half, rows, 128), BF16),
            pb=pltpu.VMEM((unit, rows, lanes), BF16),
            pk=pltpu.VMEM((7, rows // 2, 128), BF16),
            pv=pltpu.VMEM((4, 7, rows // 2, 128), BF16),
            pa=pltpu.VMEM((unit, rows, cols), BF16),
            nr=pltpu.VMEM((units, 4, 8, 128), F32),
        )
        shapes.update(self.sems())
        return shapes


def pack(pieces):
    last = pieces[7]
    return [jnp.concatenate([pieces[g], last[:, 16 * g:16 * g + 16]], axis=1) for g in range(7)]


def join(left, right):
    return jnp.concatenate([left[:, 384:448], right[:, 384:448]], axis=1)


def unpack(blocks):
    return [block[:, :112] for block in blocks] + [jnp.concatenate([block[:, 112:128] for block in blocks], axis=1)]


def dot(left, right, dims):
    return lax.dot_general(left, right, (dims, ((), ())), preferred_element_type=F32)


def newton_schulz(kind, xg, u, gram_acc):
    cols = kind.cols

    def poly(gram_mat):
        square = dot(gram_mat, gram_mat, ((1,), (0,)))
        return (COEF_B * gram_mat.astype(F32) + COEF_C * square).astype(BF16)

    if kind.single:
        block = 512

        def iteration(_, carry):
            gram_acc[...] = jnp.zeros_like(gram_acc)

            def add(b, c):
                part = xg[u, 0, :, pl.ds(pl.multiple_of(b * block, block), block)]
                gram_acc[...] += dot(part, part, ((1,), (1,)))
                return c

            lax.fori_loop(0, cols // block, add, 0)
            poly_mat = poly(gram_acc[...].astype(BF16))

            def apply(b, c):
                cut = pl.ds(pl.multiple_of(b * block, block), block)
                part = xg[u, 0, :, cut]
                update = dot(poly_mat, part, ((1,), (0,)))
                xg[u, 0, :, cut] = (COEF_A * part.astype(F32) + update).astype(BF16)
                return c

            lax.fori_loop(0, cols // block, apply, 0)
            return carry
    else:

        def iteration(_, carry):
            for j in range(kind.half):
                mat = xg[u, j]
                gram_mat = dot(mat, mat, ((1,), (1,))).astype(BF16)
                update = dot(poly(gram_mat), mat, ((1,), (0,)))
                xg[u, j] = (COEF_A * mat.astype(F32) + update).astype(BF16)
            return carry

    lax.fori_loop(0, NS_STEPS, iteration, 0)


def kernel(kinds, names, *refs):
    num = len(kinds)
    grads, moms, masters = refs[:num], refs[num:2 * num], refs[2 * num:3 * num]
    outs = refs[3 * num:8 * num]
    new_moms, new_masters, params, lands, far_lands = [outs[i * num:(i + 1) * num] for i in range(5)]
    param_land = refs[8 * num]
    far_tails = {0: refs[8 * num + 1], 4: refs[8 * num + 2]}
    rest = list(refs[8 * num + 3:])
    bufs = []
    for k in range(num):
        bufs.append({name: rest.pop(0) for name in names[k]})
    gram_acc = rest.pop(0)

    me = lax.axis_index("data")
    chip, core = me // 2, me % 2
    far, other = 1 - chip, 1 - core
    partner, far_same, far_other = 2 * chip + other, 2 * far + core, 2 * far + other

    def to(device):
        return dict(device_id={"data": device}, device_id_type=pl.DeviceIdType.MESH)

    def remote(src, dst, send, recv, device):
        return pltpu.make_async_remote_copy(src_ref=src, dst_ref=dst, send_sem=send, recv_sem=recv, **to(device))

    def local(src, dst, sem):
        return pltpu.make_async_copy(src, dst, sem)

    barrier = pltpu.get_barrier_semaphore()
    for device in (partner, far_same, far_other):
        pl.semaphore_signal(barrier, inc=1, **to(device))
    pl.semaphore_wait(barrier, 3)

    def block_of(kind, device, row=0, nrow=None):
        nrow = kind.q_rows if nrow is None else nrow
        if kind.flip:
            return pl.ds(row, nrow), pl.ds(pl.multiple_of(device * kind.q_cols, 128), kind.q_cols)
        return pl.ds(pl.multiple_of(device * kind.q_rows + row, 16), nrow), slice(None)

    class Stage:
        def __init__(self, kind):
            self.kind = kind
            self.b = bufs[kind.index]
            self.grad, self.mom, self.master = grads[kind.index], moms[kind.index], masters[kind.index]
            self.new_mom, self.new_master, self.param = new_moms[kind.index], new_masters[kind.index], params[kind.index]
            self.land, self.far_land = lands[kind.index], far_lands[kind.index]
            self.param_land = param_land
            self.far_tail = far_tails.get(kind.index)

        def mats(self, u, offset=0, size=None):
            kind = self.kind
            return pl.ds(u * kind.unit + offset, kind.unit if size is None else size)

        def slot(self, u):
            return 0 if self.kind.single else u % 2

        def exchange(self, u):
            kind, b = self.kind, self.b
            mats = self.mats(u)
            return [
                remote(self.grad.at[(0, mats) + block_of(kind, quarter)], self.land.at[mats, i],
                       b["d2d_s"].at[u, i], b["d2d_r"].at[u, i], partner)
                for i, quarter in enumerate((far_other, partner))
            ]

        def load_pair(self, u, chunk, which):
            kind, b = self.kind, self.b
            mat, nmat, row, nrow = chunk
            mats = self.mats(u, mat, nmat)
            quarter, g, d, i = (far_same, "gf", "df", 0) if which == 0 else (me,) + (("gf", "df") if kind.single else ("gn", "dn")) + (1,)
            return [
                local(self.grad.at[(0, mats) + block_of(kind, quarter, row, nrow)], b[g], b["loc"].at[2 * i]),
                local(self.land.at[mats, i, pl.ds(row, nrow), :], b[d], b["loc"].at[2 * i + 1]),
            ]

        def load_mom(self, u):
            return local(self.mom.at[self.mats(u)], self.b["mo"].at[self.slot(u)], self.b["loc"].at[4])

        def weight(self):
            return self.b["sb"].at[0] if self.kind.single else self.b["w"]

        def rounded(self):
            return self.b["xs"].at[0] if self.kind.single else self.b["pb"]

        def load_weight(self, u):
            return local(self.master.at[self.mats(u)], self.weight(), self.b["loc"].at[5])

        def partial_sends(self, u):
            b = self.b
            src, dst = b["sb"].at[self.slot(u)], self.far_land.at[self.mats(u)]
            pairs = [(src, dst)]
            if self.kind.tail:
                pairs = [(b["sb"].at[self.slot(u), :, :, 0:384], self.far_land.at[self.mats(u), :, 0:384]),
                         (b["st"].at[self.slot(u)], self.far_tail.at[u])]
            return [remote(src, dst, b["rs_s"].at[u, i], b["rs_r"].at[u, i], far_same) for i, (src, dst) in enumerate(pairs)]

        def first_loads(self, u):
            for i, copy in enumerate(self.exchange(u)):
                copy.wait()
            for copy in self.load_pair(u, self.kind.chunks[0], 0):
                copy.start()

        def partial(self, u):
            kind, b = self.kind, self.b
            for index, chunk in enumerate(kind.chunks):
                mat, nmat, row, nrow = chunk
                copies = self.load_pair(u, chunk, 0)
                if index:
                    for copy in copies:
                        copy.start()
                for copy in copies:
                    copy.wait()
                b["sb"][self.slot(u), mat:mat + nmat, row:row + nrow, :] = b["gf"][...] + b["df"][...]
            if kind.tail:
                for i in range(kind.pair):
                    b["st"][self.slot(u), i] = join(b["sb"][self.slot(u), i], b["sb"][self.slot(u), i + kind.pair])

        def partial_start(self, u):
            for copy in self.partial_sends(u):
                copy.start()

        def second_loads(self, u):
            for copy in self.load_pair(u, self.kind.chunks[0], 1):
                copy.start()
            self.load_mom(u).start()

        def norm_sends(self, u):
            b = self.b
            return [
                remote(b["nr"].at[u, me], b["nr"].at[u, me], b["nm_s"].at[u, i], b["nm_r"].at[u, i], device)
                for i, device in enumerate((partner, far_same, far_other))
            ]

        def mom_out(self, u):
            return local(self.b["mo"].at[self.slot(u)], self.new_mom.at[self.mats(u)], self.b["loc"].at[12 + self.slot(u)])

        def momentum(self, u):
            kind, b = self.kind, self.b
            slot = self.slot(u)
            for copy in self.partial_sends(u):
                copy.wait()
            self.load_mom(u).wait()
            near_g, near_d = ("gf", "df") if kind.single else ("gn", "dn")
            sums = [None] * kind.unit
            for index, chunk in enumerate(kind.chunks):
                mat, nmat, row, nrow = chunk
                if kind.tail:
                    far_copies = [local(self.far_land.at[self.mats(u), :, 0:384], b["xl"].at[:, :, 0:384], b["loc"].at[6]),
                                  local(self.far_tail.at[u], b["xt"], b["loc"].at[10])]
                else:
                    far_copies = [local(self.far_land.at[self.mats(u, mat, nmat), pl.ds(row, nrow), :], b["xl"], b["loc"].at[6])]
                for copy in far_copies:
                    copy.start()
                copies = self.load_pair(u, chunk, 1)
                if index:
                    for copy in copies:
                        copy.start()
                for copy in copies:
                    copy.wait()
                for copy in far_copies:
                    copy.wait()
                for i in range(nmat):
                    if kind.tail:
                        lane = i // kind.pair * 64
                        cuts = ((slice(0, 384), b["xl"][i, :, 0:384]),
                                (slice(384, 448), b["xt"][i % kind.pair][:, lane:lane + 64]))
                    else:
                        cuts = ((slice(0, kind.q_cols), b["xl"][i]),)
                    for cut, far_sum in cuts:
                        total = (b[near_g][i, :, cut] + b[near_d][i, :, cut]) + far_sum
                        value = MOMENTUM * b["mo"][slot, mat + i, row:row + nrow, cut] + total * 0.25
                        b["mo"][slot, mat + i, row:row + nrow, cut] = value
                        sq_sum = jnp.sum(jnp.sum(value * value, axis=0, keepdims=True), axis=1, keepdims=True)
                        sums[mat + i] = sq_sum if sums[mat + i] is None else sums[mat + i] + sq_sum
            for i in range(kind.unit):
                b["nr"][u, me, i:i + 1, :] = jnp.broadcast_to(sums[i], (1, 128))
            self.mom_out(u).start()

        def norm_start(self, u):
            for copy in self.norm_sends(u):
                copy.start()

        def start_sends(self, u):
            kind, b = self.kind, self.b
            slot = self.slot(u)
            place = b["xg"].at[(u, slice(None)) + block_of(kind, me)]
            if kind.split:
                mine = b["xs"].at[slot, pl.ds(core * kind.half, kind.half)]
                theirs = b["xs"].at[slot, pl.ds(other * kind.half, kind.half)]
                routes = [(theirs, place, partner), (mine, place, far_same), (theirs, place, far_other)]
            else:
                routes = [(b["xs"].at[slot], place, partner), (b["xs"].at[slot], place, far_same)]
            if kind.half_pair:
                main = b["xg"].at[u, :, block_of(kind, me)[0], 0:384]
                for h, base in enumerate((core * kind.half, other * kind.half)):
                    routes[1 + h] = (b["xs"].at[slot, pl.ds(base, kind.half), :, 0:384], main, routes[1 + h][2])
                routes += [(b["xts"].at[slot, h], b["xtq"].at[u, h], device) for h, device in enumerate((far_same, far_other))]
            return [remote(src, dst, b["x_s"].at[u, i], b["x_r"].at[u, i], device) for i, (src, dst, device) in enumerate(routes)]

        def start_forward(self, u):
            kind, b = self.kind, self.b
            place = b["xg"].at[(u, slice(None)) + block_of(kind, far_same)]
            return remote(place, place, b["x_s"].at[u, 2], b["x_r"].at[u, 2], partner)

        def start_matrix(self, u):
            kind, b = self.kind, self.b
            slot = self.slot(u)
            for copy in self.norm_sends(u):
                copy.wait()
            total = ((b["nr"][u, 0] + b["nr"][u, 1]) + b["nr"][u, 2]) + b["nr"][u, 3]
            norm = jnp.sqrt(total) + NORM_EPS
            for i in range(kind.unit):
                b["xs"][slot, i] = (b["mo"][slot, i] / norm[i:i + 1, 0:1]).astype(BF16)
            if kind.split:
                b["xg"][(u, slice(None)) + block_of(kind, me)] = b["xs"][slot, pl.ds(core * kind.half, kind.half)]
            else:
                b["xg"][(u, slice(None)) + block_of(kind, me)] = b["xs"][slot]
            if kind.half_pair:
                for h, base in enumerate((core * kind.half, other * kind.half)):
                    for i in range(kind.half_pair):
                        left = b["xs"][slot, base + i].astype(F32)
                        right = b["xs"][slot, base + i + kind.half_pair].astype(F32)
                        b["xts"][slot, h, i] = join(left, right).astype(BF16)
            self.mom_out(u).wait()

        def start_start(self, u):
            for copy in self.start_sends(u):
                copy.start()

        def ortho_send(self, u):
            kind, b = self.kind, self.b
            return remote(b["xg"].at[(u, slice(None)) + block_of(kind, partner)], b["orow"].at[u], b["o_s"].at[u, 0], b["o_r"].at[u, 0], partner)

        def iterate(self, u):
            for copy in self.start_sends(u):
                copy.wait()
            if not self.kind.split:
                forward = self.start_forward(u)
                forward.start()
                forward.wait()
            if self.kind.half_pair:
                kind, b = self.kind, self.b
                for h, device in enumerate((far_same, far_other)):
                    for i in range(kind.half_pair):
                        both = b["xtq"][u, h, i].astype(F32)
                        for side in range(2):
                            part = both[:, 64 * side:64 * side + 64].astype(BF16)
                            b["xg"][u, i + side * kind.half_pair, block_of(kind, device)[0], 384:448] = part
            newton_schulz(self.kind, self.b["xg"], u, gram_acc)

        def iterate_start(self, u):
            if self.kind.split:
                self.ortho_send(u).start()

        def weight_out(self, u):
            return local(self.weight(), self.new_master.at[self.mats(u)], self.b["loc"].at[8])

        def param_out(self, u):
            return local(self.rounded(), self.param.at[(self.mats(u),) + block_of(self.kind, me)], self.b["loc"].at[9])

        def param_sends(self, u):
            kind, b = self.kind, self.b
            place = self.param.at[(self.mats(u),) + block_of(kind, me)]
            routes = [(self.rounded(), place, partner, 0), (self.rounded(), place, far_same, 1)]
            if kind.tail:
                main = self.param.at[self.mats(u), block_of(kind, me)[0], 0:384]
                routes[1:] = [(b["pb"].at[:, :, 0:384], main, far_same, 1), (b["pst"], b["ptq"].at[u], far_same, 3)]
            return [remote(src, dst, b["p_s"].at[u, i], b["p_r"].at[u, i], device) for src, dst, device, i in routes]

        def param_forwards(self, u):
            kind, b = self.kind, self.b
            place = self.param.at[(self.mats(u),) + block_of(kind, far_same)]
            routes = [(place, place, 2)]
            if kind.tail:
                main = self.param.at[self.mats(u), block_of(kind, far_same)[0], 0:384]
                routes = [(main, main, 2), (b["ptu"], self.tail_place(u), 4)]
            return [remote(src, dst, b["p_s"].at[u, i], b["p_r"].at[u, i], partner) for src, dst, i in routes]

        def tail_place(self, u):
            return self.param.at[self.mats(u), block_of(self.kind, far_same)[0], 384:448]

        def tail_out(self, u):
            return local(self.b["ptu"], self.tail_place(u), self.b["loc"].at[11])

        def update(self, u):
            kind, b = self.kind, self.b
            self.load_weight(u).wait()
            weight = self.weight()
            if kind.split:
                self.ortho_send(u).wait()
                parts = ((core * kind.half, lambda j: b["xg"][(u, j) + block_of(kind, me)]),
                         (other * kind.half, lambda j: b["orow"][u, j]))
            else:
                parts = ((0, lambda j: b["xg"][(u, j) + block_of(kind, me)]),)
            for base, ortho in parts:
                for j in range(kind.half):
                    old = weight[base + j]
                    new = old - LEARN_RATE * (kind.scale * ortho(j).astype(F32) + WEIGHT_DECAY * old)
                    weight[base + j] = new
                    self.rounded()[base + j] = new.astype(BF16)
            if kind.tail:
                for i in range(kind.pair):
                    b["pst"][i] = join(b["pb"][i].astype(F32), b["pb"][i + kind.pair].astype(F32)).astype(BF16)

        def update_start(self, u):
            self.weight_out(u).start()
            self.param_out(u).start()
            for copy in self.param_sends(u):
                copy.start()

        def drain(self, u):
            self.weight_out(u).wait()

        def forward(self, u):
            self.param_out(u).wait()
            for copy in self.param_sends(u):
                copy.wait()
            kind, b = self.kind, self.b
            if kind.tail:
                for i in range(kind.unit):
                    lane = i // kind.pair * 64
                    b["ptu"][i] = b["ptq"][u, i % kind.pair].astype(F32)[:, lane:lane + 64].astype(BF16)
                self.tail_out(u).start()
            for copy in self.param_forwards(u):
                copy.start()

        def finish(self, u):
            if self.kind.tail:
                self.tail_out(u).wait()
            for copy in self.param_forwards(u):
                copy.wait()

        def load_weight_start(self, u):
            self.load_weight(u).start()

    class LaneStage(Stage):
        def exchange(self, u):
            b = self.b
            half = self.kind.half
            src = self.grad.at[0, pl.ds(u * self.kind.unit + other * half, half)]
            return [remote(src, self.land.at[pl.ds(u * half, half)], b["d2d_s"].at[u, 0], b["d2d_r"].at[u, 0], partner)]

        def own_loads(self, u):
            b = self.b
            half = self.kind.half
            return [local(self.grad.at[0, pl.ds(u * self.kind.unit + core * half, half)], b["gf"], b["loc"].at[0]),
                    local(self.land.at[pl.ds(u * half, half)], b["df"], b["loc"].at[1])]

        def first_loads(self, u):
            for copy in self.exchange(u):
                copy.wait()
            for copy in self.own_loads(u):
                copy.start()

        def partial(self, u):
            kind, b = self.kind, self.b
            slot = self.slot(u)
            for copy in self.own_loads(u):
                copy.wait()
            cut = kind.rows // 2

            def far_piece(i, j, r):
                both = b["gf"][i, r * cut:(r + 1) * cut, :] + b["df"][i, r * cut:(r + 1) * cut, :]
                quarters = [both[:, 112 * d:112 * (d + 1)] for d in range(4)]
                if j == 0:
                    near = [jnp.where(chip == 0, quarters[d], quarters[2 + d]) for d in range(2)]
                    b["nb"][slot, 0, i, r * cut:(r + 1) * cut, :] = jnp.where(core == 0, near[0], near[1])
                    b["nb"][slot, 1, i, r * cut:(r + 1) * cut, :] = jnp.where(core == 0, near[1], near[0])
                return jnp.where(chip == 0, quarters[2 + j], quarters[j])

            last = far_piece(1, 1, 1)
            for g in range(7):
                piece = far_piece(g // 4, g // 2 % 2, g % 2)
                b["sb"][slot, g] = jnp.concatenate([piece, last[:, 16 * g:16 * g + 16]], axis=1)

        def partial_sends(self, u):
            b = self.b
            return [remote(b["sb"].at[self.slot(u)], self.far_land.at[u], b["rs_s"].at[u, 0], b["rs_r"].at[u, 0], far_same)]

        def second_loads(self, u):
            self.load_mom(u).start()

        def combine(self, u):
            kind, b = self.kind, self.b
            slot = self.slot(u)
            for copy in self.partial_sends(u):
                copy.wait()
            copy = local(self.far_land.at[u], b["xl"], b["loc"].at[6])
            copy.start()
            copy.wait()
            cut = kind.rows // 2
            for i in range(kind.half):
                for r in range(2):
                    rows = slice(r * cut, (r + 1) * cut)
                    first = b["xl"][i * 4 + r][:, :112]
                    if i * 4 + 2 + r < 7:
                        second = b["xl"][i * 4 + 2 + r][:, :112]
                    else:
                        second = jnp.concatenate([b["xl"][g][:, 112:128] for g in range(7)], axis=1)
                    b["nb"][slot, 0, i, rows, :] = b["nb"][slot, 0, i, rows, :] + jnp.where(core == 0, first, second)
                    b["tq"][i, rows, :] = b["nb"][slot, 1, i, rows, :] + jnp.where(core == 0, second, first)

        def total_send(self, u):
            b = self.b
            return remote(b["tq"], b["tr"].at[u], b["t_s"].at[u, 0], b["t_r"].at[u, 0], partner)

        def combine_start(self, u):
            self.total_send(u).start()

        def momentum(self, u):
            kind, b = self.kind, self.b
            slot = self.slot(u)
            self.load_mom(u).wait()
            self.total_send(u).wait()
            for base, total in ((core * kind.half, lambda i: b["nb"][slot, 0, i]), (other * kind.half, lambda i: b["tr"][u, i])):
                for i in range(kind.half):
                    value = MOMENTUM * b["mo"][slot, base + i] + total(i) * 0.25
                    b["mo"][slot, base + i] = value
                    sq_sum = jnp.sum(jnp.sum(value * value, axis=0, keepdims=True), axis=1, keepdims=True)
                    b["nr"][u, me, pl.ds(base + i, 1), :] = jnp.broadcast_to(sq_sum, (1, 128))
            self.mom_out(u).start()

        def lane_block(self, device):
            return pl.ds(pl.multiple_of(device * 128, 128), 128)

        def start_sends(self, u):
            kind, b = self.kind, self.b
            slot = self.slot(u)
            routes = (
                (b["xs"].at[slot, pl.ds(other * kind.half, kind.half)], b["xg"].at[u, :, :, self.lane_block(me)], partner),
                (b["xp"].at[slot, 0], b["xq"].at[u, 0], far_same),
                (b["xp"].at[slot, 1], b["xq"].at[u, 1], far_other),
            )
            return [remote(src, dst, b["x_s"].at[u, i], b["x_r"].at[u, i], device) for i, (src, dst, device) in enumerate(routes)]

        def start_matrix(self, u):
            kind, b = self.kind, self.b
            slot = self.slot(u)
            for copy in self.norm_sends(u):
                copy.wait()
            total = ((b["nr"][u, 0] + b["nr"][u, 1]) + b["nr"][u, 2]) + b["nr"][u, 3]
            norm = jnp.sqrt(total) + NORM_EPS
            pad = jnp.zeros((kind.rows, 16), F32)
            for i in range(kind.unit):
                start = b["mo"][slot, i] / norm[i:i + 1, 0:1]
                b["xs"][slot, i] = jnp.concatenate([start, pad], axis=1).astype(BF16)
            b["xg"][u, :, :, self.lane_block(me)] = b["xs"][slot, pl.ds(core * kind.half, kind.half)]
            cut = kind.rows // 4
            for h, base in enumerate((core * kind.half, other * kind.half)):
                pieces = [b["xs"][slot, base + g // 4, g % 4 * cut:(g % 4 + 1) * cut, :].astype(F32)[:, :112] for g in range(8)]
                for g, block in enumerate(pack(pieces)):
                    b["xp"][slot, h, g] = block.astype(BF16)
            self.mom_out(u).wait()

        def iterate(self, u):
            kind, b = self.kind, self.b
            for copy in self.start_sends(u):
                copy.wait()
            cut = kind.rows // 4
            pad = jnp.zeros((cut, 16), F32)
            for h, device in enumerate((far_same, far_other)):
                pieces = unpack([b["xq"][u, h, g].astype(F32) for g in range(7)])
                for g, piece in enumerate(pieces):
                    block = jnp.concatenate([piece, pad], axis=1).astype(BF16)
                    b["xg"][u, g // 4, g % 4 * cut:(g % 4 + 1) * cut, self.lane_block(device)] = block
            newton_schulz(kind, b["xg"], u, gram_acc)

        def ortho_send(self, u):
            b = self.b
            return remote(b["xg"].at[u, :, :, self.lane_block(partner)], b["orow"].at[u], b["o_s"].at[u, 0], b["o_r"].at[u, 0], partner)

        def param_out(self, u):
            return local(self.b["pk"], self.param_land.at[u, me], self.b["loc"].at[9])

        def param_sends(self, u):
            b = self.b
            place = self.param_land.at[u, me]
            return [
                remote(b["pk"], place, b["p_s"].at[u, i], b["p_r"].at[u, i], device)
                for i, device in enumerate((partner, far_same))
            ]

        def param_forwards(self, u):
            b = self.b
            place = self.param_land.at[u, far_same]
            return [remote(place, place, b["p_s"].at[u, 2], b["p_r"].at[u, 2], partner)]

        def update(self, u):
            kind, b = self.kind, self.b
            self.load_weight(u).wait()
            self.ortho_send(u).wait()
            weight = b["w"]
            parts = ((core * kind.half, lambda j: b["xg"][u, j, :, self.lane_block(me)]),
                     (other * kind.half, lambda j: b["orow"][u, j]))
            for base, ortho in parts:
                for j in range(kind.half):
                    old = weight[base + j]
                    new = old - LEARN_RATE * (kind.scale * ortho(j).astype(F32)[:, :112] + WEIGHT_DECAY * old)
                    weight[base + j] = new
                    b["pb"][base + j] = new.astype(BF16)
            cut = kind.rows // 2
            pieces = [b["pb"][g // 2, g % 2 * cut:(g % 2 + 1) * cut, :].astype(F32) for g in range(8)]
            for g, block in enumerate(pack(pieces)):
                b["pk"][g] = block.astype(BF16)

        def matrix_out(self, u):
            return local(self.b["pa"], self.param.at[self.mats(u)], self.b["loc"].at[2])

        def finish(self, u):
            kind, b = self.kind, self.b
            for copy in self.param_forwards(u):
                copy.wait()
            copy = local(self.param_land.at[u], b["pv"], b["loc"].at[3])
            copy.start()
            copy.wait()
            cut = kind.rows // 2
            for g in range(8):
                if g < 7:
                    quarters = [b["pv"][d, g].astype(F32)[:, :112] for d in range(4)]
                else:
                    quarters = [unpack([b["pv"][d, k].astype(F32) for k in range(7)])[7] for d in range(4)]
                b["pa"][g // 2, g % 2 * cut:(g % 2 + 1) * cut, :] = jnp.concatenate(quarters, axis=1).astype(BF16)
            self.matrix_out(u).start()

        def close(self, u):
            self.matrix_out(u).wait()

    stages = [LaneStage(kind) if kind.lanes else Stage(kind) for kind in kinds]
    bases = {}
    total_units = 0
    for k in ORDER:
        bases[k] = total_units
        total_units += kinds[k].units

    for k in ORDER:
        stage = stages[k]

        def send_all(u, carry, stage=stage):
            for copy in stage.exchange(u):
                copy.start()
            return carry

        lax.fori_loop(0, kinds[k].units, send_all, 0)

    def step(t, carry):
        def run(name, lag):
            for k in ORDER:
                method = getattr(stages[k], name, None)
                if method is None:
                    continue
                u = t - lag - bases[k]

                @pl.when((u >= 0) & (u < kinds[k].units))
                def _(method=method, u=u):
                    method(u)

        for name, lag in SCHEDULE:
            run(name, LAGS[lag])
        return carry

    lax.fori_loop(0, total_units + LAGS[-1], step, 0)


def solution(mesh):
    def local_step(*arrays):
        num = len(arrays) // 3
        kinds = [Kind(k, *arrays[k].shape[1:]) for k in range(num)]
        scratch = [kind.scratch() for kind in kinds]
        names = [tuple(shapes) for shapes in scratch]
        flat = [shape for shapes in scratch for shape in shapes.values()]
        flat.append(pltpu.VMEM((kinds[1].rows, kinds[1].rows), F32))
        row_shapes = [jax.ShapeDtypeStruct((kind.count, kind.q_rows, kind.q_cols), F32) for kind in kinds]
        full_shapes = [jax.ShapeDtypeStruct((kind.count, kind.rows, kind.cols), BF16) for kind in kinds]
        land_shapes = [jax.ShapeDtypeStruct((kind.count, 2, kind.q_rows, kind.q_cols), F32) for kind in kinds]
        far_shapes = list(row_shapes)
        lane = kinds[3]
        land_shapes[3] = jax.ShapeDtypeStruct((lane.count // 2, lane.rows, lane.cols), F32)
        far_shapes[3] = jax.ShapeDtypeStruct((lane.units, 7, lane.rows // 2, 128), F32)
        param_shape = jax.ShapeDtypeStruct((lane.units, 4, 7, lane.rows // 2, 128), BF16)
        tail_shapes = [jax.ShapeDtypeStruct((kind.units, kind.pair, kind.q_rows, 128), F32) for kind in kinds if kind.tail]
        flipped = [jnp.swapaxes(array, -1, -2) if kinds[i % num].flip else array for i, array in enumerate(arrays)]
        outs = pl.pallas_call(
            functools.partial(kernel, kinds, names),
            out_shape=row_shapes + row_shapes + full_shapes + land_shapes + far_shapes + [param_shape] + tail_shapes,
            in_specs=[pl.BlockSpec(memory_space=pl.ANY)] * (3 * num),
            out_specs=[pl.BlockSpec(memory_space=pl.ANY)] * (5 * num + 3),
            scratch_shapes=flat,
            compiler_params=pltpu.CompilerParams(
                collective_id=0, has_side_effects=True, vmem_limit_bytes=67043328
            ),
        )(*flipped)
        return tuple(jnp.swapaxes(array, -1, -2) if kinds[i % num].flip else array for i, array in enumerate(outs[:3 * num]))

    grad_spec = P(("stage", "data"), None, None, None)
    row_spec = P("stage", "data", None)
    full_spec = P("stage", None, None)
    in_specs = (grad_spec,) * 5 + (row_spec,) * 10
    out_specs = (row_spec,) * 10 + (full_spec,) * 5
    return jax.shard_map(local_step, mesh=mesh, in_specs=in_specs, out_specs=out_specs, check_vma=False)
```

```python
import functools
import math
import jax
import jax.numpy as jnp
from jax import lax
from jax.experimental import pallas as pl
from jax.experimental.pallas import tpu as pltpu
from jax.sharding import PartitionSpec as P

NS_STEPS = 5
MOMENTUM = 0.95
LEARN_RATE = 0.2
WEIGHT_DECAY = 0.25
NORM_EPS = 1e-7
COEF_A = 3.4445
COEF_B = -4.7750
COEF_C = 2.0315
F32 = jnp.float32
BF16 = jnp.bfloat16

UNIT_MATS = (2, 2, 1, 4, 4)
ORDER = (4, 2, 1, 3, 0)
LAGS = (0, 2, 4, 5, 6, 7, 8, 9)
SCHEDULE = (
    ("combine", 1), ("start_matrix", 2), ("close", 7), ("drain", 5),
    ("load_weight_start", 4), ("first_loads", 0), ("second_loads", 1),
    ("start_start", 2), ("combine_start", 1),
    ("iterate", 3), ("finish", 6), ("forward", 5), ("update", 4), ("iterate_start", 3), ("update_start", 4),
    ("momentum", 1), ("partial", 0), ("norm_start", 1), ("partial_start", 0),
)


class Kind:
    def __init__(self, index, count, rows, cols):
        self.index = index
        self.scale = 0.2 * math.sqrt(max(rows, cols))
        self.flip = index in (2, 3)
        if self.flip:
            rows, cols = cols, rows
        self.lanes = index == 3
        self.tail = index in (0, 4)
        self.count, self.rows, self.cols = count, rows, cols
        self.q_rows, self.q_cols = (rows, cols // 4) if self.flip else (rows // 4, cols)
        self.unit = UNIT_MATS[index]
        self.units = count // self.unit
        self.split = self.unit % 2 == 0
        self.half = self.unit // 2 if self.split else self.unit
        self.single = self.units == 1
        self.late = index == 1
        self.pair = self.unit // 2
        self.half_pair = self.half // 2 if self.tail else 0
        if index == 1:
            self.chunks = [(0, 1, 0, self.q_rows), (1, 1, 0, self.q_rows)]
        elif index == 2:
            step = self.q_rows // 2
            self.chunks = [(0, 1, 0, step), (0, 1, step, step)]
        else:
            self.chunks = [(0, self.unit, 0, self.q_rows)]

    def sems(self):
        shapes = {name: pltpu.SemaphoreType.DMA((self.units, 5)) for name in (
            "d2d_s", "d2d_r", "rs_s", "rs_r", "nm_s", "nm_r", "x_s", "x_r", "o_s", "o_r", "p_s", "p_r", "t_s", "t_r")}
        shapes["loc"] = pltpu.SemaphoreType.DMA((14,))
        return shapes

    def scratch(self):
        if self.lanes:
            return self.lane_scratch()
        unit, q_rows, q_cols = self.unit, self.q_rows, self.q_cols
        slots = 1 if self.single else 2
        _, cmats, _, crows = self.chunks[0]
        chunk = pltpu.VMEM((cmats, crows, q_cols), F32)
        shapes = dict(
            gf=chunk, df=chunk, xl=chunk,
            mo=pltpu.VMEM((slots, unit, q_rows, q_cols), F32),
            sb=pltpu.VMEM((slots, unit, q_rows, q_cols), F32),
            xs=pltpu.VMEM((slots, unit, q_rows, q_cols), BF16),
            xg=pltpu.VMEM((self.units, self.half, self.rows, self.cols), BF16),
            nr=pltpu.VMEM((self.units, 4, 8, 128), F32),
        )
        if not self.single:
            shapes["gn"] = chunk
            shapes["dn"] = chunk
            shapes["w"] = pltpu.VMEM((unit, q_rows, q_cols), F32)
            shapes["pb"] = pltpu.VMEM((unit, q_rows, q_cols), BF16)
        if self.tail:
            shapes["st"] = pltpu.VMEM((slots, self.pair, q_rows, 128), F32)
            shapes["xt"] = pltpu.VMEM((self.pair, q_rows, 128), F32)
            shapes["pst"] = pltpu.VMEM((self.pair, q_rows, 128), BF16)
            shapes["ptq"] = pltpu.VMEM((self.units, self.pair, q_rows, 128), BF16)
            shapes["ptu"] = pltpu.VMEM((unit, q_rows, 64), BF16)
        if self.half_pair:
            shapes["xts"] = pltpu.VMEM((slots, 2, self.half_pair, q_rows, 128), BF16)
            shapes["xtq"] = pltpu.VMEM((self.units, 2, self.half_pair, q_rows, 128), BF16)
        if self.split:
            shapes["orow"] = pltpu.VMEM((self.units, self.half, q_rows, q_cols), BF16)
        shapes.update(self.sems())
        return shapes

    def lane_scratch(self):
        unit, half, rows, cols, lanes, units = self.unit, self.half, self.rows, self.cols, self.q_cols, self.units
        shapes = dict(
            gf=pltpu.VMEM((half, rows, cols), F32),
            df=pltpu.VMEM((half, rows, cols), F32),
            sb=pltpu.VMEM((2, 7, rows // 2, 128), F32),
            nb=pltpu.VMEM((2, 2, half, rows, lanes), F32),
            xl=pltpu.VMEM((7, rows // 2, 128), F32),
            tq=pltpu.VMEM((half, rows, lanes), F32),
            tr=pltpu.VMEM((units, half, rows, lanes), F32),
            mo=pltpu.VMEM((2, unit, rows, lanes), F32),
            w=pltpu.VMEM((unit, rows, lanes), F32),
            xs=pltpu.VMEM((2, unit, rows, 128), BF16),
            xp=pltpu.VMEM((2, 2, 7, rows // 4, 128), BF16),
            xq=pltpu.VMEM((units, 2, 7, rows // 4, 128), BF16),
            xg=pltpu.VMEM((units, half, rows, 512), BF16),
            orow=pltpu.VMEM((units, half, rows, 128), BF16),
            pb=pltpu.VMEM((unit, rows, lanes), BF16),
            pk=pltpu.VMEM((7, rows // 2, 128), BF16),
            pv=pltpu.VMEM((4, 7, rows // 2, 128), BF16),
            pa=pltpu.VMEM((unit, rows, cols), BF16),
            nr=pltpu.VMEM((units, 4, 8, 128), F32),
        )
        shapes.update(self.sems())
        return shapes


def pack(pieces):
    last = pieces[7]
    return [jnp.concatenate([pieces[g], last[:, 16 * g:16 * g + 16]], axis=1) for g in range(7)]


def join(left, right):
    return jnp.concatenate([left[:, 384:448], right[:, 384:448]], axis=1)


def unpack(blocks):
    return [block[:, :112] for block in blocks] + [jnp.concatenate([block[:, 112:128] for block in blocks], axis=1)]


def dot(left, right, dims):
    return lax.dot_general(left, right, (dims, ((), ())), preferred_element_type=F32)


def newton_schulz(kind, xg, u, gram_acc):
    cols = kind.cols

    def poly(gram_mat):
        square = dot(gram_mat, gram_mat, ((1,), (0,)))
        return (COEF_B * gram_mat.astype(F32) + COEF_C * square).astype(BF16)

    if kind.single:
        block = 512

        def iteration(_, carry):
            gram_acc[...] = jnp.zeros_like(gram_acc)

            def add(b, c):
                part = xg[u, 0, :, pl.ds(pl.multiple_of(b * block, block), block)]
                gram_acc[...] += dot(part, part, ((1,), (1,)))
                return c

            lax.fori_loop(0, cols // block, add, 0)
            poly_mat = poly(gram_acc[...].astype(BF16))

            def apply(b, c):
                cut = pl.ds(pl.multiple_of(b * block, block), block)
                part = xg[u, 0, :, cut]
                update = dot(poly_mat, part, ((1,), (0,)))
                xg[u, 0, :, cut] = (COEF_A * part.astype(F32) + update).astype(BF16)
                return c

            lax.fori_loop(0, cols // block, apply, 0)
            return carry
    else:

        def iteration(_, carry):
            for j in range(kind.half):
                mat = xg[u, j]
                gram_mat = dot(mat, mat, ((1,), (1,))).astype(BF16)
                update = dot(poly(gram_mat), mat, ((1,), (0,)))
                xg[u, j] = (COEF_A * mat.astype(F32) + update).astype(BF16)
            return carry

    lax.fori_loop(0, NS_STEPS, iteration, 0)


def kernel(kinds, names, *refs):
    num = len(kinds)
    grads, moms, masters = refs[:num], refs[num:2 * num], refs[2 * num:3 * num]
    outs = refs[3 * num:8 * num]
    new_moms, new_masters, params, lands, far_lands = [outs[i * num:(i + 1) * num] for i in range(5)]
    param_land = refs[8 * num]
    far_tails = {0: refs[8 * num + 1], 4: refs[8 * num + 2]}
    rest = list(refs[8 * num + 3:])
    bufs = []
    for k in range(num):
        bufs.append({name: rest.pop(0) for name in names[k]})
    gram_acc = rest.pop(0)

    me = lax.axis_index("data")
    chip, core = me // 2, me % 2
    far, other = 1 - chip, 1 - core
    partner, far_same, far_other = 2 * chip + other, 2 * far + core, 2 * far + other

    def to(device):
        return dict(device_id={"data": device}, device_id_type=pl.DeviceIdType.MESH)

    def remote(src, dst, send, recv, device):
        return pltpu.make_async_remote_copy(src_ref=src, dst_ref=dst, send_sem=send, recv_sem=recv, **to(device))

    def local(src, dst, sem):
        return pltpu.make_async_copy(src, dst, sem)

    barrier = pltpu.get_barrier_semaphore()
    for device in (partner, far_same, far_other):
        pl.semaphore_signal(barrier, inc=1, **to(device))
    pl.semaphore_wait(barrier, 3)

    def block_of(kind, device, row=0, nrow=None):
        nrow = kind.q_rows if nrow is None else nrow
        if kind.flip:
            return pl.ds(row, nrow), pl.ds(pl.multiple_of(device * kind.q_cols, 128), kind.q_cols)
        return pl.ds(pl.multiple_of(device * kind.q_rows + row, 16), nrow), slice(None)

    class Stage:
        def __init__(self, kind):
            self.kind = kind
            self.b = bufs[kind.index]
            self.grad, self.mom, self.master = grads[kind.index], moms[kind.index], masters[kind.index]
            self.new_mom, self.new_master, self.param = new_moms[kind.index], new_masters[kind.index], params[kind.index]
            self.land, self.far_land = lands[kind.index], far_lands[kind.index]
            self.param_land = param_land
            self.far_tail = far_tails.get(kind.index)

        def mats(self, u, offset=0, size=None):
            kind = self.kind
            return pl.ds(u * kind.unit + offset, kind.unit if size is None else size)

        def slot(self, u):
            return 0 if self.kind.single else u % 2

        def exchange(self, u):
            kind, b = self.kind, self.b
            mats = self.mats(u)
            return [
                remote(self.grad.at[(0, mats) + block_of(kind, quarter)], self.land.at[mats, i],
                       b["d2d_s"].at[u, i], b["d2d_r"].at[u, i], partner)
                for i, quarter in enumerate((far_other, partner))
            ]

        def load_pair(self, u, chunk, which):
            kind, b = self.kind, self.b
            mat, nmat, row, nrow = chunk
            mats = self.mats(u, mat, nmat)
            quarter, g, d, i = (far_same, "gf", "df", 0) if which == 0 else (me,) + (("gf", "df") if kind.single else ("gn", "dn")) + (1,)
            return [
                local(self.grad.at[(0, mats) + block_of(kind, quarter, row, nrow)], b[g], b["loc"].at[2 * i]),
                local(self.land.at[mats, i, pl.ds(row, nrow), :], b[d], b["loc"].at[2 * i + 1]),
            ]

        def load_mom(self, u):
            return local(self.mom.at[self.mats(u)], self.b["mo"].at[self.slot(u)], self.b["loc"].at[4])

        def weight(self):
            return self.b["sb"].at[0] if self.kind.single else self.b["w"]

        def rounded(self):
            return self.b["xs"].at[0] if self.kind.single else self.b["pb"]

        def load_weight(self, u):
            return local(self.master.at[self.mats(u)], self.weight(), self.b["loc"].at[5])

        def partial_sends(self, u):
            b = self.b
            src, dst = b["sb"].at[self.slot(u)], self.far_land.at[self.mats(u)]
            pairs = [(src, dst)]
            if self.kind.tail:
                pairs = [(b["sb"].at[self.slot(u), :, :, 0:384], self.far_land.at[self.mats(u), :, 0:384]),
                         (b["st"].at[self.slot(u)], self.far_tail.at[u])]
            return [remote(src, dst, b["rs_s"].at[u, i], b["rs_r"].at[u, i], far_same) for i, (src, dst) in enumerate(pairs)]

        def first_loads(self, u):
            for i, copy in enumerate(self.exchange(u)):
                copy.wait()
            for copy in self.load_pair(u, self.kind.chunks[0], 0):
                copy.start()

        def partial(self, u):
            kind, b = self.kind, self.b
            for index, chunk in enumerate(kind.chunks):
                mat, nmat, row, nrow = chunk
                copies = self.load_pair(u, chunk, 0)
                if index:
                    for copy in copies:
                        copy.start()
                for copy in copies:
                    copy.wait()
                b["sb"][self.slot(u), mat:mat + nmat, row:row + nrow, :] = b["gf"][...] + b["df"][...]
            if kind.tail:
                for i in range(kind.pair):
                    b["st"][self.slot(u), i] = join(b["sb"][self.slot(u), i], b["sb"][self.slot(u), i + kind.pair])

        def partial_start(self, u):
            for copy in self.partial_sends(u):
                copy.start()

        def second_loads(self, u):
            for copy in self.load_pair(u, self.kind.chunks[0], 1):
                copy.start()
            self.load_mom(u).start()

        def norm_sends(self, u):
            b = self.b
            return [
                remote(b["nr"].at[u, me], b["nr"].at[u, me], b["nm_s"].at[u, i], b["nm_r"].at[u, i], device)
                for i, device in enumerate((partner, far_same, far_other))
            ]

        def mom_out(self, u):
            return local(self.b["mo"].at[self.slot(u)], self.new_mom.at[self.mats(u)], self.b["loc"].at[12 + self.slot(u)])

        def momentum(self, u):
            kind, b = self.kind, self.b
            slot = self.slot(u)
            for copy in self.partial_sends(u):
                copy.wait()
            self.load_mom(u).wait()
            near_g, near_d = ("gf", "df") if kind.single else ("gn", "dn")
            sums = [None] * kind.unit
            for index, chunk in enumerate(kind.chunks):
                mat, nmat, row, nrow = chunk
                if kind.tail:
                    far_copies = [local(self.far_land.at[self.mats(u), :, 0:384], b["xl"].at[:, :, 0:384], b["loc"].at[6]),
                                  local(self.far_tail.at[u], b["xt"], b["loc"].at[10])]
                else:
                    far_copies = [local(self.far_land.at[self.mats(u, mat, nmat), pl.ds(row, nrow), :], b["xl"], b["loc"].at[6])]
                for copy in far_copies:
                    copy.start()
                copies = self.load_pair(u, chunk, 1)
                if index:
                    for copy in copies:
                        copy.start()
                for copy in copies:
                    copy.wait()
                for copy in far_copies:
                    copy.wait()
                for i in range(nmat):
                    if kind.tail:
                        lane = i // kind.pair * 64
                        cuts = ((slice(0, 384), b["xl"][i, :, 0:384]),
                                (slice(384, 448), b["xt"][i % kind.pair][:, lane:lane + 64]))
                    else:
                        cuts = ((slice(0, kind.q_cols), b["xl"][i]),)
                    for cut, far_sum in cuts:
                        total = (b[near_g][i, :, cut] + b[near_d][i, :, cut]) + far_sum
                        value = MOMENTUM * b["mo"][slot, mat + i, row:row + nrow, cut] + total * 0.25
                        b["mo"][slot, mat + i, row:row + nrow, cut] = value
                        sq_sum = jnp.sum(jnp.sum(value * value, axis=0, keepdims=True), axis=1, keepdims=True)
                        sums[mat + i] = sq_sum if sums[mat + i] is None else sums[mat + i] + sq_sum
            for i in range(kind.unit):
                b["nr"][u, me, i:i + 1, :] = jnp.broadcast_to(sums[i], (1, 128))
            self.mom_out(u).start()

        def norm_start(self, u):
            for copy in self.norm_sends(u):
                copy.start()

        def start_sends(self, u):
            kind, b = self.kind, self.b
            slot = self.slot(u)
            place = b["xg"].at[(u, slice(None)) + block_of(kind, me)]
            if kind.split:
                mine = b["xs"].at[slot, pl.ds(core * kind.half, kind.half)]
                theirs = b["xs"].at[slot, pl.ds(other * kind.half, kind.half)]
                routes = [(theirs, place, partner), (mine, place, far_same), (theirs, place, far_other)]
            else:
                routes = [(b["xs"].at[slot], place, partner), (b["xs"].at[slot], place, far_same)]
            if kind.half_pair:
                main = b["xg"].at[u, :, block_of(kind, me)[0], 0:384]
                for h, base in enumerate((core * kind.half, other * kind.half)):
                    routes[1 + h] = (b["xs"].at[slot, pl.ds(base, kind.half), :, 0:384], main, routes[1 + h][2])
                routes += [(b["xts"].at[slot, h], b["xtq"].at[u, h], device) for h, device in enumerate((far_same, far_other))]
            return [remote(src, dst, b["x_s"].at[u, i], b["x_r"].at[u, i], device) for i, (src, dst, device) in enumerate(routes)]

        def start_forward(self, u):
            kind, b = self.kind, self.b
            place = b["xg"].at[(u, slice(None)) + block_of(kind, far_same)]
            return remote(place, place, b["x_s"].at[u, 2], b["x_r"].at[u, 2], partner)

        def start_matrix(self, u):
            kind, b = self.kind, self.b
            slot = self.slot(u)
            for copy in self.norm_sends(u):
                copy.wait()
            total = ((b["nr"][u, 0] + b["nr"][u, 1]) + b["nr"][u, 2]) + b["nr"][u, 3]
            norm = jnp.sqrt(total) + NORM_EPS
            for i in range(kind.unit):
                b["xs"][slot, i] = (b["mo"][slot, i] / norm[i:i + 1, 0:1]).astype(BF16)
            if kind.split:
                b["xg"][(u, slice(None)) + block_of(kind, me)] = b["xs"][slot, pl.ds(core * kind.half, kind.half)]
            else:
                b["xg"][(u, slice(None)) + block_of(kind, me)] = b["xs"][slot]
            if kind.half_pair:
                for h, base in enumerate((core * kind.half, other * kind.half)):
                    for i in range(kind.half_pair):
                        left = b["xs"][slot, base + i].astype(F32)
                        right = b["xs"][slot, base + i + kind.half_pair].astype(F32)
                        b["xts"][slot, h, i] = join(left, right).astype(BF16)
            self.mom_out(u).wait()

        def start_start(self, u):
            for copy in self.start_sends(u):
                copy.start()

        def ortho_send(self, u):
            kind, b = self.kind, self.b
            return remote(b["xg"].at[(u, slice(None)) + block_of(kind, partner)], b["orow"].at[u], b["o_s"].at[u, 0], b["o_r"].at[u, 0], partner)

        def iterate(self, u):
            for copy in self.start_sends(u):
                copy.wait()
            if not self.kind.split:
                forward = self.start_forward(u)
                forward.start()
                forward.wait()
            if self.kind.half_pair:
                kind, b = self.kind, self.b
                for h, device in enumerate((far_same, far_other)):
                    for i in range(kind.half_pair):
                        both = b["xtq"][u, h, i].astype(F32)
                        for side in range(2):
                            part = both[:, 64 * side:64 * side + 64].astype(BF16)
                            b["xg"][u, i + side * kind.half_pair, block_of(kind, device)[0], 384:448] = part
            newton_schulz(self.kind, self.b["xg"], u, gram_acc)

        def iterate_start(self, u):
            if self.kind.split:
                self.ortho_send(u).start()

        def weight_out(self, u):
            return local(self.weight(), self.new_master.at[self.mats(u)], self.b["loc"].at[8])

        def param_out(self, u):
            if self.kind.late:
                return local(self.rounded(), self.param.at[self.mats(u)], self.b["loc"].at[9])
            return local(self.rounded(), self.param.at[(self.mats(u),) + block_of(self.kind, me)], self.b["loc"].at[9])

        def param_sends(self, u):
            kind, b = self.kind, self.b
            if kind.late:
                return []
            place = self.param.at[(self.mats(u),) + block_of(kind, me)]
            routes = [(self.rounded(), place, partner, 0), (self.rounded(), place, far_same, 1)]
            if kind.tail:
                main = self.param.at[self.mats(u), block_of(kind, me)[0], 0:384]
                routes[1:] = [(b["pb"].at[:, :, 0:384], main, far_same, 1), (b["pst"], b["ptq"].at[u], far_same, 3)]
            return [remote(src, dst, b["p_s"].at[u, i], b["p_r"].at[u, i], device) for src, dst, device, i in routes]

        def param_forwards(self, u):
            kind, b = self.kind, self.b
            if kind.late:
                return []
            place = self.param.at[(self.mats(u),) + block_of(kind, far_same)]
            routes = [(place, place, 2)]
            if kind.tail:
                main = self.param.at[self.mats(u), block_of(kind, far_same)[0], 0:384]
                routes = [(main, main, 2), (b["ptu"], self.tail_place(u), 4)]
            return [remote(src, dst, b["p_s"].at[u, i], b["p_r"].at[u, i], partner) for src, dst, i in routes]

        def tail_place(self, u):
            return self.param.at[self.mats(u), block_of(self.kind, far_same)[0], 384:448]

        def tail_out(self, u):
            return local(self.b["ptu"], self.tail_place(u), self.b["loc"].at[11])

        def update(self, u):
            kind, b = self.kind, self.b
            self.load_weight(u).wait()
            weight = self.weight()
            if kind.split:
                self.ortho_send(u).wait()
                parts = ((core * kind.half, lambda j: b["xg"][(u, j) + block_of(kind, me)]),
                         (other * kind.half, lambda j: b["orow"][u, j]))
            else:
                parts = ((0, lambda j: b["xg"][(u, j) + block_of(kind, me)]),)
            for base, ortho in parts:
                for j in range(kind.half):
                    old = weight[base + j]
                    new = old - LEARN_RATE * (kind.scale * ortho(j).astype(F32) + WEIGHT_DECAY * old)
                    weight[base + j] = new
                    self.rounded()[base + j] = new.astype(BF16)
            if kind.tail:
                for i in range(kind.pair):
                    b["pst"][i] = join(b["pb"][i].astype(F32), b["pb"][i + kind.pair].astype(F32)).astype(BF16)

        def update_start(self, u):
            self.weight_out(u).start()
            self.param_out(u).start()
            for copy in self.param_sends(u):
                copy.start()

        def drain(self, u):
            self.weight_out(u).wait()

        def forward(self, u):
            self.param_out(u).wait()
            for copy in self.param_sends(u):
                copy.wait()
            kind, b = self.kind, self.b
            if kind.tail:
                for i in range(kind.unit):
                    lane = i // kind.pair * 64
                    b["ptu"][i] = b["ptq"][u, i % kind.pair].astype(F32)[:, lane:lane + 64].astype(BF16)
                self.tail_out(u).start()
            for copy in self.param_forwards(u):
                copy.start()

        def finish(self, u):
            if self.kind.tail:
                self.tail_out(u).wait()
            for copy in self.param_forwards(u):
                copy.wait()

        def load_weight_start(self, u):
            self.load_weight(u).start()

    class LaneStage(Stage):
        def exchange(self, u):
            b = self.b
            half = self.kind.half
            src = self.grad.at[0, pl.ds(u * self.kind.unit + other * half, half)]
            return [remote(src, self.land.at[pl.ds(u * half, half)], b["d2d_s"].at[u, 0], b["d2d_r"].at[u, 0], partner)]

        def own_loads(self, u):
            b = self.b
            half = self.kind.half
            return [local(self.grad.at[0, pl.ds(u * self.kind.unit + core * half, half)], b["gf"], b["loc"].at[0]),
                    local(self.land.at[pl.ds(u * half, half)], b["df"], b["loc"].at[1])]

        def first_loads(self, u):
            for copy in self.exchange(u):
                copy.wait()
            for copy in self.own_loads(u):
                copy.start()

        def partial(self, u):
            kind, b = self.kind, self.b
            slot = self.slot(u)
            for copy in self.own_loads(u):
                copy.wait()
            cut = kind.rows // 2

            def far_piece(i, j, r):
                both = b["gf"][i, r * cut:(r + 1) * cut, :] + b["df"][i, r * cut:(r + 1) * cut, :]
                quarters = [both[:, 112 * d:112 * (d + 1)] for d in range(4)]
                if j == 0:
                    near = [jnp.where(chip == 0, quarters[d], quarters[2 + d]) for d in range(2)]
                    b["nb"][slot, 0, i, r * cut:(r + 1) * cut, :] = jnp.where(core == 0, near[0], near[1])
                    b["nb"][slot, 1, i, r * cut:(r + 1) * cut, :] = jnp.where(core == 0, near[1], near[0])
                return jnp.where(chip == 0, quarters[2 + j], quarters[j])

            last = far_piece(1, 1, 1)
            for g in range(7):
                piece = far_piece(g // 4, g // 2 % 2, g % 2)
                b["sb"][slot, g] = jnp.concatenate([piece, last[:, 16 * g:16 * g + 16]], axis=1)

        def partial_sends(self, u):
            b = self.b
            return [remote(b["sb"].at[self.slot(u)], self.far_land.at[u], b["rs_s"].at[u, 0], b["rs_r"].at[u, 0], far_same)]

        def second_loads(self, u):
            self.load_mom(u).start()

        def combine(self, u):
            kind, b = self.kind, self.b
            slot = self.slot(u)
            for copy in self.partial_sends(u):
                copy.wait()
            copy = local(self.far_land.at[u], b["xl"], b["loc"].at[6])
            copy.start()
            copy.wait()
            cut = kind.rows // 2
            for i in range(kind.half):
                for r in range(2):
                    rows = slice(r * cut, (r + 1) * cut)
                    first = b["xl"][i * 4 + r][:, :112]
                    if i * 4 + 2 + r < 7:
                        second = b["xl"][i * 4 + 2 + r][:, :112]
                    else:
                        second = jnp.concatenate([b["xl"][g][:, 112:128] for g in range(7)], axis=1)
                    b["nb"][slot, 0, i, rows, :] = b["nb"][slot, 0, i, rows, :] + jnp.where(core == 0, first, second)
                    b["tq"][i, rows, :] = b["nb"][slot, 1, i, rows, :] + jnp.where(core == 0, second, first)

        def total_send(self, u):
            b = self.b
            return remote(b["tq"], b["tr"].at[u], b["t_s"].at[u, 0], b["t_r"].at[u, 0], partner)

        def combine_start(self, u):
            self.total_send(u).start()

        def momentum(self, u):
            kind, b = self.kind, self.b
            slot = self.slot(u)
            self.load_mom(u).wait()
            self.total_send(u).wait()
            for base, total in ((core * kind.half, lambda i: b["nb"][slot, 0, i]), (other * kind.half, lambda i: b["tr"][u, i])):
                for i in range(kind.half):
                    value = MOMENTUM * b["mo"][slot, base + i] + total(i) * 0.25
                    b["mo"][slot, base + i] = value
                    sq_sum = jnp.sum(jnp.sum(value * value, axis=0, keepdims=True), axis=1, keepdims=True)
                    b["nr"][u, me, pl.ds(base + i, 1), :] = jnp.broadcast_to(sq_sum, (1, 128))
            self.mom_out(u).start()

        def lane_block(self, device):
            return pl.ds(pl.multiple_of(device * 128, 128), 128)

        def start_sends(self, u):
            kind, b = self.kind, self.b
            slot = self.slot(u)
            routes = (
                (b["xs"].at[slot, pl.ds(other * kind.half, kind.half)], b["xg"].at[u, :, :, self.lane_block(me)], partner),
                (b["xp"].at[slot, 0], b["xq"].at[u, 0], far_same),
                (b["xp"].at[slot, 1], b["xq"].at[u, 1], far_other),
            )
            return [remote(src, dst, b["x_s"].at[u, i], b["x_r"].at[u, i], device) for i, (src, dst, device) in enumerate(routes)]

        def start_matrix(self, u):
            kind, b = self.kind, self.b
            slot = self.slot(u)
            for copy in self.norm_sends(u):
                copy.wait()
            total = ((b["nr"][u, 0] + b["nr"][u, 1]) + b["nr"][u, 2]) + b["nr"][u, 3]
            norm = jnp.sqrt(total) + NORM_EPS
            pad = jnp.zeros((kind.rows, 16), F32)
            for i in range(kind.unit):
                start = b["mo"][slot, i] / norm[i:i + 1, 0:1]
                b["xs"][slot, i] = jnp.concatenate([start, pad], axis=1).astype(BF16)
            b["xg"][u, :, :, self.lane_block(me)] = b["xs"][slot, pl.ds(core * kind.half, kind.half)]
            cut = kind.rows // 4
            for h, base in enumerate((core * kind.half, other * kind.half)):
                pieces = [b["xs"][slot, base + g // 4, g % 4 * cut:(g % 4 + 1) * cut, :].astype(F32)[:, :112] for g in range(8)]
                for g, block in enumerate(pack(pieces)):
                    b["xp"][slot, h, g] = block.astype(BF16)
            self.mom_out(u).wait()

        def iterate(self, u):
            kind, b = self.kind, self.b
            for copy in self.start_sends(u):
                copy.wait()
            cut = kind.rows // 4
            pad = jnp.zeros((cut, 16), F32)
            for h, device in enumerate((far_same, far_other)):
                pieces = unpack([b["xq"][u, h, g].astype(F32) for g in range(7)])
                for g, piece in enumerate(pieces):
                    block = jnp.concatenate([piece, pad], axis=1).astype(BF16)
                    b["xg"][u, g // 4, g % 4 * cut:(g % 4 + 1) * cut, self.lane_block(device)] = block
            newton_schulz(kind, b["xg"], u, gram_acc)

        def ortho_send(self, u):
            b = self.b
            return remote(b["xg"].at[u, :, :, self.lane_block(partner)], b["orow"].at[u], b["o_s"].at[u, 0], b["o_r"].at[u, 0], partner)

        def param_out(self, u):
            return local(self.b["pk"], self.param_land.at[u, me], self.b["loc"].at[9])

        def param_sends(self, u):
            b = self.b
            place = self.param_land.at[u, me]
            return [
                remote(b["pk"], place, b["p_s"].at[u, i], b["p_r"].at[u, i], device)
                for i, device in enumerate((partner, far_same))
            ]

        def param_forwards(self, u):
            b = self.b
            place = self.param_land.at[u, far_same]
            return [remote(place, place, b["p_s"].at[u, 2], b["p_r"].at[u, 2], partner)]

        def update(self, u):
            kind, b = self.kind, self.b
            self.load_weight(u).wait()
            self.ortho_send(u).wait()
            weight = b["w"]
            parts = ((core * kind.half, lambda j: b["xg"][u, j, :, self.lane_block(me)]),
                     (other * kind.half, lambda j: b["orow"][u, j]))
            for base, ortho in parts:
                for j in range(kind.half):
                    old = weight[base + j]
                    new = old - LEARN_RATE * (kind.scale * ortho(j).astype(F32)[:, :112] + WEIGHT_DECAY * old)
                    weight[base + j] = new
                    b["pb"][base + j] = new.astype(BF16)
            cut = kind.rows // 2
            pieces = [b["pb"][g // 2, g % 2 * cut:(g % 2 + 1) * cut, :].astype(F32) for g in range(8)]
            for g, block in enumerate(pack(pieces)):
                b["pk"][g] = block.astype(BF16)

        def matrix_out(self, u):
            return local(self.b["pa"], self.param.at[self.mats(u)], self.b["loc"].at[2])

        def finish(self, u):
            kind, b = self.kind, self.b
            for copy in self.param_forwards(u):
                copy.wait()
            copy = local(self.param_land.at[u], b["pv"], b["loc"].at[3])
            copy.start()
            copy.wait()
            cut = kind.rows // 2
            for g in range(8):
                if g < 7:
                    quarters = [b["pv"][d, g].astype(F32)[:, :112] for d in range(4)]
                else:
                    quarters = [unpack([b["pv"][d, k].astype(F32) for k in range(7)])[7] for d in range(4)]
                b["pa"][g // 2, g % 2 * cut:(g % 2 + 1) * cut, :] = jnp.concatenate(quarters, axis=1).astype(BF16)
            self.matrix_out(u).start()

        def close(self, u):
            self.matrix_out(u).wait()

    stages = [LaneStage(kind) if kind.lanes else Stage(kind) for kind in kinds]
    bases = {}
    total_units = 0
    for k in ORDER:
        bases[k] = total_units
        total_units += kinds[k].units

    for k in ORDER:
        stage = stages[k]

        def send_all(u, carry, stage=stage):
            for copy in stage.exchange(u):
                copy.start()
            return carry

        lax.fori_loop(0, kinds[k].units, send_all, 0)

    def step(t, carry):
        def run(name, lag):
            for k in ORDER:
                method = getattr(stages[k], name, None)
                if method is None:
                    continue
                u = t - lag - bases[k]

                @pl.when((u >= 0) & (u < kinds[k].units))
                def _(method=method, u=u):
                    method(u)

        for name, lag in SCHEDULE:
            run(name, LAGS[lag])
        return carry

    lax.fori_loop(0, total_units + LAGS[-1], step, 0)


def copy_kernel(cuts, num, *refs):
    sources, targets, stores = refs[:num], refs[num:2 * num], refs[2 * num:3 * num]
    in_sem, out_sem = refs[3 * num:]
    loads = [pltpu.make_async_copy(sources[i].at[pl.ds(lo, size)], stores[i].at[pl.ds(lo, size)], in_sem.at[n])
             for n, (i, lo, size) in enumerate(cuts)]
    saves = [pltpu.make_async_copy(stores[i].at[pl.ds(lo, size)], targets[i].at[pl.ds(lo, size)], out_sem.at[n])
             for n, (i, lo, size) in enumerate(cuts)]
    for load in loads:
        load.start()
    for load, save in zip(loads, saves):
        load.wait()
        save.start()
    for save in saves:
        save.wait()


def copy_out(arrays, pieces):
    cuts = []
    for i, array in enumerate(arrays):
        size = max(1, array.shape[0] // pieces)
        cuts += [(i, lo, size) for lo in range(0, array.shape[0], size)]
    total = sum(array.size * array.dtype.itemsize for array in arrays)
    return pl.pallas_call(
        functools.partial(copy_kernel, cuts, len(arrays)),
        out_shape=[jax.ShapeDtypeStruct(array.shape, array.dtype) for array in arrays],
        in_specs=[pl.BlockSpec(memory_space=pl.ANY)] * len(arrays),
        out_specs=[pl.BlockSpec(memory_space=pl.ANY)] * len(arrays),
        scratch_shapes=[pltpu.VMEM(array.shape, array.dtype) for array in arrays]
        + [pltpu.SemaphoreType.DMA((len(cuts),))] * 2,
        compiler_params=pltpu.CompilerParams(vmem_limit_bytes=67043328),
        cost_estimate=pl.CostEstimate(flops=1200 * total, bytes_accessed=2 * total, transcendentals=0),
    )(*arrays)


def gather_kernel(own, far, near, near_far, target, *rest):
    stores, sem = rest[:4], rest[4]
    me = lax.axis_index("data")
    chip, core = me // 2, me % 2
    places = (me, 2 * (1 - chip) + core, 2 * chip + 1 - core, 2 * (1 - chip) + 1 - core)
    rows = own.shape[1]
    loads = [pltpu.make_async_copy(source, stores[i], sem.at[0, i]) for i, source in enumerate((own, far, near, near_far))]
    saves = [pltpu.make_async_copy(stores[i], target.at[:, pl.ds(pl.multiple_of(place * rows, 16), rows), :], sem.at[1, i])
             for i, place in enumerate(places)]
    for load in loads:
        load.start()
    for load, save in zip(loads, saves):
        load.wait()
        save.start()
    for save in saves:
        save.wait()


def gather_rows(own, arrays):
    far = lax.ppermute(own, "data", [(0, 2), (2, 0), (1, 3), (3, 1)])
    cores = [(0, 1), (1, 0), (2, 3), (3, 2)]
    near = lax.ppermute(own, "data", cores)
    copied = copy_out(arrays, 4)
    far, near, copied = lax.optimization_barrier((far, near, copied))
    near_far = lax.ppermute(far, "data", cores)
    gathered = pl.pallas_call(
        gather_kernel,
        out_shape=jax.ShapeDtypeStruct((own.shape[0], 4 * own.shape[1], own.shape[2]), own.dtype),
        in_specs=[pl.BlockSpec(memory_space=pl.ANY)] * 4,
        out_specs=pl.BlockSpec(memory_space=pl.ANY),
        scratch_shapes=[pltpu.VMEM(own.shape, own.dtype)] * 4 + [pltpu.SemaphoreType.DMA((2, 4))],
        cost_estimate=pl.CostEstimate(flops=0, bytes_accessed=8 * own.size * 2, transcendentals=0),
    )(own, far, near, near_far)
    return gathered, copied


def solution(mesh):
    def local_step(*arrays):
        num = len(arrays) // 3
        kinds = [Kind(k, *arrays[k].shape[1:]) for k in range(num)]
        scratch = [kind.scratch() for kind in kinds]
        names = [tuple(shapes) for shapes in scratch]
        flat = [shape for shapes in scratch for shape in shapes.values()]
        flat.append(pltpu.VMEM((kinds[1].rows, kinds[1].rows), F32))
        row_shapes = [jax.ShapeDtypeStruct((kind.count, kind.q_rows, kind.q_cols), F32) for kind in kinds]
        full_shapes = [
            jax.ShapeDtypeStruct((kind.count,) + ((kind.q_rows, kind.q_cols) if kind.late else (kind.rows, kind.cols)), BF16)
            for kind in kinds
        ]
        land_shapes = [jax.ShapeDtypeStruct((kind.count, 2, kind.q_rows, kind.q_cols), F32) for kind in kinds]
        far_shapes = list(row_shapes)
        lane = kinds[3]
        land_shapes[3] = jax.ShapeDtypeStruct((lane.count // 2, lane.rows, lane.cols), F32)
        far_shapes[3] = jax.ShapeDtypeStruct((lane.units, 7, lane.rows // 2, 128), F32)
        param_shape = jax.ShapeDtypeStruct((lane.units, 4, 7, lane.rows // 2, 128), BF16)
        tail_shapes = [jax.ShapeDtypeStruct((kind.units, kind.pair, kind.q_rows, 128), F32) for kind in kinds if kind.tail]
        flipped = [jnp.swapaxes(array, -1, -2) if kinds[i % num].flip else array for i, array in enumerate(arrays)]
        outs = pl.pallas_call(
            functools.partial(kernel, kinds, names),
            out_shape=row_shapes + row_shapes + full_shapes + land_shapes + far_shapes + [param_shape] + tail_shapes,
            in_specs=[pl.BlockSpec(memory_space=pl.ANY)] * (3 * num),
            out_specs=[pl.BlockSpec(memory_space=pl.ANY)] * (5 * num + 3),
            scratch_shapes=flat,
            compiler_params=pltpu.CompilerParams(
                collective_id=0, has_side_effects=True, vmem_limit_bytes=67043328
            ),
        )(*flipped)
        outs = list(outs[:3 * num])
        late = next(2 * num + kind.index for kind in kinds if kind.late)
        early = [i for i in range(3 * num) if i != late]
        gathered, copied = gather_rows(outs[late], [outs[i] for i in early])
        for i, array in zip(early + [late], list(copied) + [gathered]):
            outs[i] = array
        return tuple(jnp.swapaxes(array, -1, -2) if kinds[i % num].flip else array for i, array in enumerate(outs[:3 * num]))

    grad_spec = P(("stage", "data"), None, None, None)
    row_spec = P("stage", "data", None)
    full_spec = P("stage", None, None)
    in_specs = (grad_spec,) * 5 + (row_spec,) * 10
    out_specs = (row_spec,) * 10 + (full_spec,) * 5
    return jax.shard_map(local_step, mesh=mesh, in_specs=in_specs, out_specs=out_specs, check_vma=False)
```

```python
import functools
import math
import jax
import jax.numpy as jnp
from jax import lax
from jax.experimental import pallas as pl
from jax.experimental.pallas import tpu as pltpu
from jax.sharding import PartitionSpec as P

NS_STEPS = 5
MOMENTUM = 0.95
LEARN_RATE = 0.2
WEIGHT_DECAY = 0.25
NORM_EPS = 1e-7
COEF_A = 3.4445
COEF_B = -4.7750
COEF_C = 2.0315
F32 = jnp.float32
BF16 = jnp.bfloat16

UNIT_MATS = (2, 2, 1, 4, 4)
ORDER = (4, 2, 1, 3, 0)
LANE, MAIN, TAIL, BLOCK, PAD = 128, 384, 64, 112, 16
UPDATE = 9
SCHEDULE = (
    ("exchange_start", 0), ("combine", 4), ("start_matrix", 6), ("close", UPDATE + 3), ("drain", UPDATE + 1),
    ("load_weight_start", UPDATE), ("first_loads", 2), ("second_loads", 4),
    ("start_start", 6), ("combine_start", 4), ("momentum", 4), ("norm_start", 4),
    ("partial", 2), ("iterate", 7), ("partial_start", 2), ("iterate_start", 7),
    ("update", UPDATE), ("update_start", UPDATE), ("finish", UPDATE + 2), ("forward", UPDATE + 1),
)
STEPS_BEHIND = max(lag for _, lag in SCHEDULE)


class Kind:
    def __init__(self, index, count, rows, cols):
        self.index = index
        self.scale = 0.2 * math.sqrt(max(rows, cols))
        self.flip = index in (2, 3)
        if self.flip:
            rows, cols = cols, rows
        self.lanes = index == 3
        self.tail = index in (0, 4)
        self.count, self.rows, self.cols = count, rows, cols
        self.q_rows, self.q_cols = (rows, cols // 4) if self.flip else (rows // 4, cols)
        self.unit = UNIT_MATS[index]
        self.units = count // self.unit
        self.split = self.unit % 2 == 0
        self.half = self.unit // 2 if self.split else self.unit
        self.single = self.units == 1
        self.late = index == 1
        self.pair = self.unit // 2
        self.half_pair = self.half // 2 if self.tail else 0
        if index == 1:
            self.chunks = [(0, 1, 0, self.q_rows), (1, 1, 0, self.q_rows)]
        elif index == 2:
            step = self.q_rows // 2
            self.chunks = [(0, 1, 0, step), (0, 1, step, step)]
        else:
            self.chunks = [(0, self.unit, 0, self.q_rows)]

    def sems(self):
        shapes = {name: pltpu.SemaphoreType.DMA((self.units, 5)) for name in (
            "d2d_s", "d2d_r", "rs_s", "rs_r", "nm_s", "nm_r", "x_s", "x_r", "o_s", "o_r", "p_s", "p_r", "t_s", "t_r")}
        shapes["loc"] = pltpu.SemaphoreType.DMA((16,))
        return shapes

    def scratch(self):
        if self.lanes:
            return self.lane_scratch()
        unit, q_rows, q_cols = self.unit, self.q_rows, self.q_cols
        slots = 1 if self.single else 2
        _, cmats, _, crows = self.chunks[0]
        chunk = pltpu.VMEM((cmats, crows, q_cols), F32)
        shapes = dict(
            gf=chunk, df=chunk, xl=chunk,
            mo=pltpu.VMEM((slots, unit, q_rows, q_cols), F32),
            sb=pltpu.VMEM((slots, unit, q_rows, q_cols), F32),
            xs=pltpu.VMEM((slots, unit, q_rows, q_cols), BF16),
            xg=pltpu.VMEM((self.units, self.half, self.rows, self.cols), BF16),
            nr=pltpu.VMEM((self.units, 4, 8, LANE), F32),
        )
        if not self.single:
            shapes["gn"] = chunk
            shapes["dn"] = chunk
            shapes["w"] = pltpu.VMEM((unit, q_rows, q_cols), F32)
            shapes["pb"] = pltpu.VMEM((2, unit, q_rows, q_cols), BF16)
        if self.tail:
            shapes["st"] = pltpu.VMEM((slots, self.pair, q_rows, LANE), F32)
            shapes["xt"] = pltpu.VMEM((self.pair, q_rows, LANE), F32)
            shapes["pst"] = pltpu.VMEM((2, self.pair, q_rows, LANE), BF16)
            shapes["ptq"] = pltpu.VMEM((self.units, self.pair, q_rows, LANE), BF16)
            shapes["ptu"] = pltpu.VMEM((unit, q_rows, TAIL), BF16)
        if self.half_pair:
            shapes["xts"] = pltpu.VMEM((slots, 2, self.half_pair, q_rows, LANE), BF16)
            shapes["xtq"] = pltpu.VMEM((self.units, 2, self.half_pair, q_rows, LANE), BF16)
        if self.split:
            shapes["orow"] = pltpu.VMEM((self.units, self.half, q_rows, q_cols), BF16)
        shapes.update(self.sems())
        return shapes

    def lane_scratch(self):
        unit, half, rows, cols, lanes, units = self.unit, self.half, self.rows, self.cols, self.q_cols, self.units
        shapes = dict(
            gf=pltpu.VMEM((half, rows, cols), F32),
            df=pltpu.VMEM((half, rows, cols), F32),
            sb=pltpu.VMEM((2, 7, rows // 2, LANE), F32),
            nb=pltpu.VMEM((2, 2, half, rows, lanes), F32),
            xl=pltpu.VMEM((7, rows // 2, LANE), F32),
            tq=pltpu.VMEM((half, rows, lanes), F32),
            tr=pltpu.VMEM((units, half, rows, lanes), F32),
            mo=pltpu.VMEM((2, unit, rows, lanes), F32),
            w=pltpu.VMEM((unit, rows, lanes), F32),
            xs=pltpu.VMEM((2, unit, rows, LANE), BF16),
            xp=pltpu.VMEM((2, 2, 7, rows // 4, LANE), BF16),
            xq=pltpu.VMEM((units, 2, 7, rows // 4, LANE), BF16),
            xg=pltpu.VMEM((units, half, rows, 512), BF16),
            orow=pltpu.VMEM((units, half, rows, LANE), BF16),
            pb=pltpu.VMEM((unit, rows, lanes), BF16),
            pk=pltpu.VMEM((2, 7, rows // 2, LANE), BF16),
            pv=pltpu.VMEM((4, 7, rows // 2, LANE), BF16),
            pa=pltpu.VMEM((unit, rows, cols), BF16),
            nr=pltpu.VMEM((units, 4, 8, LANE), F32),
        )
        shapes.update(self.sems())
        return shapes


def pack(pieces):
    last = pieces[7]
    return [jnp.concatenate([pieces[g], last[:, 16 * g:16 * g + 16]], axis=1) for g in range(7)]


def join(left, right):
    return jnp.concatenate([left[:, MAIN:MAIN + TAIL], right[:, MAIN:MAIN + TAIL]], axis=1)


def unpack(blocks):
    return [block[:, :BLOCK] for block in blocks] + [jnp.concatenate([block[:, BLOCK:LANE] for block in blocks], axis=1)]


def dot(left, right, dims):
    return lax.dot_general(left, right, (dims, ((), ())), preferred_element_type=F32)


def newton_schulz(kind, xg, u, gram_acc):
    cols = kind.cols

    def poly(gram_mat):
        square = dot(gram_mat, gram_mat, ((1,), (0,)))
        return (COEF_B * gram_mat.astype(F32) + COEF_C * square).astype(BF16)

    if kind.single:
        block = 512

        def iteration(_, carry):
            gram_acc[...] = jnp.zeros_like(gram_acc)

            def add(b, c):
                part = xg[u, 0, :, pl.ds(pl.multiple_of(b * block, block), block)]
                gram_acc[...] += dot(part, part, ((1,), (1,)))
                return c

            lax.fori_loop(0, cols // block, add, 0)
            poly_mat = poly(gram_acc[...].astype(BF16))

            def apply(b, c):
                cut = pl.ds(pl.multiple_of(b * block, block), block)
                part = xg[u, 0, :, cut]
                update = dot(poly_mat, part, ((1,), (0,)))
                xg[u, 0, :, cut] = (COEF_A * part.astype(F32) + update).astype(BF16)
                return c

            lax.fori_loop(0, cols // block, apply, 0)
            return carry
    else:

        def iteration(_, carry):
            mats = [xg[u, j] for j in range(kind.half)]
            polys = [poly(gram_mat) for gram_mat in [dot(mat, mat, ((1,), (1,))).astype(BF16) for mat in mats]]
            news = [COEF_A * mat.astype(F32) + dot(poly_mat, mat, ((1,), (0,))) for poly_mat, mat in zip(polys, mats)]
            for j, new in enumerate(news):
                xg[u, j] = new.astype(BF16)
            return carry

    lax.fori_loop(0, NS_STEPS, iteration, 0)


def kernel(kinds, names, *refs):
    num = len(kinds)
    grads, moms, masters = refs[:num], refs[num:2 * num], refs[2 * num:3 * num]
    outs = refs[3 * num:8 * num]
    new_moms, new_masters, params, lands, far_lands = [outs[i * num:(i + 1) * num] for i in range(5)]
    param_land = refs[8 * num]
    far_tails = {0: refs[8 * num + 1], 4: refs[8 * num + 2]}
    rest = list(refs[8 * num + 3:])
    bufs = []
    for k in range(num):
        bufs.append({name: rest.pop(0) for name in names[k]})
    gram_acc = rest.pop(0)

    me = lax.axis_index("data")
    chip, core = me // 2, me % 2
    far, other = 1 - chip, 1 - core
    partner, far_same, far_other = 2 * chip + other, 2 * far + core, 2 * far + other

    def to(device):
        return dict(device_id={"data": device}, device_id_type=pl.DeviceIdType.MESH)

    def remote(src, dst, send, recv, device):
        return pltpu.make_async_remote_copy(src_ref=src, dst_ref=dst, send_sem=send, recv_sem=recv, **to(device))

    def local(src, dst, sem):
        return pltpu.make_async_copy(src, dst, sem)

    barrier = pltpu.get_barrier_semaphore()
    for device in (partner, far_same, far_other):
        pl.semaphore_signal(barrier, inc=1, **to(device))
    pl.semaphore_wait(barrier, 3)

    def block_of(kind, device, row=0, nrow=None):
        nrow = kind.q_rows if nrow is None else nrow
        if kind.flip:
            return pl.ds(row, nrow), pl.ds(pl.multiple_of(device * kind.q_cols, LANE), kind.q_cols)
        return pl.ds(pl.multiple_of(device * kind.q_rows + row, 16), nrow), slice(None)

    class Stage:
        def __init__(self, kind):
            self.kind = kind
            self.b = bufs[kind.index]
            self.grad, self.mom, self.master = grads[kind.index], moms[kind.index], masters[kind.index]
            self.new_mom, self.new_master, self.param = new_moms[kind.index], new_masters[kind.index], params[kind.index]
            self.land, self.far_land = lands[kind.index], far_lands[kind.index]
            self.param_land = param_land
            self.far_tail = far_tails.get(kind.index)

        def mats(self, u, offset=0, size=None):
            kind = self.kind
            return pl.ds(u * kind.unit + offset, kind.unit if size is None else size)

        def slot(self, u):
            return 0 if self.kind.single else u % 2

        def exchange(self, u):
            kind, b = self.kind, self.b
            mats = self.mats(u)
            return [
                remote(self.grad.at[(0, mats) + block_of(kind, quarter)], self.land.at[mats, i],
                       b["d2d_s"].at[u, i], b["d2d_r"].at[u, i], partner)
                for i, quarter in enumerate((far_other, partner))
            ]

        def exchange_start(self, u):
            for copy in self.exchange(u):
                copy.start()

        def load_pair(self, u, chunk, which):
            kind, b = self.kind, self.b
            mat, nmat, row, nrow = chunk
            mats = self.mats(u, mat, nmat)
            quarter, g, d, i = (far_same, "gf", "df", 0) if which == 0 else (me,) + (("gf", "df") if kind.single else ("gn", "dn")) + (1,)
            return [
                local(self.grad.at[(0, mats) + block_of(kind, quarter, row, nrow)], b[g], b["loc"].at[2 * i]),
                local(self.land.at[mats, i, pl.ds(row, nrow), :], b[d], b["loc"].at[2 * i + 1]),
            ]

        def load_mom(self, u):
            return local(self.mom.at[self.mats(u)], self.b["mo"].at[self.slot(u)], self.b["loc"].at[4])

        def weight(self):
            return self.b["sb"].at[0] if self.kind.single else self.b["w"]

        def rounded(self, u):
            return self.b["xs"].at[0] if self.kind.single else self.b["pb"].at[self.slot(u)]

        def load_weight(self, u):
            return local(self.master.at[self.mats(u)], self.weight(), self.b["loc"].at[5])

        def partial_sends(self, u):
            b = self.b
            src, dst = b["sb"].at[self.slot(u)], self.far_land.at[self.mats(u)]
            pairs = [(src, dst)]
            if self.kind.tail:
                pairs = [(b["sb"].at[self.slot(u), :, :, 0:MAIN], self.far_land.at[self.mats(u), :, 0:MAIN]),
                         (b["st"].at[self.slot(u)], self.far_tail.at[u])]
            return [remote(src, dst, b["rs_s"].at[u, i], b["rs_r"].at[u, i], far_same) for i, (src, dst) in enumerate(pairs)]

        def first_loads(self, u):
            for i, copy in enumerate(self.exchange(u)):
                copy.wait()
            for copy in self.load_pair(u, self.kind.chunks[0], 0):
                copy.start()

        def partial(self, u):
            kind, b = self.kind, self.b
            for index, chunk in enumerate(kind.chunks):
                mat, nmat, row, nrow = chunk
                copies = self.load_pair(u, chunk, 0)
                if index:
                    for copy in copies:
                        copy.start()
                for copy in copies:
                    copy.wait()
                b["sb"][self.slot(u), mat:mat + nmat, row:row + nrow, :] = b["gf"][...] + b["df"][...]
            if kind.tail:
                for i in range(kind.pair):
                    b["st"][self.slot(u), i] = join(b["sb"][self.slot(u), i], b["sb"][self.slot(u), i + kind.pair])

        def partial_start(self, u):
            for copy in self.partial_sends(u):
                copy.start()

        def second_loads(self, u):
            for copy in self.load_pair(u, self.kind.chunks[0], 1):
                copy.start()
            self.load_mom(u).start()

        def norm_sends(self, u):
            b = self.b
            return [
                remote(b["nr"].at[u, me], b["nr"].at[u, me], b["nm_s"].at[u, i], b["nm_r"].at[u, i], device)
                for i, device in enumerate((partner, far_same, far_other))
            ]

        def mom_out(self, u):
            return local(self.b["mo"].at[self.slot(u)], self.new_mom.at[self.mats(u)], self.b["loc"].at[12 + self.slot(u)])

        def momentum(self, u):
            kind, b = self.kind, self.b
            slot = self.slot(u)
            for copy in self.partial_sends(u):
                copy.wait()
            self.load_mom(u).wait()
            near_g, near_d = ("gf", "df") if kind.single else ("gn", "dn")
            sums = [None] * kind.unit
            for index, chunk in enumerate(kind.chunks):
                mat, nmat, row, nrow = chunk
                if kind.tail:
                    far_copies = [local(self.far_land.at[self.mats(u), :, 0:MAIN], b["xl"].at[:, :, 0:MAIN], b["loc"].at[6]),
                                  local(self.far_tail.at[u], b["xt"], b["loc"].at[10])]
                else:
                    far_copies = [local(self.far_land.at[self.mats(u, mat, nmat), pl.ds(row, nrow), :], b["xl"], b["loc"].at[6])]
                for copy in far_copies:
                    copy.start()
                copies = self.load_pair(u, chunk, 1)
                if index:
                    for copy in copies:
                        copy.start()
                for copy in copies:
                    copy.wait()
                for copy in far_copies:
                    copy.wait()
                for i in range(nmat):
                    if kind.tail:
                        lane = i // kind.pair * TAIL
                        cuts = ((slice(0, MAIN), b["xl"][i, :, 0:MAIN]),
                                (slice(MAIN, MAIN + TAIL), b["xt"][i % kind.pair][:, lane:lane + TAIL]))
                    else:
                        cuts = ((slice(0, kind.q_cols), b["xl"][i]),)
                    for cut, far_sum in cuts:
                        total = (b[near_g][i, :, cut] + b[near_d][i, :, cut]) + far_sum
                        value = MOMENTUM * b["mo"][slot, mat + i, row:row + nrow, cut] + total * 0.25
                        b["mo"][slot, mat + i, row:row + nrow, cut] = value
                        sq_sum = jnp.sum(jnp.sum(value * value, axis=0, keepdims=True), axis=1, keepdims=True)
                        sums[mat + i] = sq_sum if sums[mat + i] is None else sums[mat + i] + sq_sum
            for i in range(kind.unit):
                b["nr"][u, me, i:i + 1, :] = jnp.broadcast_to(sums[i], (1, LANE))
            self.mom_out(u).start()

        def norm_start(self, u):
            for copy in self.norm_sends(u):
                copy.start()

        def start_sends(self, u):
            kind, b = self.kind, self.b
            slot = self.slot(u)
            place = b["xg"].at[(u, slice(None)) + block_of(kind, me)]
            if kind.split:
                mine = b["xs"].at[slot, pl.ds(core * kind.half, kind.half)]
                theirs = b["xs"].at[slot, pl.ds(other * kind.half, kind.half)]
                routes = [(theirs, place, partner), (mine, place, far_same), (theirs, place, far_other)]
            else:
                routes = [(b["xs"].at[slot], place, partner), (b["xs"].at[slot], place, far_same)]
            if kind.half_pair:
                main = b["xg"].at[u, :, block_of(kind, me)[0], 0:MAIN]
                for h, base in enumerate((core * kind.half, other * kind.half)):
                    routes[1 + h] = (b["xs"].at[slot, pl.ds(base, kind.half), :, 0:MAIN], main, routes[1 + h][2])
                routes += [(b["xts"].at[slot, h], b["xtq"].at[u, h], device) for h, device in enumerate((far_same, far_other))]
            return [remote(src, dst, b["x_s"].at[u, i], b["x_r"].at[u, i], device) for i, (src, dst, device) in enumerate(routes)]

        def start_forward(self, u):
            kind, b = self.kind, self.b
            place = b["xg"].at[(u, slice(None)) + block_of(kind, far_same)]
            return remote(place, place, b["x_s"].at[u, 2], b["x_r"].at[u, 2], partner)

        def start_matrix(self, u):
            kind, b = self.kind, self.b
            slot = self.slot(u)
            for copy in self.norm_sends(u):
                copy.wait()
            total = ((b["nr"][u, 0] + b["nr"][u, 1]) + b["nr"][u, 2]) + b["nr"][u, 3]
            norm = jnp.sqrt(total) + NORM_EPS
            for i in range(kind.unit):
                b["xs"][slot, i] = (b["mo"][slot, i] / norm[i:i + 1, 0:1]).astype(BF16)
            if kind.split:
                b["xg"][(u, slice(None)) + block_of(kind, me)] = b["xs"][slot, pl.ds(core * kind.half, kind.half)]
            else:
                b["xg"][(u, slice(None)) + block_of(kind, me)] = b["xs"][slot]
            if kind.half_pair:
                for h, base in enumerate((core * kind.half, other * kind.half)):
                    for i in range(kind.half_pair):
                        left = b["xs"][slot, base + i].astype(F32)
                        right = b["xs"][slot, base + i + kind.half_pair].astype(F32)
                        b["xts"][slot, h, i] = join(left, right).astype(BF16)
            self.mom_out(u).wait()

        def start_start(self, u):
            for copy in self.start_sends(u):
                copy.start()

        def ortho_send(self, u):
            kind, b = self.kind, self.b
            return remote(b["xg"].at[(u, slice(None)) + block_of(kind, partner)], b["orow"].at[u], b["o_s"].at[u, 0], b["o_r"].at[u, 0], partner)

        def iterate(self, u):
            for copy in self.start_sends(u):
                copy.wait()
            if not self.kind.split:
                forward = self.start_forward(u)
                forward.start()
                forward.wait()
            if self.kind.half_pair:
                kind, b = self.kind, self.b
                for h, device in enumerate((far_same, far_other)):
                    for i in range(kind.half_pair):
                        both = b["xtq"][u, h, i].astype(F32)
                        for side in range(2):
                            part = both[:, TAIL * side:TAIL * side + TAIL].astype(BF16)
                            b["xg"][u, i + side * kind.half_pair, block_of(kind, device)[0], MAIN:MAIN + TAIL] = part
            newton_schulz(self.kind, self.b["xg"], u, gram_acc)

        def iterate_start(self, u):
            if self.kind.split:
                self.ortho_send(u).start()

        def weight_out(self, u):
            return local(self.weight(), self.new_master.at[self.mats(u)], self.b["loc"].at[8])

        def param_out(self, u):
            if self.kind.late:
                return local(self.rounded(u), self.param.at[self.mats(u)], self.b["loc"].at[14 + self.slot(u)])
            return local(self.rounded(u), self.param.at[(self.mats(u),) + block_of(self.kind, me)], self.b["loc"].at[14 + self.slot(u)])

        def param_sends(self, u):
            kind, b = self.kind, self.b
            if kind.late:
                return []
            place = self.param.at[(self.mats(u),) + block_of(kind, me)]
            routes = [(self.rounded(u), place, partner, 0), (self.rounded(u), place, far_same, 1)]
            if kind.tail:
                main = self.param.at[self.mats(u), block_of(kind, me)[0], 0:MAIN]
                routes[1:] = [(b["pb"].at[self.slot(u), :, :, 0:MAIN], main, far_same, 1), (b["pst"].at[self.slot(u)], b["ptq"].at[u], far_same, 3)]
            return [remote(src, dst, b["p_s"].at[u, i], b["p_r"].at[u, i], device) for src, dst, device, i in routes]

        def param_forwards(self, u):
            kind, b = self.kind, self.b
            if kind.late:
                return []
            place = self.param.at[(self.mats(u),) + block_of(kind, far_same)]
            routes = [(place, place, 2)]
            if kind.tail:
                main = self.param.at[self.mats(u), block_of(kind, far_same)[0], 0:MAIN]
                routes = [(main, main, 2), (b["ptu"], self.tail_place(u), 4)]
            return [remote(src, dst, b["p_s"].at[u, i], b["p_r"].at[u, i], partner) for src, dst, i in routes]

        def tail_place(self, u):
            return self.param.at[self.mats(u), block_of(self.kind, far_same)[0], MAIN:MAIN + TAIL]

        def tail_out(self, u):
            return local(self.b["ptu"], self.tail_place(u), self.b["loc"].at[11])

        def update(self, u):
            kind, b = self.kind, self.b
            self.load_weight(u).wait()
            weight = self.weight()
            if kind.split:
                self.ortho_send(u).wait()
                parts = ((core * kind.half, lambda j: b["xg"][(u, j) + block_of(kind, me)]),
                         (other * kind.half, lambda j: b["orow"][u, j]))
            else:
                parts = ((0, lambda j: b["xg"][(u, j) + block_of(kind, me)]),)
            for base, ortho in parts:
                for j in range(kind.half):
                    old = weight[base + j]
                    new = old - LEARN_RATE * (kind.scale * ortho(j).astype(F32) + WEIGHT_DECAY * old)
                    weight[base + j] = new
                    self.rounded(u)[base + j] = new.astype(BF16)
            if kind.tail and not kind.late:
                for i in range(kind.pair):
                    left, right = (b["pb"][self.slot(u), j].astype(F32) for j in (i, i + kind.pair))
                    b["pst"][self.slot(u), i] = join(left, right).astype(BF16)

        def update_start(self, u):
            self.weight_out(u).start()
            self.param_out(u).start()
            for copy in self.param_sends(u):
                copy.start()

        def drain(self, u):
            self.weight_out(u).wait()

        def forward(self, u):
            self.param_out(u).wait()
            for copy in self.param_sends(u):
                copy.wait()
            kind, b = self.kind, self.b
            if kind.tail and not kind.late:
                for i in range(kind.unit):
                    lane = i // kind.pair * TAIL
                    b["ptu"][i] = b["ptq"][u, i % kind.pair].astype(F32)[:, lane:lane + TAIL].astype(BF16)
                self.tail_out(u).start()
            for copy in self.param_forwards(u):
                copy.start()

        def finish(self, u):
            if self.kind.tail and not self.kind.late:
                self.tail_out(u).wait()
            for copy in self.param_forwards(u):
                copy.wait()

        def load_weight_start(self, u):
            self.load_weight(u).start()

    class LaneStage(Stage):
        def exchange(self, u):
            b = self.b
            half = self.kind.half
            src = self.grad.at[0, pl.ds(u * self.kind.unit + other * half, half)]
            return [remote(src, self.land.at[pl.ds(u * half, half)], b["d2d_s"].at[u, 0], b["d2d_r"].at[u, 0], partner)]

        def own_loads(self, u):
            b = self.b
            half = self.kind.half
            return [local(self.grad.at[0, pl.ds(u * self.kind.unit + core * half, half)], b["gf"], b["loc"].at[0]),
                    local(self.land.at[pl.ds(u * half, half)], b["df"], b["loc"].at[1])]

        def first_loads(self, u):
            for copy in self.exchange(u):
                copy.wait()
            for copy in self.own_loads(u):
                copy.start()

        def partial(self, u):
            kind, b = self.kind, self.b
            slot = self.slot(u)
            for copy in self.own_loads(u):
                copy.wait()
            cut = kind.rows // 2

            def far_piece(i, j, r):
                both = b["gf"][i, r * cut:(r + 1) * cut, :] + b["df"][i, r * cut:(r + 1) * cut, :]
                quarters = [both[:, BLOCK * d:BLOCK * (d + 1)] for d in range(4)]
                if j == 0:
                    near = [jnp.where(chip == 0, quarters[d], quarters[2 + d]) for d in range(2)]
                    b["nb"][slot, 0, i, r * cut:(r + 1) * cut, :] = jnp.where(core == 0, near[0], near[1])
                    b["nb"][slot, 1, i, r * cut:(r + 1) * cut, :] = jnp.where(core == 0, near[1], near[0])
                return jnp.where(chip == 0, quarters[2 + j], quarters[j])

            last = far_piece(1, 1, 1)
            for g in range(7):
                piece = far_piece(g // 4, g // 2 % 2, g % 2)
                b["sb"][slot, g] = jnp.concatenate([piece, last[:, 16 * g:16 * g + 16]], axis=1)

        def partial_sends(self, u):
            b = self.b
            return [remote(b["sb"].at[self.slot(u)], self.far_land.at[u], b["rs_s"].at[u, 0], b["rs_r"].at[u, 0], far_same)]

        def second_loads(self, u):
            self.load_mom(u).start()

        def combine(self, u):
            kind, b = self.kind, self.b
            slot = self.slot(u)
            for copy in self.partial_sends(u):
                copy.wait()
            copy = local(self.far_land.at[u], b["xl"], b["loc"].at[6])
            copy.start()
            copy.wait()
            cut = kind.rows // 2
            for i in range(kind.half):
                for r in range(2):
                    rows = slice(r * cut, (r + 1) * cut)
                    first = b["xl"][i * 4 + r][:, :BLOCK]
                    if i * 4 + 2 + r < 7:
                        second = b["xl"][i * 4 + 2 + r][:, :BLOCK]
                    else:
                        second = jnp.concatenate([b["xl"][g][:, BLOCK:LANE] for g in range(7)], axis=1)
                    b["nb"][slot, 0, i, rows, :] = b["nb"][slot, 0, i, rows, :] + jnp.where(core == 0, first, second)
                    b["tq"][i, rows, :] = b["nb"][slot, 1, i, rows, :] + jnp.where(core == 0, second, first)

        def total_send(self, u):
            b = self.b
            return remote(b["tq"], b["tr"].at[u], b["t_s"].at[u, 0], b["t_r"].at[u, 0], partner)

        def combine_start(self, u):
            self.total_send(u).start()

        def momentum(self, u):
            kind, b = self.kind, self.b
            slot = self.slot(u)
            self.load_mom(u).wait()
            self.total_send(u).wait()
            for base, total in ((core * kind.half, lambda i: b["nb"][slot, 0, i]), (other * kind.half, lambda i: b["tr"][u, i])):
                for i in range(kind.half):
                    value = MOMENTUM * b["mo"][slot, base + i] + total(i) * 0.25
                    b["mo"][slot, base + i] = value
                    sq_sum = jnp.sum(jnp.sum(value * value, axis=0, keepdims=True), axis=1, keepdims=True)
                    b["nr"][u, me, pl.ds(base + i, 1), :] = jnp.broadcast_to(sq_sum, (1, LANE))
            self.mom_out(u).start()

        def lane_block(self, device):
            return pl.ds(pl.multiple_of(device * LANE, LANE), LANE)

        def start_sends(self, u):
            kind, b = self.kind, self.b
            slot = self.slot(u)
            routes = (
                (b["xs"].at[slot, pl.ds(other * kind.half, kind.half)], b["xg"].at[u, :, :, self.lane_block(me)], partner),
                (b["xp"].at[slot, 0], b["xq"].at[u, 0], far_same),
                (b["xp"].at[slot, 1], b["xq"].at[u, 1], far_other),
            )
            return [remote(src, dst, b["x_s"].at[u, i], b["x_r"].at[u, i], device) for i, (src, dst, device) in enumerate(routes)]

        def start_matrix(self, u):
            kind, b = self.kind, self.b
            slot = self.slot(u)
            for copy in self.norm_sends(u):
                copy.wait()
            total = ((b["nr"][u, 0] + b["nr"][u, 1]) + b["nr"][u, 2]) + b["nr"][u, 3]
            norm = jnp.sqrt(total) + NORM_EPS
            pad = jnp.zeros((kind.rows, 16), F32)
            for i in range(kind.unit):
                start = b["mo"][slot, i] / norm[i:i + 1, 0:1]
                b["xs"][slot, i] = jnp.concatenate([start, pad], axis=1).astype(BF16)
            b["xg"][u, :, :, self.lane_block(me)] = b["xs"][slot, pl.ds(core * kind.half, kind.half)]
            cut = kind.rows // 4
            for h, base in enumerate((core * kind.half, other * kind.half)):
                pieces = [b["xs"][slot, base + g // 4, g % 4 * cut:(g % 4 + 1) * cut, :].astype(F32)[:, :BLOCK] for g in range(8)]
                for g, block in enumerate(pack(pieces)):
                    b["xp"][slot, h, g] = block.astype(BF16)
            self.mom_out(u).wait()

        def iterate(self, u):
            kind, b = self.kind, self.b
            for copy in self.start_sends(u):
                copy.wait()
            cut = kind.rows // 4
            pad = jnp.zeros((cut, 16), F32)
            for h, device in enumerate((far_same, far_other)):
                pieces = unpack([b["xq"][u, h, g].astype(F32) for g in range(7)])
                for g, piece in enumerate(pieces):
                    block = jnp.concatenate([piece, pad], axis=1).astype(BF16)
                    b["xg"][u, g // 4, g % 4 * cut:(g % 4 + 1) * cut, self.lane_block(device)] = block
            newton_schulz(kind, b["xg"], u, gram_acc)

        def ortho_send(self, u):
            b = self.b
            return remote(b["xg"].at[u, :, :, self.lane_block(partner)], b["orow"].at[u], b["o_s"].at[u, 0], b["o_r"].at[u, 0], partner)

        def param_out(self, u):
            return local(self.b["pk"].at[self.slot(u)], self.param_land.at[u, me], self.b["loc"].at[14 + self.slot(u)])

        def param_sends(self, u):
            b = self.b
            place = self.param_land.at[u, me]
            return [
                remote(b["pk"].at[self.slot(u)], place, b["p_s"].at[u, i], b["p_r"].at[u, i], device)
                for i, device in enumerate((partner, far_same))
            ]

        def param_forwards(self, u):
            b = self.b
            place = self.param_land.at[u, far_same]
            return [remote(place, place, b["p_s"].at[u, 2], b["p_r"].at[u, 2], partner)]

        def update(self, u):
            kind, b = self.kind, self.b
            self.load_weight(u).wait()
            self.ortho_send(u).wait()
            weight = b["w"]
            parts = ((core * kind.half, lambda j: b["xg"][u, j, :, self.lane_block(me)]),
                     (other * kind.half, lambda j: b["orow"][u, j]))
            for base, ortho in parts:
                for j in range(kind.half):
                    old = weight[base + j]
                    new = old - LEARN_RATE * (kind.scale * ortho(j).astype(F32)[:, :BLOCK] + WEIGHT_DECAY * old)
                    weight[base + j] = new
                    b["pb"][base + j] = new.astype(BF16)
            cut = kind.rows // 2
            pieces = [b["pb"][g // 2, g % 2 * cut:(g % 2 + 1) * cut, :].astype(F32) for g in range(8)]
            for g, block in enumerate(pack(pieces)):
                b["pk"][self.slot(u), g] = block.astype(BF16)

        def matrix_out(self, u):
            return local(self.b["pa"], self.param.at[self.mats(u)], self.b["loc"].at[2])

        def finish(self, u):
            kind, b = self.kind, self.b
            for copy in self.param_forwards(u):
                copy.wait()
            copy = local(self.param_land.at[u], b["pv"], b["loc"].at[3])
            copy.start()
            copy.wait()
            cut = kind.rows // 2
            for g in range(8):
                if g < 7:
                    quarters = [b["pv"][d, g].astype(F32)[:, :BLOCK] for d in range(4)]
                else:
                    quarters = [unpack([b["pv"][d, k].astype(F32) for k in range(7)])[7] for d in range(4)]
                b["pa"][g // 2, g % 2 * cut:(g % 2 + 1) * cut, :] = jnp.concatenate(quarters, axis=1).astype(BF16)
            self.matrix_out(u).start()

        def close(self, u):
            self.matrix_out(u).wait()

    stages = [LaneStage(kind) if kind.lanes else Stage(kind) for kind in kinds]
    bases = {}
    total_units = 0
    for k in ORDER:
        bases[k] = total_units
        total_units += kinds[k].units

    def step(t, carry):
        def run(name, lag):
            for k in ORDER:
                method = getattr(stages[k], name, None)
                if method is None:
                    continue
                u = t - lag - bases[k]

                @pl.when((u >= 0) & (u < kinds[k].units))
                def _(method=method, u=u):
                    method(u)

        for name, lag in SCHEDULE:
            run(name, lag)
        return carry

    lax.fori_loop(0, total_units + STEPS_BEHIND, step, 0)


def copy_kernel(cuts, num, *refs):
    sources, targets, stores = refs[:num], refs[num:2 * num], refs[2 * num:3 * num]
    in_sem, out_sem = refs[3 * num:]
    loads = [pltpu.make_async_copy(sources[i].at[pl.ds(lo, size)], stores[i].at[pl.ds(lo, size)], in_sem.at[n])
             for n, (i, lo, size) in enumerate(cuts)]
    saves = [pltpu.make_async_copy(stores[i].at[pl.ds(lo, size)], targets[i].at[pl.ds(lo, size)], out_sem.at[n])
             for n, (i, lo, size) in enumerate(cuts)]
    for load in loads:
        load.start()
    for load, save in zip(loads, saves):
        load.wait()
        save.start()
    for save in saves:
        save.wait()


def copy_out(arrays, pieces):
    cuts = []
    for i, array in enumerate(arrays):
        size = max(1, array.shape[0] // pieces)
        cuts += [(i, lo, size) for lo in range(0, array.shape[0], size)]
    total = sum(array.size * array.dtype.itemsize for array in arrays)
    return pl.pallas_call(
        functools.partial(copy_kernel, cuts, len(arrays)),
        out_shape=[jax.ShapeDtypeStruct(array.shape, array.dtype) for array in arrays],
        in_specs=[pl.BlockSpec(memory_space=pl.ANY)] * len(arrays),
        out_specs=[pl.BlockSpec(memory_space=pl.ANY)] * len(arrays),
        scratch_shapes=[pltpu.VMEM(array.shape, array.dtype) for array in arrays]
        + [pltpu.SemaphoreType.DMA((len(cuts),))] * 2,
        compiler_params=pltpu.CompilerParams(vmem_limit_bytes=67043328),
        cost_estimate=pl.CostEstimate(flops=1200 * total, bytes_accessed=2 * total, transcendentals=0),
    )(*arrays)


def gather_kernel(num, *refs):
    sources, targets, stores, sems = refs[:4 * num], refs[4 * num:5 * num], refs[5 * num:8 * num], refs[8 * num:]
    me = lax.axis_index("data")
    chip, core = me // 2, me % 2
    places = (me, 2 * (1 - chip) + core, 2 * chip + 1 - core, 2 * (1 - chip) + 1 - core)
    loads, saves = [], []
    for k in range(num):
        rows = sources[k].shape[1]
        for i, place in enumerate(places):
            source = sources[i * num + k]
            if i < 3:
                store = stores[i * num + k]
                loads.append(pltpu.make_async_copy(source, store, sems[0].at[i, k]))
                source = store
            cut = pl.ds(pl.multiple_of(place * rows, PAD), rows)
            saves.append((i < 3, pltpu.make_async_copy(source, targets[k].at[:, cut, :], sems[1].at[i, k])))
    for load in loads:
        load.start()
    for ready in (False, True):
        for load in loads if ready else []:
            load.wait()
        for waits, save in saves:
            if waits == ready:
                save.start()
    for _, save in saves:
        save.wait()


def gather_rows(owns, arrays):
    num = len(owns)
    cores = [(0, 1), (1, 0), (2, 3), (3, 2)]
    fars = [lax.ppermute(own, "data", [(0, 2), (2, 0), (1, 3), (3, 1)]) for own in owns]
    nears = [lax.ppermute(own, "data", cores) for own in owns]
    copied = copy_out(arrays, 4)
    fars, nears, copied = lax.optimization_barrier((fars, nears, copied))
    near_fars = [lax.ppermute(far, "data", cores) for far in fars]
    gathered = pl.pallas_call(
        functools.partial(gather_kernel, num),
        out_shape=[jax.ShapeDtypeStruct((own.shape[0], 4 * own.shape[1], own.shape[2]), own.dtype) for own in owns],
        in_specs=[pl.BlockSpec(memory_space=pl.ANY)] * (3 * num) + [pl.BlockSpec(memory_space=pltpu.VMEM)] * num,
        out_specs=[pl.BlockSpec(memory_space=pl.ANY)] * num,
        scratch_shapes=[pltpu.VMEM(own.shape, own.dtype) for own in owns] * 3 + [pltpu.SemaphoreType.DMA((4, num))] * 2,
        cost_estimate=pl.CostEstimate(flops=0, bytes_accessed=16 * sum(own.size for own in owns), transcendentals=0),
    )(*owns, *fars, *nears, *near_fars)
    return gathered, copied


def solution(mesh):
    def local_step(*arrays):
        num = len(arrays) // 3
        kinds = [Kind(k, *arrays[k].shape[1:]) for k in range(num)]
        scratch = [kind.scratch() for kind in kinds]
        names = [tuple(shapes) for shapes in scratch]
        flat = [shape for shapes in scratch for shape in shapes.values()]
        flat.append(pltpu.VMEM((kinds[1].rows, kinds[1].rows), F32))
        row_shapes = [jax.ShapeDtypeStruct((kind.count, kind.q_rows, kind.q_cols), F32) for kind in kinds]
        full_shapes = [
            jax.ShapeDtypeStruct((kind.count,) + ((kind.q_rows, kind.q_cols) if kind.late else (kind.rows, kind.cols)), BF16)
            for kind in kinds
        ]
        land_shapes = [jax.ShapeDtypeStruct((kind.count, 2, kind.q_rows, kind.q_cols), F32) for kind in kinds]
        far_shapes = list(row_shapes)
        lane = kinds[3]
        land_shapes[3] = jax.ShapeDtypeStruct((lane.count // 2, lane.rows, lane.cols), F32)
        far_shapes[3] = jax.ShapeDtypeStruct((lane.units, 7, lane.rows // 2, LANE), F32)
        param_shape = jax.ShapeDtypeStruct((lane.units, 4, 7, lane.rows // 2, LANE), BF16)
        tail_shapes = [jax.ShapeDtypeStruct((kind.units, kind.pair, kind.q_rows, LANE), F32) for kind in kinds if kind.tail]
        flipped = [jnp.swapaxes(array, -1, -2) if kinds[i % num].flip else array for i, array in enumerate(arrays)]
        outs = pl.pallas_call(
            functools.partial(kernel, kinds, names),
            out_shape=row_shapes + row_shapes + full_shapes + land_shapes + far_shapes + [param_shape] + tail_shapes,
            in_specs=[pl.BlockSpec(memory_space=pl.ANY)] * (3 * num),
            out_specs=[pl.BlockSpec(memory_space=pl.ANY)] * (5 * num + 3),
            scratch_shapes=flat,
            compiler_params=pltpu.CompilerParams(
                collective_id=0, has_side_effects=True, vmem_limit_bytes=67043328
            ),
        )(*flipped)
        outs = list(outs[:3 * num])
        late = [2 * num + kind.index for kind in kinds if kind.late]
        early = [i for i in range(3 * num) if i not in late]
        gathered, copied = gather_rows([outs[i] for i in late], [outs[i] for i in early])
        for i, array in zip(early + late, list(copied) + list(gathered)):
            outs[i] = array
        return tuple(jnp.swapaxes(array, -1, -2) if kinds[i % num].flip else array for i, array in enumerate(outs[:3 * num]))

    grad_spec = P(("stage", "data"), None, None, None)
    row_spec = P("stage", "data", None)
    full_spec = P("stage", None, None)
    in_specs = (grad_spec,) * 5 + (row_spec,) * 10
    out_specs = (row_spec,) * 10 + (full_spec,) * 5
    return jax.shard_map(local_step, mesh=mesh, in_specs=in_specs, out_specs=out_specs, check_vma=False)
```

```python
import functools
import math
import jax
import jax.numpy as jnp
from jax import lax
from jax.experimental import pallas as pl
from jax.experimental.pallas import tpu as pltpu
from jax.sharding import PartitionSpec as P

NS_STEPS = 5
MOMENTUM = 0.95
LEARN_RATE = 0.2
WEIGHT_DECAY = 0.25
NORM_EPS = 1e-7
COEF_A = 3.4445
COEF_B = -4.7750
COEF_C = 2.0315
F32 = jnp.float32
BF16 = jnp.bfloat16

UNIT_MATS = (2, 2, 1, 4, 4)
ORDER = (4, 2, 1, 3, 0)
LANE, MAIN, TAIL, BLOCK, PAD = 128, 384, 64, 112, 16
UPDATE = 9
SCHEDULE = (
    ("exchange_start", 0), ("combine", 4), ("start_matrix", 6), ("close", UPDATE + 3), ("drain", UPDATE + 1),
    ("load_weight_start", UPDATE), ("first_loads", 2), ("second_loads", 4),
    ("start_start", 6), ("combine_start", 4), ("momentum", 4), ("norm_start", 4),
    ("partial", 2), ("iterate", 7), ("partial_start", 2), ("iterate_start", 7),
    ("update", UPDATE), ("update_start", UPDATE), ("finish", UPDATE + 2), ("forward", UPDATE + 1),
)
STEPS_BEHIND = max(lag for _, lag in SCHEDULE)


class Kind:
    def __init__(self, index, count, rows, cols):
        self.index = index
        self.scale = 0.2 * math.sqrt(max(rows, cols))
        self.flip = index in (2, 3)
        if self.flip:
            rows, cols = cols, rows
        self.lanes = index == 3
        self.tail = index in (0, 4)
        self.count, self.rows, self.cols = count, rows, cols
        self.q_rows, self.q_cols = (rows, cols // 4) if self.flip else (rows // 4, cols)
        self.unit = UNIT_MATS[index]
        self.units = count // self.unit
        self.split = self.unit % 2 == 0
        self.half = self.unit // 2 if self.split else self.unit
        self.single = self.units == 1
        self.late = index == 1
        self.pair = self.unit // 2
        self.half_pair = self.half // 2 if self.tail else 0
        if index == 1:
            self.chunks = [(0, 1, 0, self.q_rows), (1, 1, 0, self.q_rows)]
        elif index == 2:
            step = self.q_rows // 2
            self.chunks = [(0, 1, 0, step), (0, 1, step, step)]
        else:
            self.chunks = [(0, self.unit, 0, self.q_rows)]

    def sems(self):
        shapes = {name: pltpu.SemaphoreType.DMA((self.units, 5)) for name in (
            "d2d_s", "d2d_r", "rs_s", "rs_r", "nm_s", "nm_r", "x_s", "x_r", "o_s", "o_r", "p_s", "p_r", "t_s", "t_r")}
        shapes["loc"] = pltpu.SemaphoreType.DMA((16,))
        return shapes

    def scratch(self):
        if self.lanes:
            return self.lane_scratch()
        unit, q_rows, q_cols = self.unit, self.q_rows, self.q_cols
        slots = 1 if self.single else 2
        _, cmats, _, crows = self.chunks[0]
        chunk = pltpu.VMEM((cmats, crows, q_cols), F32)
        shapes = dict(
            gf=chunk, df=chunk, xl=chunk,
            mo=pltpu.VMEM((slots, unit, q_rows, q_cols), F32),
            sb=pltpu.VMEM((slots, unit, q_rows, q_cols), F32),
            xs=pltpu.VMEM((slots, unit, q_rows, q_cols), BF16),
            xg=pltpu.VMEM((self.units, self.half, self.rows, self.cols), BF16),
            nr=pltpu.VMEM((self.units, 4, 8, LANE), F32),
        )
        if not self.single:
            shapes["gn"] = chunk
            shapes["dn"] = chunk
            shapes["w"] = pltpu.VMEM((unit, q_rows, q_cols), F32)
            shapes["pb"] = pltpu.VMEM((2, unit, q_rows, q_cols), BF16)
        if self.tail:
            shapes["st"] = pltpu.VMEM((slots, self.pair, q_rows, LANE), F32)
            shapes["xt"] = pltpu.VMEM((self.pair, q_rows, LANE), F32)
            shapes["pst"] = pltpu.VMEM((2, self.pair, q_rows, LANE), BF16)
            shapes["ptq"] = pltpu.VMEM((self.units, self.pair, q_rows, LANE), BF16)
            shapes["ptu"] = pltpu.VMEM((unit, q_rows, TAIL), BF16)
        if self.half_pair:
            shapes["xts"] = pltpu.VMEM((slots, 2, self.half_pair, q_rows, LANE), BF16)
            shapes["xtq"] = pltpu.VMEM((self.units, 2, self.half_pair, q_rows, LANE), BF16)
        if self.split:
            shapes["orow"] = pltpu.VMEM((self.units, self.half, q_rows, q_cols), BF16)
        shapes.update(self.sems())
        return shapes

    def lane_scratch(self):
        unit, half, rows, cols, lanes, units = self.unit, self.half, self.rows, self.cols, self.q_cols, self.units
        shapes = dict(
            gf=pltpu.VMEM((half, rows, cols), F32),
            df=pltpu.VMEM((half, rows, cols), F32),
            sb=pltpu.VMEM((2, 7, rows // 2, LANE), F32),
            nb=pltpu.VMEM((2, 2, half, rows, lanes), F32),
            xl=pltpu.VMEM((7, rows // 2, LANE), F32),
            tq=pltpu.VMEM((half, rows, lanes), F32),
            tr=pltpu.VMEM((units, half, rows, lanes), F32),
            mo=pltpu.VMEM((2, unit, rows, lanes), F32),
            w=pltpu.VMEM((unit, rows, lanes), F32),
            xs=pltpu.VMEM((2, unit, rows, LANE), BF16),
            xp=pltpu.VMEM((2, 2, 7, rows // 4, LANE), BF16),
            xq=pltpu.VMEM((units, 2, 7, rows // 4, LANE), BF16),
            xg=pltpu.VMEM((units, half, rows, 512), BF16),
            orow=pltpu.VMEM((units, half, rows, LANE), BF16),
            pb=pltpu.VMEM((unit, rows, lanes), BF16),
            pk=pltpu.VMEM((2, 7, rows // 2, LANE), BF16),
            pv=pltpu.VMEM((4, 7, rows // 2, LANE), BF16),
            pa=pltpu.VMEM((unit, rows, cols), BF16),
            nr=pltpu.VMEM((units, 4, 8, LANE), F32),
        )
        shapes.update(self.sems())
        return shapes


def pack(pieces):
    last = pieces[7]
    return [jnp.concatenate([pieces[g], last[:, 16 * g:16 * g + 16]], axis=1) for g in range(7)]


def join(left, right):
    return jnp.concatenate([left[:, MAIN:MAIN + TAIL], right[:, MAIN:MAIN + TAIL]], axis=1)


def unpack(blocks):
    return [block[:, :BLOCK] for block in blocks] + [jnp.concatenate([block[:, BLOCK:LANE] for block in blocks], axis=1)]


def dot(left, right, dims):
    return lax.dot_general(left, right, (dims, ((), ())), preferred_element_type=F32)


def newton_schulz(kind, xg, u, gram_acc):
    cols = kind.cols

    def poly(gram_mat):
        square = dot(gram_mat, gram_mat, ((1,), (0,)))
        return (COEF_B * gram_mat.astype(F32) + COEF_C * square).astype(BF16)

    if kind.single:
        block = 512

        def iteration(_, carry):
            gram_acc[...] = jnp.zeros_like(gram_acc)

            def add(b, c):
                part = xg[u, 0, :, pl.ds(pl.multiple_of(b * block, block), block)]
                gram_acc[...] += dot(part, part, ((1,), (1,)))
                return c

            lax.fori_loop(0, cols // block, add, 0)
            poly_mat = poly(gram_acc[...].astype(BF16))

            def apply(b, c):
                cut = pl.ds(pl.multiple_of(b * block, block), block)
                part = xg[u, 0, :, cut]
                update = dot(poly_mat, part, ((1,), (0,)))
                xg[u, 0, :, cut] = (COEF_A * part.astype(F32) + update).astype(BF16)
                return c

            lax.fori_loop(0, cols // block, apply, 0)
            return carry
    else:

        def iteration(_, carry):
            mats = [xg[u, j] for j in range(kind.half)]
            polys = [poly(gram_mat) for gram_mat in [dot(mat, mat, ((1,), (1,))).astype(BF16) for mat in mats]]
            news = [COEF_A * mat.astype(F32) + dot(poly_mat, mat, ((1,), (0,))) for poly_mat, mat in zip(polys, mats)]
            for j, new in enumerate(news):
                xg[u, j] = new.astype(BF16)
            return carry

    lax.fori_loop(0, NS_STEPS, iteration, 0)


def kernel(kinds, names, *refs):
    num = len(kinds)
    grads, moms, masters = refs[:num], refs[num:2 * num], refs[2 * num:3 * num]
    outs = refs[3 * num:8 * num]
    new_moms, new_masters, params, lands, far_lands = [outs[i * num:(i + 1) * num] for i in range(5)]
    param_land = refs[8 * num]
    far_tails = {0: refs[8 * num + 1], 4: refs[8 * num + 2]}
    rest = list(refs[8 * num + 3:])
    bufs = []
    for k in range(num):
        bufs.append({name: rest.pop(0) for name in names[k]})
    gram_acc = rest.pop(0)

    me = lax.axis_index("data")
    chip, core = me // 2, me % 2
    far, other = 1 - chip, 1 - core
    partner, far_same, far_other = 2 * chip + other, 2 * far + core, 2 * far + other

    def to(device):
        return dict(device_id={"data": device}, device_id_type=pl.DeviceIdType.MESH)

    def remote(src, dst, send, recv, device):
        return pltpu.make_async_remote_copy(src_ref=src, dst_ref=dst, send_sem=send, recv_sem=recv, **to(device))

    def local(src, dst, sem):
        return pltpu.make_async_copy(src, dst, sem)

    barrier = pltpu.get_barrier_semaphore()
    for device in (partner, far_same, far_other):
        pl.semaphore_signal(barrier, inc=1, **to(device))
    pl.semaphore_wait(barrier, 3)

    def block_of(kind, device, row=0, nrow=None):
        nrow = kind.q_rows if nrow is None else nrow
        if kind.flip:
            return pl.ds(row, nrow), pl.ds(pl.multiple_of(device * kind.q_cols, LANE), kind.q_cols)
        return pl.ds(pl.multiple_of(device * kind.q_rows + row, 16), nrow), slice(None)

    class Stage:
        def __init__(self, kind):
            self.kind = kind
            self.b = bufs[kind.index]
            self.grad, self.mom, self.master = grads[kind.index], moms[kind.index], masters[kind.index]
            self.new_mom, self.new_master, self.param = new_moms[kind.index], new_masters[kind.index], params[kind.index]
            self.land, self.far_land = lands[kind.index], far_lands[kind.index]
            self.param_land = param_land
            self.far_tail = far_tails.get(kind.index)

        def mats(self, u, offset=0, size=None):
            kind = self.kind
            return pl.ds(u * kind.unit + offset, kind.unit if size is None else size)

        def slot(self, u):
            return 0 if self.kind.single else u % 2

        def exchange(self, u):
            kind, b = self.kind, self.b
            mats = self.mats(u)
            return [
                remote(self.grad.at[(0, mats) + block_of(kind, quarter)], self.land.at[mats, i],
                       b["d2d_s"].at[u, i], b["d2d_r"].at[u, i], partner)
                for i, quarter in enumerate((far_other, partner))
            ]

        def exchange_start(self, u):
            for copy in self.exchange(u):
                copy.start()

        def load_pair(self, u, chunk, which):
            kind, b = self.kind, self.b
            mat, nmat, row, nrow = chunk
            mats = self.mats(u, mat, nmat)
            quarter, g, d, i = (far_same, "gf", "df", 0) if which == 0 else (me,) + (("gf", "df") if kind.single else ("gn", "dn")) + (1,)
            return [
                local(self.grad.at[(0, mats) + block_of(kind, quarter, row, nrow)], b[g], b["loc"].at[2 * i]),
                local(self.land.at[mats, i, pl.ds(row, nrow), :], b[d], b["loc"].at[2 * i + 1]),
            ]

        def load_mom(self, u):
            return local(self.mom.at[self.mats(u)], self.b["mo"].at[self.slot(u)], self.b["loc"].at[4])

        def weight(self):
            return self.b["sb"].at[0] if self.kind.single else self.b["w"]

        def rounded(self, u):
            return self.b["xs"].at[0] if self.kind.single else self.b["pb"].at[self.slot(u)]

        def load_weight(self, u):
            return local(self.master.at[self.mats(u)], self.weight(), self.b["loc"].at[5])

        def partial_sends(self, u):
            b = self.b
            src, dst = b["sb"].at[self.slot(u)], self.far_land.at[self.mats(u)]
            pairs = [(src, dst)]
            if self.kind.tail:
                pairs = [(b["sb"].at[self.slot(u), :, :, 0:MAIN], self.far_land.at[self.mats(u), :, 0:MAIN]),
                         (b["st"].at[self.slot(u)], self.far_tail.at[u])]
            return [remote(src, dst, b["rs_s"].at[u, i], b["rs_r"].at[u, i], far_same) for i, (src, dst) in enumerate(pairs)]

        def first_loads(self, u):
            for i, copy in enumerate(self.exchange(u)):
                copy.wait()
            for copy in self.load_pair(u, self.kind.chunks[0], 0):
                copy.start()

        def partial(self, u):
            kind, b = self.kind, self.b
            for index, chunk in enumerate(kind.chunks):
                mat, nmat, row, nrow = chunk
                copies = self.load_pair(u, chunk, 0)
                if index:
                    for copy in copies:
                        copy.start()
                for copy in copies:
                    copy.wait()
                b["sb"][self.slot(u), mat:mat + nmat, row:row + nrow, :] = b["gf"][...] + b["df"][...]
            if kind.tail:
                for i in range(kind.pair):
                    b["st"][self.slot(u), i] = join(b["sb"][self.slot(u), i], b["sb"][self.slot(u), i + kind.pair])

        def partial_start(self, u):
            for copy in self.partial_sends(u):
                copy.start()

        def second_loads(self, u):
            for copy in self.load_pair(u, self.kind.chunks[0], 1):
                copy.start()
            self.load_mom(u).start()

        def norm_sends(self, u):
            b = self.b
            return [
                remote(b["nr"].at[u, me], b["nr"].at[u, me], b["nm_s"].at[u, i], b["nm_r"].at[u, i], device)
                for i, device in enumerate((partner, far_same, far_other))
            ]

        def mom_out(self, u):
            return local(self.b["mo"].at[self.slot(u)], self.new_mom.at[self.mats(u)], self.b["loc"].at[12 + self.slot(u)])

        def momentum(self, u):
            kind, b = self.kind, self.b
            slot = self.slot(u)
            for copy in self.partial_sends(u):
                copy.wait()
            self.load_mom(u).wait()
            near_g, near_d = ("gf", "df") if kind.single else ("gn", "dn")
            sums = [None] * kind.unit
            for index, chunk in enumerate(kind.chunks):
                mat, nmat, row, nrow = chunk
                if kind.tail:
                    far_copies = [local(self.far_land.at[self.mats(u), :, 0:MAIN], b["xl"].at[:, :, 0:MAIN], b["loc"].at[6]),
                                  local(self.far_tail.at[u], b["xt"], b["loc"].at[10])]
                else:
                    far_copies = [local(self.far_land.at[self.mats(u, mat, nmat), pl.ds(row, nrow), :], b["xl"], b["loc"].at[6])]
                for copy in far_copies:
                    copy.start()
                copies = self.load_pair(u, chunk, 1)
                if index:
                    for copy in copies:
                        copy.start()
                for copy in copies:
                    copy.wait()
                for copy in far_copies:
                    copy.wait()
                for i in range(nmat):
                    if kind.tail:
                        lane = i // kind.pair * TAIL
                        cuts = ((slice(0, MAIN), b["xl"][i, :, 0:MAIN]),
                                (slice(MAIN, MAIN + TAIL), b["xt"][i % kind.pair][:, lane:lane + TAIL]))
                    else:
                        cuts = ((slice(0, kind.q_cols), b["xl"][i]),)
                    for cut, far_sum in cuts:
                        total = (b[near_g][i, :, cut] + b[near_d][i, :, cut]) + far_sum
                        value = MOMENTUM * b["mo"][slot, mat + i, row:row + nrow, cut] + total * 0.25
                        b["mo"][slot, mat + i, row:row + nrow, cut] = value
                        sq_sum = jnp.sum(jnp.sum(value * value, axis=0, keepdims=True), axis=1, keepdims=True)
                        sums[mat + i] = sq_sum if sums[mat + i] is None else sums[mat + i] + sq_sum
            for i in range(kind.unit):
                b["nr"][u, me, i:i + 1, :] = jnp.broadcast_to(sums[i], (1, LANE))
            self.mom_out(u).start()

        def norm_start(self, u):
            for copy in self.norm_sends(u):
                copy.start()

        def start_sends(self, u):
            kind, b = self.kind, self.b
            slot = self.slot(u)
            place = b["xg"].at[(u, slice(None)) + block_of(kind, me)]
            if kind.split:
                mine = b["xs"].at[slot, pl.ds(core * kind.half, kind.half)]
                theirs = b["xs"].at[slot, pl.ds(other * kind.half, kind.half)]
                routes = [(theirs, place, partner), (mine, place, far_same), (theirs, place, far_other)]
            else:
                routes = [(b["xs"].at[slot], place, partner), (b["xs"].at[slot], place, far_same)]
            if kind.half_pair:
                main = b["xg"].at[u, :, block_of(kind, me)[0], 0:MAIN]
                for h, base in enumerate((core * kind.half, other * kind.half)):
                    routes[1 + h] = (b["xs"].at[slot, pl.ds(base, kind.half), :, 0:MAIN], main, routes[1 + h][2])
                routes += [(b["xts"].at[slot, h], b["xtq"].at[u, h], device) for h, device in enumerate((far_same, far_other))]
            return [remote(src, dst, b["x_s"].at[u, i], b["x_r"].at[u, i], device) for i, (src, dst, device) in enumerate(routes)]

        def start_forward(self, u):
            kind, b = self.kind, self.b
            place = b["xg"].at[(u, slice(None)) + block_of(kind, far_same)]
            return remote(place, place, b["x_s"].at[u, 2], b["x_r"].at[u, 2], partner)

        def start_matrix(self, u):
            kind, b = self.kind, self.b
            slot = self.slot(u)
            for copy in self.norm_sends(u):
                copy.wait()
            total = ((b["nr"][u, 0] + b["nr"][u, 1]) + b["nr"][u, 2]) + b["nr"][u, 3]
            norm = jnp.sqrt(total) + NORM_EPS
            for i in range(kind.unit):
                b["xs"][slot, i] = (b["mo"][slot, i] / norm[i:i + 1, 0:1]).astype(BF16)
            if kind.split:
                b["xg"][(u, slice(None)) + block_of(kind, me)] = b["xs"][slot, pl.ds(core * kind.half, kind.half)]
            else:
                b["xg"][(u, slice(None)) + block_of(kind, me)] = b["xs"][slot]
            if kind.half_pair:
                for h, base in enumerate((core * kind.half, other * kind.half)):
                    for i in range(kind.half_pair):
                        left = b["xs"][slot, base + i].astype(F32)
                        right = b["xs"][slot, base + i + kind.half_pair].astype(F32)
                        b["xts"][slot, h, i] = join(left, right).astype(BF16)
            self.mom_out(u).wait()

        def start_start(self, u):
            for copy in self.start_sends(u):
                copy.start()

        def ortho_send(self, u):
            kind, b = self.kind, self.b
            return remote(b["xg"].at[(u, slice(None)) + block_of(kind, partner)], b["orow"].at[u], b["o_s"].at[u, 0], b["o_r"].at[u, 0], partner)

        def iterate(self, u):
            for copy in self.start_sends(u):
                copy.wait()
            if not self.kind.split:
                forward = self.start_forward(u)
                forward.start()
                forward.wait()
            if self.kind.half_pair:
                kind, b = self.kind, self.b
                for h, device in enumerate((far_same, far_other)):
                    for i in range(kind.half_pair):
                        both = b["xtq"][u, h, i].astype(F32)
                        for side in range(2):
                            part = both[:, TAIL * side:TAIL * side + TAIL].astype(BF16)
                            b["xg"][u, i + side * kind.half_pair, block_of(kind, device)[0], MAIN:MAIN + TAIL] = part
            newton_schulz(self.kind, self.b["xg"], u, gram_acc)

        def iterate_start(self, u):
            if self.kind.split:
                self.ortho_send(u).start()

        def weight_out(self, u):
            return local(self.weight(), self.new_master.at[self.mats(u)], self.b["loc"].at[8])

        def param_out(self, u):
            if self.kind.late:
                return local(self.rounded(u), self.param.at[self.mats(u)], self.b["loc"].at[14 + self.slot(u)])
            return local(self.rounded(u), self.param.at[(self.mats(u),) + block_of(self.kind, me)], self.b["loc"].at[14 + self.slot(u)])

        def param_sends(self, u):
            kind, b = self.kind, self.b
            if kind.late:
                return []
            place = self.param.at[(self.mats(u),) + block_of(kind, me)]
            routes = [(self.rounded(u), place, partner, 0), (self.rounded(u), place, far_same, 1)]
            if kind.tail:
                main = self.param.at[self.mats(u), block_of(kind, me)[0], 0:MAIN]
                routes[1:] = [(b["pb"].at[self.slot(u), :, :, 0:MAIN], main, far_same, 1), (b["pst"].at[self.slot(u)], b["ptq"].at[u], far_same, 3)]
            return [remote(src, dst, b["p_s"].at[u, i], b["p_r"].at[u, i], device) for src, dst, device, i in routes]

        def param_forwards(self, u):
            kind, b = self.kind, self.b
            if kind.late:
                return []
            place = self.param.at[(self.mats(u),) + block_of(kind, far_same)]
            routes = [(place, place, 2)]
            if kind.tail:
                main = self.param.at[self.mats(u), block_of(kind, far_same)[0], 0:MAIN]
                routes = [(main, main, 2), (b["ptu"], self.tail_place(u), 4)]
            return [remote(src, dst, b["p_s"].at[u, i], b["p_r"].at[u, i], partner) for src, dst, i in routes]

        def tail_place(self, u):
            return self.param.at[self.mats(u), block_of(self.kind, far_same)[0], MAIN:MAIN + TAIL]

        def tail_out(self, u):
            return local(self.b["ptu"], self.tail_place(u), self.b["loc"].at[11])

        def update(self, u):
            kind, b = self.kind, self.b
            self.load_weight(u).wait()
            weight = self.weight()
            if kind.split:
                self.ortho_send(u).wait()
                parts = ((core * kind.half, lambda j: b["xg"][(u, j) + block_of(kind, me)]),
                         (other * kind.half, lambda j: b["orow"][u, j]))
            else:
                parts = ((0, lambda j: b["xg"][(u, j) + block_of(kind, me)]),)
            for base, ortho in parts:
                for j in range(kind.half):
                    old = weight[base + j]
                    new = old - LEARN_RATE * (kind.scale * ortho(j).astype(F32) + WEIGHT_DECAY * old)
                    weight[base + j] = new
                    self.rounded(u)[base + j] = new.astype(BF16)
            if kind.tail and not kind.late:
                for i in range(kind.pair):
                    left, right = (b["pb"][self.slot(u), j].astype(F32) for j in (i, i + kind.pair))
                    b["pst"][self.slot(u), i] = join(left, right).astype(BF16)

        def update_start(self, u):
            self.weight_out(u).start()
            self.param_out(u).start()
            for copy in self.param_sends(u):
                copy.start()

        def drain(self, u):
            self.weight_out(u).wait()

        def forward(self, u):
            self.param_out(u).wait()
            for copy in self.param_sends(u):
                copy.wait()
            kind, b = self.kind, self.b
            if kind.tail and not kind.late:
                for i in range(kind.unit):
                    lane = i // kind.pair * TAIL
                    b["ptu"][i] = b["ptq"][u, i % kind.pair].astype(F32)[:, lane:lane + TAIL].astype(BF16)
                self.tail_out(u).start()
            for copy in self.param_forwards(u):
                copy.start()

        def finish(self, u):
            if self.kind.tail and not self.kind.late:
                self.tail_out(u).wait()
            for copy in self.param_forwards(u):
                copy.wait()

        def load_weight_start(self, u):
            self.load_weight(u).start()

    class LaneStage(Stage):
        def exchange(self, u):
            b = self.b
            half = self.kind.half
            src = self.grad.at[0, pl.ds(u * self.kind.unit + other * half, half)]
            return [remote(src, self.land.at[pl.ds(u * half, half)], b["d2d_s"].at[u, 0], b["d2d_r"].at[u, 0], partner)]

        def own_loads(self, u):
            b = self.b
            half = self.kind.half
            return [local(self.grad.at[0, pl.ds(u * self.kind.unit + core * half, half)], b["gf"], b["loc"].at[0]),
                    local(self.land.at[pl.ds(u * half, half)], b["df"], b["loc"].at[1])]

        def first_loads(self, u):
            for copy in self.exchange(u):
                copy.wait()
            for copy in self.own_loads(u):
                copy.start()

        def partial(self, u):
            kind, b = self.kind, self.b
            slot = self.slot(u)
            for copy in self.own_loads(u):
                copy.wait()
            cut = kind.rows // 2

            def far_piece(i, j, r):
                both = b["gf"][i, r * cut:(r + 1) * cut, :] + b["df"][i, r * cut:(r + 1) * cut, :]
                quarters = [both[:, BLOCK * d:BLOCK * (d + 1)] for d in range(4)]
                if j == 0:
                    near = [jnp.where(chip == 0, quarters[d], quarters[2 + d]) for d in range(2)]
                    b["nb"][slot, 0, i, r * cut:(r + 1) * cut, :] = jnp.where(core == 0, near[0], near[1])
                    b["nb"][slot, 1, i, r * cut:(r + 1) * cut, :] = jnp.where(core == 0, near[1], near[0])
                return jnp.where(chip == 0, quarters[2 + j], quarters[j])

            last = far_piece(1, 1, 1)
            for g in range(7):
                piece = far_piece(g // 4, g // 2 % 2, g % 2)
                b["sb"][slot, g] = jnp.concatenate([piece, last[:, 16 * g:16 * g + 16]], axis=1)

        def partial_sends(self, u):
            b = self.b
            return [remote(b["sb"].at[self.slot(u)], self.far_land.at[u], b["rs_s"].at[u, 0], b["rs_r"].at[u, 0], far_same)]

        def second_loads(self, u):
            self.load_mom(u).start()

        def combine(self, u):
            kind, b = self.kind, self.b
            slot = self.slot(u)
            for copy in self.partial_sends(u):
                copy.wait()
            copy = local(self.far_land.at[u], b["xl"], b["loc"].at[6])
            copy.start()
            copy.wait()
            cut = kind.rows // 2
            for i in range(kind.half):
                for r in range(2):
                    rows = slice(r * cut, (r + 1) * cut)
                    first = b["xl"][i * 4 + r][:, :BLOCK]
                    if i * 4 + 2 + r < 7:
                        second = b["xl"][i * 4 + 2 + r][:, :BLOCK]
                    else:
                        second = jnp.concatenate([b["xl"][g][:, BLOCK:LANE] for g in range(7)], axis=1)
                    b["nb"][slot, 0, i, rows, :] = b["nb"][slot, 0, i, rows, :] + jnp.where(core == 0, first, second)
                    b["tq"][i, rows, :] = b["nb"][slot, 1, i, rows, :] + jnp.where(core == 0, second, first)

        def total_send(self, u):
            b = self.b
            return remote(b["tq"], b["tr"].at[u], b["t_s"].at[u, 0], b["t_r"].at[u, 0], partner)

        def combine_start(self, u):
            self.total_send(u).start()

        def momentum(self, u):
            kind, b = self.kind, self.b
            slot = self.slot(u)
            self.load_mom(u).wait()
            self.total_send(u).wait()
            for base, total in ((core * kind.half, lambda i: b["nb"][slot, 0, i]), (other * kind.half, lambda i: b["tr"][u, i])):
                for i in range(kind.half):
                    value = MOMENTUM * b["mo"][slot, base + i] + total(i) * 0.25
                    b["mo"][slot, base + i] = value
                    sq_sum = jnp.sum(jnp.sum(value * value, axis=0, keepdims=True), axis=1, keepdims=True)
                    b["nr"][u, me, pl.ds(base + i, 1), :] = jnp.broadcast_to(sq_sum, (1, LANE))
            self.mom_out(u).start()

        def lane_block(self, device):
            return pl.ds(pl.multiple_of(device * LANE, LANE), LANE)

        def start_sends(self, u):
            kind, b = self.kind, self.b
            slot = self.slot(u)
            routes = (
                (b["xs"].at[slot, pl.ds(other * kind.half, kind.half)], b["xg"].at[u, :, :, self.lane_block(me)], partner),
                (b["xp"].at[slot, 0], b["xq"].at[u, 0], far_same),
                (b["xp"].at[slot, 1], b["xq"].at[u, 1], far_other),
            )
            return [remote(src, dst, b["x_s"].at[u, i], b["x_r"].at[u, i], device) for i, (src, dst, device) in enumerate(routes)]

        def start_matrix(self, u):
            kind, b = self.kind, self.b
            slot = self.slot(u)
            for copy in self.norm_sends(u):
                copy.wait()
            total = ((b["nr"][u, 0] + b["nr"][u, 1]) + b["nr"][u, 2]) + b["nr"][u, 3]
            norm = jnp.sqrt(total) + NORM_EPS
            pad = jnp.zeros((kind.rows, 16), F32)
            for i in range(kind.unit):
                start = b["mo"][slot, i] / norm[i:i + 1, 0:1]
                b["xs"][slot, i] = jnp.concatenate([start, pad], axis=1).astype(BF16)
            b["xg"][u, :, :, self.lane_block(me)] = b["xs"][slot, pl.ds(core * kind.half, kind.half)]
            cut = kind.rows // 4
            for h, base in enumerate((core * kind.half, other * kind.half)):
                pieces = [b["xs"][slot, base + g // 4, g % 4 * cut:(g % 4 + 1) * cut, :].astype(F32)[:, :BLOCK] for g in range(8)]
                for g, block in enumerate(pack(pieces)):
                    b["xp"][slot, h, g] = block.astype(BF16)
            self.mom_out(u).wait()

        def iterate(self, u):
            kind, b = self.kind, self.b
            for copy in self.start_sends(u):
                copy.wait()
            cut = kind.rows // 4
            pad = jnp.zeros((cut, 16), F32)
            for h, device in enumerate((far_same, far_other)):
                pieces = unpack([b["xq"][u, h, g].astype(F32) for g in range(7)])
                for g, piece in enumerate(pieces):
                    block = jnp.concatenate([piece, pad], axis=1).astype(BF16)
                    b["xg"][u, g // 4, g % 4 * cut:(g % 4 + 1) * cut, self.lane_block(device)] = block
            newton_schulz(kind, b["xg"], u, gram_acc)

        def ortho_send(self, u):
            b = self.b
            return remote(b["xg"].at[u, :, :, self.lane_block(partner)], b["orow"].at[u], b["o_s"].at[u, 0], b["o_r"].at[u, 0], partner)

        def param_out(self, u):
            return local(self.b["pk"].at[self.slot(u)], self.param_land.at[u, me], self.b["loc"].at[14 + self.slot(u)])

        def param_sends(self, u):
            b = self.b
            place = self.param_land.at[u, me]
            return [
                remote(b["pk"].at[self.slot(u)], place, b["p_s"].at[u, i], b["p_r"].at[u, i], device)
                for i, device in enumerate((partner, far_same))
            ]

        def param_forwards(self, u):
            b = self.b
            place = self.param_land.at[u, far_same]
            return [remote(place, place, b["p_s"].at[u, 2], b["p_r"].at[u, 2], partner)]

        def update(self, u):
            kind, b = self.kind, self.b
            self.load_weight(u).wait()
            self.ortho_send(u).wait()
            weight = b["w"]
            parts = ((core * kind.half, lambda j: b["xg"][u, j, :, self.lane_block(me)]),
                     (other * kind.half, lambda j: b["orow"][u, j]))
            for base, ortho in parts:
                for j in range(kind.half):
                    old = weight[base + j]
                    new = old - LEARN_RATE * (kind.scale * ortho(j).astype(F32)[:, :BLOCK] + WEIGHT_DECAY * old)
                    weight[base + j] = new
                    b["pb"][base + j] = new.astype(BF16)
            cut = kind.rows // 2
            pieces = [b["pb"][g // 2, g % 2 * cut:(g % 2 + 1) * cut, :].astype(F32) for g in range(8)]
            for g, block in enumerate(pack(pieces)):
                b["pk"][self.slot(u), g] = block.astype(BF16)

        def matrix_out(self, u):
            return local(self.b["pa"], self.param.at[self.mats(u)], self.b["loc"].at[2])

        def finish(self, u):
            kind, b = self.kind, self.b
            for copy in self.param_forwards(u):
                copy.wait()
            copy = local(self.param_land.at[u], b["pv"], b["loc"].at[3])
            copy.start()
            copy.wait()
            cut = kind.rows // 2
            for g in range(8):
                if g < 7:
                    quarters = [b["pv"][d, g].astype(F32)[:, :BLOCK] for d in range(4)]
                else:
                    quarters = [unpack([b["pv"][d, k].astype(F32) for k in range(7)])[7] for d in range(4)]
                b["pa"][g // 2, g % 2 * cut:(g % 2 + 1) * cut, :] = jnp.concatenate(quarters, axis=1).astype(BF16)
            self.matrix_out(u).start()

        def close(self, u):
            self.matrix_out(u).wait()

    stages = [LaneStage(kind) if kind.lanes else Stage(kind) for kind in kinds]
    bases = {}
    total_units = 0
    for k in ORDER:
        bases[k] = total_units
        total_units += kinds[k].units

    def step(t, carry):
        def run(name, lag):
            for k in ORDER:
                method = getattr(stages[k], name, None)
                if method is None:
                    continue
                u = t - lag - bases[k]

                @pl.when((u >= 0) & (u < kinds[k].units))
                def _(method=method, u=u):
                    method(u)

        for name, lag in SCHEDULE:
            run(name, lag)
        return carry

    lax.fori_loop(0, total_units + STEPS_BEHIND, step, 0)


def row_cut(array, place):
    rows = array.shape[1]
    return pl.ds(pl.multiple_of(place * rows, PAD), rows)


def copy_kernel(cuts, num, parts, *refs):
    total = num + parts
    sources, refs = refs[:total], refs[total:]
    targets, refs = refs[:num], refs[num:]
    if parts:
        whole, refs = refs[0], refs[1:]
    stores, (in_sem, out_sem) = refs[:total], refs[total:]
    routes = [(sources[i].at[pl.ds(lo, size)], stores[i].at[pl.ds(lo, size)], targets[i].at[pl.ds(lo, size)]) for i, lo, size in cuts]
    if parts:
        me = lax.axis_index("data")
        chip, core = me // 2, me % 2
        places = (me, 2 * (1 - chip) + core, 2 * chip + 1 - core)
        routes += [(source, store, whole.at[:, row_cut(source, place), :])
                   for source, store, place in zip(sources[num:], stores[num:], places)]
    loads = [pltpu.make_async_copy(source, store, in_sem.at[n]) for n, (source, store, _) in enumerate(routes)]
    saves = [pltpu.make_async_copy(store, target, out_sem.at[n]) for n, (_, store, target) in enumerate(routes)]
    for load in loads:
        load.start()
    for load, save in zip(loads, saves):
        load.wait()
        save.start()
    for save in saves:
        save.wait()


def copy_out(arrays, pieces, parts=()):
    cuts = []
    for i, array in enumerate(arrays):
        size = max(1, array.shape[0] // pieces)
        cuts += [(i, lo, size) for lo in range(0, array.shape[0], size)]
    total = sum(array.size * array.dtype.itemsize for array in arrays)
    shapes = [jax.ShapeDtypeStruct(array.shape, array.dtype) for array in arrays]
    if parts:
        count, rows, cols = parts[0].shape
        shapes.append(jax.ShapeDtypeStruct((count, 4 * rows, cols), parts[0].dtype))
    return pl.pallas_call(
        functools.partial(copy_kernel, cuts, len(arrays), len(parts)),
        out_shape=shapes,
        in_specs=[pl.BlockSpec(memory_space=pl.ANY)] * (len(arrays) + len(parts)),
        out_specs=[pl.BlockSpec(memory_space=pl.ANY)] * len(shapes),
        scratch_shapes=[pltpu.VMEM(array.shape, array.dtype) for array in (*arrays, *parts)]
        + [pltpu.SemaphoreType.DMA((len(cuts) + len(parts),))] * 2,
        compiler_params=pltpu.CompilerParams(vmem_limit_bytes=67043328),
        cost_estimate=pl.CostEstimate(flops=1200 * total, bytes_accessed=2 * total, transcendentals=0),
    )(*arrays, *parts)


def place_kernel(rows, _, whole, store, sem):
    me = lax.axis_index("data")
    place = 2 * (1 - me // 2) + 1 - me % 2
    load = pltpu.make_async_copy(rows, store, sem.at[0])
    save = pltpu.make_async_copy(store, whole.at[:, row_cut(rows, place), :], sem.at[1])
    load.start()
    load.wait()
    save.start()
    save.wait()


def gather_rows(own, arrays, later):
    cores = [(0, 1), (1, 0), (2, 3), (3, 2)]
    far = lax.ppermute(own, "data", [(0, 2), (2, 0), (1, 3), (3, 1)])
    near = lax.ppermute(own, "data", cores)
    copied = copy_out(arrays, 4)
    far, near, later, copied = lax.optimization_barrier((far, near, later, copied))
    near_far = lax.ppermute(far, "data", cores)
    *copied_later, whole = copy_out(later, 4, (own, far, near))
    near_far, whole = lax.optimization_barrier((near_far, whole))
    whole = pl.pallas_call(
        place_kernel,
        out_shape=jax.ShapeDtypeStruct(whole.shape, whole.dtype),
        in_specs=[pl.BlockSpec(memory_space=pl.ANY)] * 2,
        out_specs=pl.BlockSpec(memory_space=pl.ANY),
        scratch_shapes=[pltpu.VMEM(own.shape, own.dtype), pltpu.SemaphoreType.DMA((2,))],
        input_output_aliases={1: 0},
    )(near_far, whole)
    return list(copied) + copied_later + [whole]


def solution(mesh):
    def local_step(*arrays):
        num = len(arrays) // 3
        kinds = [Kind(k, *arrays[k].shape[1:]) for k in range(num)]
        scratch = [kind.scratch() for kind in kinds]
        names = [tuple(shapes) for shapes in scratch]
        flat = [shape for shapes in scratch for shape in shapes.values()]
        flat.append(pltpu.VMEM((kinds[1].rows, kinds[1].rows), F32))
        row_shapes = [jax.ShapeDtypeStruct((kind.count, kind.q_rows, kind.q_cols), F32) for kind in kinds]
        full_shapes = [
            jax.ShapeDtypeStruct((kind.count,) + ((kind.q_rows, kind.q_cols) if kind.late else (kind.rows, kind.cols)), BF16)
            for kind in kinds
        ]
        land_shapes = [jax.ShapeDtypeStruct((kind.count, 2, kind.q_rows, kind.q_cols), F32) for kind in kinds]
        far_shapes = list(row_shapes)
        lane = kinds[3]
        land_shapes[3] = jax.ShapeDtypeStruct((lane.count // 2, lane.rows, lane.cols), F32)
        far_shapes[3] = jax.ShapeDtypeStruct((lane.units, 7, lane.rows // 2, LANE), F32)
        param_shape = jax.ShapeDtypeStruct((lane.units, 4, 7, lane.rows // 2, LANE), BF16)
        tail_shapes = [jax.ShapeDtypeStruct((kind.units, kind.pair, kind.q_rows, LANE), F32) for kind in kinds if kind.tail]
        flipped = [jnp.swapaxes(array, -1, -2) if kinds[i % num].flip else array for i, array in enumerate(arrays)]
        outs = pl.pallas_call(
            functools.partial(kernel, kinds, names),
            out_shape=row_shapes + row_shapes + full_shapes + land_shapes + far_shapes + [param_shape] + tail_shapes,
            in_specs=[pl.BlockSpec(memory_space=pl.ANY)] * (3 * num),
            out_specs=[pl.BlockSpec(memory_space=pl.ANY)] * (5 * num + 3),
            scratch_shapes=flat,
            compiler_params=pltpu.CompilerParams(
                collective_id=0, has_side_effects=True, vmem_limit_bytes=67043328
            ),
        )(*flipped)
        outs = list(outs[:3 * num])
        late = next(2 * num + kind.index for kind in kinds if kind.late)
        later = [1, num - 1]
        early = [i for i in range(3 * num) if i != late and i not in later]
        finals = gather_rows(outs[late], [outs[i] for i in early], [outs[i] for i in later])
        for i, array in zip(early + later + [late], finals):
            outs[i] = array
        return tuple(jnp.swapaxes(array, -1, -2) if kinds[i % num].flip else array for i, array in enumerate(outs[:3 * num]))

    grad_spec = P(("stage", "data"), None, None, None)
    row_spec = P("stage", "data", None)
    full_spec = P("stage", None, None)
    in_specs = (grad_spec,) * 5 + (row_spec,) * 10
    out_specs = (row_spec,) * 10 + (full_spec,) * 5
    return jax.shard_map(local_step, mesh=mesh, in_specs=in_specs, out_specs=out_specs, check_vma=False)
```
